512 devices in a mesh: seq: 64 (over x, y, core), tp: 8 (over z).
Axes of the slice: x: 4, y: 8, z: 8, core: 2. Of those that a mesh axis runs over, the one named last changes fastest.
Arguments:
- img: bfloat16 [4, 2048, 3072], P(None, 'seq', 'tp'), may hold values from -6 to 6
- txt: bfloat16 [4, 256, 3072], P(None, 'seq', 'tp'), may hold values from -6 to 6
- prev_mod: bfloat16 [4, 2048, 3072], P(None, 'seq', 'tp'), may hold values from -47 to 47
- cache: float32 [4, 2048, 3072], P(None, 'seq', 'tp'), may hold values from -6 to 6
- modulation: bfloat16 [3, 4, 3072], P(None, None, 'tp'), may hold values from -4 to 4
- w_qkv: bfloat16 [3072, 3, 2048], P('seq', None, 'tp'), may hold values from -1 to 1, as said below
- qk_gain: float32 [2, 2048], P(None, 'tp'), may hold values from 0.5 to 6, as said below
- output_weight: bfloat16 [2048, 3072], P('tp'), may hold values from -0.1875 to 0.1875
- text_len: int32 [4], replicated, may hold values from 1 to 256
- refresh: int32 [4], replicated, may hold values from 0 to 1, as said below
Outputs:
- out_img: float32 [4, 2048, 3072], P(None, 'seq', 'tp')
- new_cache: float32 [4, 2048, 3072], P(None, 'seq', 'tp')
- rel_l1: float32 [4], replicated
The draws below stay inside these ranges and needn't reach their ends.
Inputs may be any that keep to these rules, and one draw needn't show every extreme that they name: `refresh`: at least one sequence has flag 1 and at least one has flag 0. `w_qkv`: entries of spread about one over the square root of 3072. `qk_gain`: positive.
All inputs are finite; a program needn't handle non-finite values.
Results may differ from the reference program's by a relative error of at most 0.013.
The reference program's roundings to bfloat16 on the way count: a program that leaves them out, or rounds other values in their place, can miss the bound.
Values may be sent and summed in bfloat16 or wider, within the bound.
No kernel may reach another device: no remote copies, remote signals or barrier semaphores. Data moves between devices by JAX's collectives and lax.ppermute only.
A program may use at most 128 MiB of HBM per device.

```python
import math
import jax
import jax.numpy as jnp
from jax import lax

D = 3072
HEADS = 16
HD = 128
BATCH = 4
IMG = 2048
TXT = 256


def draw_w_qkv(key, part):
    limit = 6.0 / math.sqrt(D)
    base = jnp.clip(jax.random.normal(key, (D, 3, HEADS * HD), jnp.float32) / math.sqrt(D), -limit, limit)
    return base.astype(jnp.bfloat16)


def draw_qk_gain(key, part):
    logs = jax.random.uniform(key, (2, HEADS * HD), jnp.float32, math.log(0.5), math.log(3.0))
    return jnp.exp(logs)


def draw_prev_mod(key, part):
    first = jax.random.fold_in(key, 11)
    second = jax.random.fold_in(key, 12)
    third = jax.random.fold_in(key, 13)
    base = jnp.clip(jax.random.normal(first, (BATCH, IMG, D), jnp.float32), -4.0, 4.0)
    rough = jnp.exp(jax.random.uniform(second, (BATCH, IMG, 1), jnp.float32, math.log(0.5), math.log(2.0)))
    slope = jax.random.uniform(third, (BATCH, 1, 1), jnp.float32, -3.5, 3.5)
    place = (jnp.arange(IMG, dtype=jnp.float32) + 0.5) / IMG - 0.5
    ramp = jnp.exp(slope * place[None, :, None])
    return (base * rough * ramp).astype(jnp.bfloat16)


def draw_refresh(key, part):
    flags = jax.random.randint(jax.random.fold_in(key, 21), (BATCH,), 0, 2)
    chosen_on = jax.random.randint(jax.random.fold_in(key, 22), (), 0, BATCH)
    stride = jax.random.randint(jax.random.fold_in(key, 23), (), 0, BATCH - 1)
    chosen_off = (chosen_on + 1 + stride) % BATCH
    index = jnp.arange(BATCH, dtype=jnp.int32)
    flags = jnp.where(index == chosen_on, 1, jnp.where(index == chosen_off, 0, flags))
    return flags.astype(jnp.int32)


def touch_ends(values, key, low, top_value):
    longest = values.shape.index(max(values.shape))
    spots = []
    for shift in (0, 1):
        where = [jax.random.randint(jax.random.fold_in(key, axis), (), 0, length) for axis, length in enumerate(values.shape)]
        where[longest] = (where[longest] + shift) % values.shape[longest]
        spots.append(tuple(where))
    return values.at[spots[0]].set(low).at[spots[1]].set(top_value)


def spiked(values, rng, source, target, blocks, factor):
    owner, partner = [(jnp.arange(values.shape[position]) // (values.shape[position] // blocks)).reshape([-1 if axis == position else 1 for axis in range(values.ndim)]) for position in (source, target)]
    chosen = jax.random.permutation(rng, blocks)[partner]
    strong = (owner == chosen) | (owner == (partner + blocks // 2) % blocks)
    return jnp.where(strong, factor * values, values)


def block_scale(stream_key, extent, cuts, smallest, top_value):
    factor_of, own = 1.0, jax.random.fold_in(stream_key, 6)
    for dim, shards_of in cuts:
        draws = jnp.exp(jax.random.uniform(jax.random.fold_in(own, dim), (shards_of,), jnp.float32, smallest / len(cuts), top_value / len(cuts)))
        factor_of = factor_of * jnp.repeat(draws, extent[dim] // shards_of).reshape([-1 if axis == dim else 1 for axis in range(len(extent))])
    return factor_of


def gaussian(stream_key, extent, deviation, reach, pieces=(), kind=jnp.bfloat16):
    array = jax.random.normal(stream_key, extent, jnp.float32) * deviation
    if len(pieces) > 0:
        array = block_scale(stream_key, extent, pieces, -0.22, 0.18) * array
    return jnp.clip(array, min=-reach, max=reach).astype(kind)


def bell_draw_with(stream_key, extent, deviation, bound, shards, heavy, kind=jnp.bfloat16):
    result = deviation * jax.random.normal(stream_key, extent, jnp.float32)
    if shards:
        result = result * block_scale(stream_key, extent, shards, -0.22, 0.18)
    return jnp.clip(spiked(result, jax.random.fold_in(stream_key, 3), *heavy), -bound, bound).astype(kind)


def setup_inputs(seed: int = 0) -> dict:
    seeds = jax.random.split(jax.random.key(seed), 11)
    return {
        "img": gaussian(seeds[0], (BATCH, IMG, D), 1.0, 6.0, ((1, 64), (2, 8))),
        "txt": gaussian(seeds[1], (BATCH, TXT, D), 1.0, 6.0, ((1, 64), (2, 8))),
        "prev_mod": draw_prev_mod(jax.random.fold_in(seeds[10], 71), 0),
        "cache": gaussian(seeds[3], (BATCH, IMG, D), 1.0, 6.0, ((1, 64), (2, 8)), jnp.float32),
        "modulation": gaussian(seeds[4], (3, BATCH, D), 1.0, 4.0, ((2, 8),)),
        "w_qkv": draw_w_qkv(jax.random.fold_in(seeds[10], 71), 0),
        "qk_gain": draw_qk_gain(jax.random.fold_in(seeds[10], 71), 0),
        "output_weight": bell_draw_with(seeds[7], (HEADS * HD, D), (HEADS * HD) ** -0.5, 0.1875, ((0, 8),), (0, 1, 8, 2.0)),
        "text_len": touch_ends(jax.random.randint(seeds[8], (BATCH,), 1, TXT + 1), jax.random.fold_in(seeds[8], 1), 1, TXT).astype(jnp.int32),
        "refresh": draw_refresh(jax.random.fold_in(seeds[10], 71), 0),
    }


EPS = 0.1
NEG = -1e+30

def unit_heads(block, gain):
    shaped = block.reshape(block.shape[:-1] + (block.shape[-1] // HD, HD))
    scaled = shaped * lax.rsqrt(lax.optimization_barrier(jnp.mean(jnp.square(shaped), axis=-1, keepdims=True)) + EPS)
    return scaled.reshape(block.shape) * gain

def reference(img, txt, prev_mod, cache, modulation, w_qkv, qk_gain, output_weight, text_len, refresh):
    mods = modulation.astype(jnp.float32)
    joined = jnp.concatenate([txt, img], axis=1).astype(jnp.float32)
    center = lax.optimization_barrier(jnp.mean(joined, axis=2, keepdims=True))
    spread = lax.optimization_barrier(jnp.mean(jnp.square(joined - center), axis=2, keepdims=True))
    normed = (joined - center) * lax.rsqrt(spread + EPS)
    modded = (normed * (1.0 + mods[1][:, None, :]) + mods[0][:, None, :]).astype(jnp.bfloat16)
    image_mod = modded[:, TXT:, :].astype(jnp.float32)
    previous = prev_mod.astype(jnp.float32)
    numer = lax.optimization_barrier(jnp.sum(jnp.abs(image_mod - previous), axis=(1, 2)))
    denom = lax.optimization_barrier(jnp.sum(jnp.abs(previous), axis=(1, 2)))
    rel_l1 = numer / jnp.maximum(denom, 1.0)
    projected = jnp.einsum('btd,dkc->btkc', modded.astype(jnp.float32), w_qkv.astype(jnp.float32))
    query = unit_heads(projected[:, TXT:, 0, :], qk_gain[0]).astype(jnp.bfloat16)
    keyed = unit_heads(projected[:, :, 1, :], qk_gain[1]).astype(jnp.bfloat16)
    valued = projected[:, :, 2, :].astype(jnp.bfloat16)
    total_keys = TXT + IMG
    positions = jnp.arange(total_keys, dtype=jnp.int32)
    valid = (positions[None, :] >= TXT) | (positions[None, :] < text_len[:, None])
    query_heads = query.reshape(BATCH, IMG, HEADS, HD).transpose(2, 0, 1, 3)
    key_heads = keyed.reshape(BATCH, total_keys, HEADS, HD).transpose(2, 0, 1, 3)
    value_heads = valued.reshape(BATCH, total_keys, HEADS, HD).transpose(2, 0, 1, 3)
    score_scale = 1.0 / HD ** 0.5

    def one_head(group):
        query_slice, key_slice, value_slice = group
        logit_scores = jnp.einsum('sna,sva->snv', query_slice.astype(jnp.float32), key_slice.astype(jnp.float32)) * score_scale
        logit_scores = jnp.where(valid[:, None, :], logit_scores, NEG)
        top = lax.optimization_barrier(jnp.max(logit_scores, axis=2, keepdims=True))
        attention_weights = jnp.where(valid[:, None, :], jnp.exp(logit_scores - top), 0.0)
        total = lax.optimization_barrier(jnp.sum(attention_weights, axis=2, keepdims=True))
        summed_output = jnp.einsum('yef,yfp->yep', attention_weights.astype(jnp.bfloat16).astype(jnp.float32), value_slice.astype(jnp.float32))
        return (summed_output / total).astype(jnp.bfloat16)
    attended_values = lax.map(one_head, (query_heads, key_heads, value_heads))
    attended_values = attended_values.transpose(1, 2, 0, 3).reshape(BATCH, IMG, HEADS * HD)
    mixed_heads = jnp.einsum('pxr,ro->pxo', attended_values.astype(jnp.float32), output_weight.astype(jnp.float32))
    resid = mods[2][:, None, :] * mixed_heads
    flag = (refresh == 1)[:, None, None]
    new_cache = jnp.where(flag, resid, cache)
    out_img = img.astype(jnp.float32) + new_cache
    return (out_img, new_cache, rel_l1)
```

```python
import functools

import jax
import jax.numpy as jnp
from jax import lax
from jax.experimental import pallas as pl
from jax.experimental.pallas import tpu as pltpu
from jax.sharding import Mesh
from jax.sharding import PartitionSpec as P

HD = 128
SEQ = ("seq_0", "seq_1", "seq_2")
EPS = 0.1
NEG = -1e30
F32 = jnp.float32
BF16 = jnp.bfloat16

IMG_R = 32
TXT_R = 4
ROWS = 40
REL_ROW = IMG_R + TXT_R

VMEM = pl.BlockSpec(memory_space=pltpu.VMEM)
SMEM = pl.BlockSpec(memory_space=pltpu.SMEM)


def call(body, out_shape, in_specs, limit=40 << 20):
    outs = jax.tree.map(lambda _: VMEM, out_shape)
    return pl.pallas_call(
        body,
        out_shape=out_shape,
        in_specs=in_specs,
        out_specs=outs,
        compiler_params=pltpu.CompilerParams(vmem_limit_bytes=limit),
    )


def swap(value, axis):
    return lax.all_to_all(value, axis, 0, 0, tiled=True)


def spread_copies(value, count):
    return jnp.broadcast_to(value[None], (count,) + value.shape)


def split_three(value):
    high = value.astype(BF16).astype(F32)
    rest = value - high
    middle = rest.astype(BF16).astype(F32)
    return high, middle, rest - middle


def norm_body(tp_ref, x_ref, prev_ref, mod_ref, rel_ref):
    groups, rows, width = x_ref.shape
    batch = rows // ROWS
    features = groups * width
    sums = jnp.zeros((rows, 1), F32)
    for g in range(groups):
        sums = sums + jnp.sum(x_ref[g].astype(F32), axis=1, keepdims=True)
    center = sums / features
    squares = jnp.zeros((rows, 1), F32)
    for g in range(groups):
        squares = squares + jnp.sum(
            jnp.square(x_ref[g].astype(F32) - center), axis=1, keepdims=True
        )
    inv = lax.rsqrt(squares / features + EPS)
    for g in range(groups):
        normed = (x_ref[g].astype(F32) - center) * inv
        values = x_ref[g].astype(F32)
        parts = []
        for b in range(batch):
            at = b * ROWS
            shift = values[at + REL_ROW : at + REL_ROW + 1]
            scale = values[at + REL_ROW + 1 : at + REL_ROW + 2]
            parts.append(normed[at : at + ROWS] * (1.0 + scale) + shift)
        mod_ref[g] = jnp.concatenate(parts, axis=0).astype(BF16)
    own = mod_ref[tp_ref[0]].astype(F32)
    lane = lax.broadcasted_iota(jnp.int32, (8, 128), 1)
    rel = jnp.zeros((8, 128), F32)
    for b in range(batch):
        previous = prev_ref[b].astype(F32)
        gap = jnp.abs(own[b * ROWS : b * ROWS + IMG_R] - previous)
        rel = jnp.where(lane == b, jnp.sum(gap), rel)
        rel = jnp.where(lane == batch + b, jnp.sum(jnp.abs(previous)), rel)
    rel_ref[...] = rel


def project_body(mod_ref, w_ref, gain_ref, rel_ref, out_ref):
    groups, rows, width = mod_ref.shape
    cores, xs, ys, kinds, deep, columns = w_ref.shape
    batch = rows // ROWS
    heads = columns // HD
    high, middle, low = split_three(rel_ref[0:1, :])
    row = lax.broadcasted_iota(jnp.int32, (ROWS, HD), 0)
    per_group = width // (cores * deep)
    for kind in range(kinds):
        total = jnp.zeros((rows, columns), F32)
        for g in range(groups):
            pieces = []
            for step in range(per_group):
                flat = g * per_group + step
                for core in range(cores):
                    pieces.append(w_ref[core, flat // ys, flat % ys, kind])
            total = total + jnp.dot(
                mod_ref[g], jnp.concatenate(pieces, axis=0), preferred_element_type=F32
            )
        for h in range(heads):
            part = total[:, h * HD : (h + 1) * HD]
            if kind < 2:
                mean = jnp.mean(jnp.square(part), axis=1, keepdims=True)
                part = part * lax.rsqrt(mean + EPS) * gain_ref[kind : kind + 1, h * HD : (h + 1) * HD]
            for b in range(batch):
                block = part[b * ROWS : (b + 1) * ROWS]
                if kind == 1:
                    block = jnp.where(row == REL_ROW, high, block)
                    block = jnp.where(row == REL_ROW + 1, middle, block)
                    block = jnp.where(row == REL_ROW + 2, low, block)
                out_ref[b * heads + h, :, kind * HD : (kind + 1) * HD] = block.astype(BF16)


def attend_body(limit_ref, qkv_ref, kv_ref, out_ref, rel_ref):
    ys = qkv_ref.shape[0]
    spots = kv_ref.shape[0]
    count = spots * ys * ROWS
    query = jnp.concatenate([qkv_ref[y, :IMG_R, :HD] for y in range(ys)], axis=0)
    pairs = kv_ref[...].reshape(count, 2 * HD)
    keys = pairs[:, :HD]
    values = pairs[:, HD:]
    scores = lax.dot_general(
        query, keys, (((1,), (1,)), ((), ())), preferred_element_type=F32
    ) * (1.0 / HD**0.5)
    index = lax.broadcasted_iota(jnp.int32, (1, count), 1)
    slot = index % ROWS
    block = index // ROWS
    y = block % ys
    spot = block // ys
    place = (spot // 2) * (2 * ys) + y * 2 + spot % 2
    text = place * TXT_R + slot - IMG_R
    valid = (slot < IMG_R) | ((slot < IMG_R + TXT_R) & (text < limit_ref[0]))
    scores = jnp.where(valid, scores, NEG)
    top = jnp.max(scores, axis=1, keepdims=True)
    weights = jnp.where(valid, jnp.exp(scores - top), 0.0)
    total = jnp.sum(weights, axis=1, keepdims=True)
    summed = jnp.dot(weights.astype(BF16), values, preferred_element_type=F32)
    attended = (summed / total).astype(BF16)
    for y in range(ys):
        out_ref[y] = attended[y * IMG_R : (y + 1) * IMG_R]
    down = lax.broadcasted_iota(jnp.int32, (ROWS, HD), 0)
    held = (down >= REL_ROW) & (down < REL_ROW + 3)
    rel = jnp.zeros((1, HD), F32)
    for spot in range(spots):
        for y in range(ys):
            block = kv_ref[spot, y, :, :HD].astype(F32)
            rel = rel + jnp.sum(jnp.where(held, block, 0.0), axis=0, keepdims=True)
    rel_ref[...] = jnp.broadcast_to(rel, (8, HD))


def mix_body(att_ref, w_ref, rel_ref, out_ref):
    pairs = att_ref.shape[0]
    groups, _, width = out_ref.shape
    heads = w_ref.shape[0] // HD
    batch = pairs // heads
    rows = batch * IMG_R
    lefts = []
    for h in range(heads):
        lefts.append(jnp.concatenate([att_ref[b * heads + h] for b in range(batch)], axis=0))
    left = jnp.concatenate(lefts, axis=1)
    high, middle, low = split_three(rel_ref[0:1, :])
    row = lax.broadcasted_iota(jnp.int32, (8, HD), 0)
    tail = jnp.where(row == 0, high, jnp.where(row == 1, middle, jnp.where(row == 2, low, 0.0)))
    tail = jnp.concatenate([tail, jnp.zeros((8, width - HD), F32)], axis=1).astype(BF16)
    for g in range(groups):
        mixed = jnp.dot(left, w_ref[:, g * width : (g + 1) * width], preferred_element_type=F32)
        out_ref[g, :rows] = mixed.astype(BF16)
        out_ref[g, rows:] = tail


def final_body(flag_ref, part_ref, cache_ref, img_ref, mod_ref, out_ref, new_ref, rel_ref):
    groups = part_ref.shape[0]
    batch = img_ref.shape[0]
    rows = batch * IMG_R
    mixed = part_ref[0, :rows].astype(F32)
    rel = part_ref[0, rows:, :HD].astype(F32)
    for g in range(1, groups):
        mixed = mixed + part_ref[g, :rows].astype(F32)
        rel = rel + part_ref[g, rows:, :HD].astype(F32)
    for b in range(batch):
        gate = mod_ref[2, b : b + 1].astype(F32)
        resid = gate * mixed[b * IMG_R : (b + 1) * IMG_R]
        fresh = jnp.where(flag_ref[b] == 1, resid, cache_ref[b])
        new_ref[b] = fresh
        out_ref[b] = img_ref[b].astype(F32) + fresh
    sums = jnp.sum(rel, axis=0, keepdims=True)
    lane = lax.broadcasted_iota(jnp.int32, (1, HD), 1)
    ratio = jnp.zeros((8, HD), F32)
    for b in range(batch):
        numer = jnp.sum(jnp.where(lane == b, sums, 0.0), axis=1, keepdims=True)
        denom = jnp.sum(jnp.where(lane == batch + b, sums, 0.0), axis=1, keepdims=True)
        wide = lax.broadcasted_iota(jnp.int32, (8, HD), 1)
        ratio = jnp.where(wide == b, numer / jnp.maximum(denom, 1.0), ratio)
    rel_ref[...] = ratio


def local(img, txt, prev_mod, cache, modulation, w_qkv, qk_gain, output_weight, text_len, refresh):
    batch, img_rows, width = img.shape
    xs, ys, cores = (lax.axis_size(a) for a in SEQ)
    tps = lax.axis_size("tp")
    kinds, columns = w_qkv.shape[1:]
    deep = w_qkv.shape[0]
    heads = columns // HD

    with jax.named_scope("xgather"):
        pads = jnp.zeros((batch, ROWS - img_rows - txt.shape[1] - 2, width), BF16)
        joined = jnp.concatenate(
            [img, txt, modulation[0][:, None], modulation[1][:, None], pads], axis=1
        ).reshape(batch * ROWS, width)
        wide = swap(spread_copies(joined, tps), "tp")

    with jax.named_scope("wy"):
        weight = w_qkv.transpose(1, 0, 2)
        weight = swap(spread_copies(weight, ys), "seq_1")
    with jax.named_scope("wx"):
        weight = swap(spread_copies(weight, xs).reshape(xs, ys * kinds * deep, columns), "seq_0")
    with jax.named_scope("wc"):
        weight = swap(
            spread_copies(weight.reshape(xs * ys * kinds * deep, columns), cores), "seq_2"
        )
        weight = weight.reshape(cores, xs, ys, kinds, deep, columns)

    tp_index = lax.axis_index("tp").astype(jnp.int32)[None]
    modded, rel = call(
        norm_body,
        (
            jax.ShapeDtypeStruct((tps, batch * ROWS, width), BF16),
            jax.ShapeDtypeStruct((8, 128), F32),
        ),
        [SMEM, VMEM, VMEM],
    )(tp_index, wide, prev_mod)

    pairs = call(
        project_body,
        jax.ShapeDtypeStruct((batch * heads, ROWS, kinds * HD), BF16),
        [VMEM] * 4,
    )(modded, weight, qk_gain, rel)

    with jax.named_scope("qkvy"):
        pairs = swap(pairs, "seq_1")
    with jax.named_scope("kvxc"):
        gathered = swap(spread_copies(pairs[:, :, HD:], xs * cores), ("seq_0", "seq_2"))

    mine = lax.axis_index("seq_1") // heads
    limit = lax.dynamic_slice_in_dim(text_len, mine, 1)
    attended, rel = call(
        attend_body,
        (
            jax.ShapeDtypeStruct((ys, IMG_R, HD), BF16),
            jax.ShapeDtypeStruct((8, HD), F32),
        ),
        [SMEM, VMEM, VMEM],
    )(limit, pairs, gathered)

    with jax.named_scope("atty"):
        attended = swap(attended, "seq_1")
    parts = call(
        mix_body,
        jax.ShapeDtypeStruct((tps, batch * IMG_R + 8, width), BF16),
        [VMEM] * 3,
    )(attended, output_weight, rel)
    with jax.named_scope("mixz"):
        parts = swap(parts, "tp")

    shape = jax.ShapeDtypeStruct((batch, img_rows, width), F32)
    out_img, new_cache, ratio = call(
        final_body,
        (shape, shape, jax.ShapeDtypeStruct((8, HD), F32)),
        [SMEM, VMEM, VMEM, VMEM, VMEM],
    )(refresh, parts, cache, img, modulation)
    return (out_img, new_cache, ratio[0, :batch])


def solution(mesh):
    finer = Mesh(mesh.devices.reshape(4, 8, 2, mesh.shape["tp"]), ("seq_0", "seq_1", "seq_2", "tp"))
    in_specs = (
        P(None, SEQ, "tp"),
        P(None, SEQ, "tp"),
        P(None, SEQ, "tp"),
        P(None, SEQ, "tp"),
        P(None, None, "tp"),
        P(SEQ, None, "tp"),
        P(None, "tp"),
        P("tp", None),
        P(),
        P(),
    )
    out_specs = (P(None, SEQ, "tp"), P(None, SEQ, "tp"), P())
    return jax.shard_map(local, mesh=finer, in_specs=in_specs, out_specs=out_specs, check_vma=False)
```

```python
import jax
import jax.numpy as jnp
from jax import lax
from jax.experimental import pallas as pl
from jax.experimental.pallas import tpu as pltpu
from jax.sharding import Mesh
from jax.sharding import PartitionSpec as P


HD = 128
SEQ = ("seq_0", "seq_1", "seq_2")
EPS = 0.1
NEG = -1e30
F32 = jnp.float32
BF16 = jnp.bfloat16

IMG_R = 32
TXT_R = 4
ROWS = 40
REL_ROW = IMG_R + TXT_R

VMEM = pl.BlockSpec(memory_space=pltpu.VMEM)
SMEM = pl.BlockSpec(memory_space=pltpu.SMEM)


def call(body, out_shape, in_specs, limit=40 << 20):
    outs = jax.tree.map(lambda _: VMEM, out_shape)
    return pl.pallas_call(
        body,
        out_shape=out_shape,
        in_specs=in_specs,
        out_specs=outs,
        compiler_params=pltpu.CompilerParams(vmem_limit_bytes=limit),
    )


def swap(value, axis):
    return lax.all_to_all(value, axis, 0, 0, tiled=True)


def spread_copies(value, count):
    return jnp.broadcast_to(value[None], (count,) + value.shape)


def split_three(value):
    high = value.astype(BF16).astype(F32)
    rest = value - high
    middle = rest.astype(BF16).astype(F32)
    return high, middle, rest - middle


def norm_body(tp_ref, x_ref, prev_ref, mod_ref, rel_ref):
    groups, rows, width = x_ref.shape
    batch = rows // ROWS
    features = groups * width
    sums = jnp.zeros((rows, 1), F32)
    for g in range(groups):
        sums = sums + jnp.sum(x_ref[g].astype(F32), axis=1, keepdims=True)
    center = sums / features
    squares = jnp.zeros((rows, 1), F32)
    for g in range(groups):
        squares = squares + jnp.sum(
            jnp.square(x_ref[g].astype(F32) - center), axis=1, keepdims=True
        )
    inv = lax.rsqrt(squares / features + EPS)
    for g in range(groups):
        normed = (x_ref[g].astype(F32) - center) * inv
        values = x_ref[g].astype(F32)
        parts = []
        for b in range(batch):
            at = b * ROWS
            shift = values[at + REL_ROW : at + REL_ROW + 1]
            scale = values[at + REL_ROW + 1 : at + REL_ROW + 2]
            parts.append(normed[at : at + ROWS] * (1.0 + scale) + shift)
        mod_ref[g] = jnp.concatenate(parts, axis=0).astype(BF16)
    own = mod_ref[tp_ref[0]].astype(F32)
    lane = lax.broadcasted_iota(jnp.int32, (8, 128), 1)
    rel = jnp.zeros((8, 128), F32)
    for b in range(batch):
        previous = prev_ref[b].astype(F32)
        gap = jnp.abs(own[b * ROWS : b * ROWS + IMG_R] - previous)
        rel = jnp.where(lane == b, jnp.sum(gap), rel)
        rel = jnp.where(lane == batch + b, jnp.sum(jnp.abs(previous)), rel)
    rel_ref[...] = rel


def project_body(core_ref, mod_ref, own_ref, other_ref, gain_ref, rel_ref, out_ref):
    @pl.when(core_ref[0] == 0)
    def _():
        project(mod_ref, (own_ref, other_ref), gain_ref, rel_ref, out_ref)

    @pl.when(core_ref[0] == 1)
    def _():
        project(mod_ref, (other_ref, own_ref), gain_ref, rel_ref, out_ref)


def project(mod_ref, w_refs, gain_ref, rel_ref, out_ref):
    groups, rows, width = mod_ref.shape
    cores = len(w_refs)
    _, ys, kinds, deep, columns = w_refs[0].shape
    batch = rows // ROWS
    heads = columns // HD
    high, middle, low = split_three(rel_ref[0:1, :])
    row = lax.broadcasted_iota(jnp.int32, (ROWS, HD), 0)
    per_group = width // (cores * deep)
    for kind in range(kinds):
        total = jnp.zeros((rows, columns), F32)
        for g in range(groups):
            pieces = []
            for step in range(per_group):
                flat = g * per_group + step
                for core in range(cores):
                    pieces.append(w_refs[core][flat // ys, flat % ys, kind])
            total = total + jnp.dot(
                mod_ref[g], jnp.concatenate(pieces, axis=0), preferred_element_type=F32
            )
        for h in range(heads):
            part = total[:, h * HD : (h + 1) * HD]
            if kind < 2:
                mean = jnp.mean(jnp.square(part), axis=1, keepdims=True)
                part = part * lax.rsqrt(mean + EPS) * gain_ref[kind : kind + 1, h * HD : (h + 1) * HD]
            for b in range(batch):
                block = part[b * ROWS : (b + 1) * ROWS]
                if kind == 1:
                    block = jnp.where(row == REL_ROW, high, block)
                    block = jnp.where(row == REL_ROW + 1, middle, block)
                    block = jnp.where(row == REL_ROW + 2, low, block)
                out_ref[b * heads + h, :, kind * HD : (kind + 1) * HD] = block.astype(BF16)


def attend_body(limit_ref, qkv_ref, kv_ref, out_ref, rel_ref):
    ys = qkv_ref.shape[0]
    spots = kv_ref.shape[0]
    count = spots * ys * ROWS
    query = jnp.concatenate([qkv_ref[y, :IMG_R, :HD] for y in range(ys)], axis=0)
    pairs = kv_ref[...].reshape(count, 2 * HD)
    keys = pairs[:, :HD]
    values = pairs[:, HD:]
    scores = lax.dot_general(
        query, keys, (((1,), (1,)), ((), ())), preferred_element_type=F32
    ) * (1.0 / HD**0.5)
    index = lax.broadcasted_iota(jnp.int32, (1, count), 1)
    slot = index % ROWS
    block = index // ROWS
    y = block % ys
    spot = block // ys
    place = (spot // 2) * (2 * ys) + y * 2 + spot % 2
    text = place * TXT_R + slot - IMG_R
    valid = (slot < IMG_R) | ((slot < IMG_R + TXT_R) & (text < limit_ref[0]))
    scores = jnp.where(valid, scores, NEG)
    top = jnp.max(scores, axis=1, keepdims=True)
    weights = jnp.where(valid, jnp.exp(scores - top), 0.0)
    total = jnp.sum(weights, axis=1, keepdims=True)
    summed = jnp.dot(weights.astype(BF16), values, preferred_element_type=F32)
    attended = (summed / total).astype(BF16)
    for y in range(ys):
        out_ref[y] = attended[y * IMG_R : (y + 1) * IMG_R]
    down = lax.broadcasted_iota(jnp.int32, (ROWS, HD), 0)
    held = (down >= REL_ROW) & (down < REL_ROW + 3)
    rel = jnp.zeros((1, HD), F32)
    for spot in range(spots):
        for y in range(ys):
            block = kv_ref[spot, y, :, :HD].astype(F32)
            rel = rel + jnp.sum(jnp.where(held, block, 0.0), axis=0, keepdims=True)
    rel_ref[...] = jnp.broadcast_to(rel, (8, HD))


def mix_body(att_ref, w_ref, rel_ref, out_ref):
    pairs = att_ref.shape[0]
    groups, _, width = out_ref.shape
    heads = w_ref.shape[0] // HD
    batch = pairs // heads
    rows = batch * IMG_R
    lefts = []
    for h in range(heads):
        lefts.append(jnp.concatenate([att_ref[b * heads + h] for b in range(batch)], axis=0))
    left = jnp.concatenate(lefts, axis=1)
    high, middle, low = split_three(rel_ref[0:1, :])
    row = lax.broadcasted_iota(jnp.int32, (8, HD), 0)
    tail = jnp.where(row == 0, high, jnp.where(row == 1, middle, jnp.where(row == 2, low, 0.0)))
    tail = jnp.concatenate([tail, jnp.zeros((8, width - HD), F32)], axis=1).astype(BF16)
    for g in range(groups):
        mixed = jnp.dot(left, w_ref[:, g * width : (g + 1) * width], preferred_element_type=F32)
        out_ref[g, :rows] = mixed.astype(BF16)
        out_ref[g, rows:] = tail


def final_body(flag_ref, part_ref, cache_ref, img_ref, mod_ref, out_ref, new_ref, rel_ref):
    groups = part_ref.shape[0]
    batch = img_ref.shape[0]
    rows = batch * IMG_R
    mixed = part_ref[0, :rows].astype(F32)
    rel = part_ref[0, rows:, :HD].astype(F32)
    for g in range(1, groups):
        mixed = mixed + part_ref[g, :rows].astype(F32)
        rel = rel + part_ref[g, rows:, :HD].astype(F32)
    for b in range(batch):
        gate = mod_ref[2, b : b + 1].astype(F32)
        resid = gate * mixed[b * IMG_R : (b + 1) * IMG_R]
        fresh = jnp.where(flag_ref[b] == 1, resid, cache_ref[b])
        new_ref[b] = fresh
        out_ref[b] = img_ref[b].astype(F32) + fresh
    sums = jnp.sum(rel, axis=0, keepdims=True)
    lane = lax.broadcasted_iota(jnp.int32, (1, HD), 1)
    ratio = jnp.zeros((8, HD), F32)
    for b in range(batch):
        numer = jnp.sum(jnp.where(lane == b, sums, 0.0), axis=1, keepdims=True)
        denom = jnp.sum(jnp.where(lane == batch + b, sums, 0.0), axis=1, keepdims=True)
        wide = lax.broadcasted_iota(jnp.int32, (8, HD), 1)
        ratio = jnp.where(wide == b, numer / jnp.maximum(denom, 1.0), ratio)
    rel_ref[...] = ratio


def local(img, txt, prev_mod, cache, modulation, w_qkv, qk_gain, output_weight, text_len, refresh):
    batch, img_rows, width = img.shape
    xs, ys, cores = (lax.axis_size(a) for a in SEQ)
    tps = lax.axis_size("tp")
    kinds, columns = w_qkv.shape[1:]
    deep = w_qkv.shape[0]
    heads = columns // HD

    pads = jnp.zeros((batch, ROWS - img_rows - txt.shape[1] - 2, width), BF16)
    joined = jnp.concatenate(
        [img, txt, modulation[0][:, None], modulation[1][:, None], pads], axis=1
    ).reshape(batch * ROWS, width)
    wide = lax.all_gather(joined, "tp", axis=0, tiled=False)

    weight = w_qkv.transpose(1, 0, 2)
    weight = swap(spread_copies(weight, ys), "seq_1")
    weight = swap(spread_copies(weight, xs).reshape(xs, ys * kinds * deep, columns), "seq_0")
    weight = weight.reshape(xs, ys, kinds, deep, columns)
    other = lax.ppermute(weight, "seq_2", [(0, 1), (1, 0)])

    tp_index = lax.axis_index("tp").astype(jnp.int32)[None]
    core_index = lax.axis_index("seq_2").astype(jnp.int32)[None]
    modded, rel = call(
        norm_body,
        (
            jax.ShapeDtypeStruct((tps, batch * ROWS, width), BF16),
            jax.ShapeDtypeStruct((8, 128), F32),
        ),
        [SMEM, VMEM, VMEM],
    )(tp_index, wide, prev_mod)

    pairs = call(
        project_body,
        jax.ShapeDtypeStruct((batch * heads, ROWS, kinds * HD), BF16),
        [SMEM] + [VMEM] * 5,
    )(core_index, modded, weight, other, qk_gain, rel)

    pairs = swap(pairs, "seq_1")
    gathered = swap(spread_copies(pairs[:, :, HD:], xs * cores), ("seq_0", "seq_2"))

    mine = lax.axis_index("seq_1") // heads
    limit = lax.dynamic_slice_in_dim(text_len, mine, 1)
    attended, rel = call(
        attend_body,
        (
            jax.ShapeDtypeStruct((ys, IMG_R, HD), BF16),
            jax.ShapeDtypeStruct((8, HD), F32),
        ),
        [SMEM, VMEM, VMEM],
    )(limit, pairs, gathered)

    attended = swap(attended, "seq_1")
    parts = call(
        mix_body,
        jax.ShapeDtypeStruct((tps, batch * IMG_R + 8, width), BF16),
        [VMEM] * 3,
    )(attended, output_weight, rel)
    parts = swap(parts, "tp")

    shape = jax.ShapeDtypeStruct((batch, img_rows, width), F32)
    out_img, new_cache, ratio = call(
        final_body,
        (shape, shape, jax.ShapeDtypeStruct((8, HD), F32)),
        [SMEM, VMEM, VMEM, VMEM, VMEM],
    )(refresh, parts, cache, img, modulation)
    return (out_img, new_cache, ratio[0, :batch])


def solution(mesh):
    finer = Mesh(mesh.devices.reshape(4, 8, 2, mesh.shape["tp"]), ("seq_0", "seq_1", "seq_2", "tp"))
    in_specs = (
        P(None, SEQ, "tp"),
        P(None, SEQ, "tp"),
        P(None, SEQ, "tp"),
        P(None, SEQ, "tp"),
        P(None, None, "tp"),
        P(SEQ, None, "tp"),
        P(None, "tp"),
        P("tp", None),
        P(),
        P(),
    )
    out_specs = (P(None, SEQ, "tp"), P(None, SEQ, "tp"), P())

    return jax.shard_map(local, mesh=finer, in_specs=in_specs, out_specs=out_specs, check_vma=False)
```

```python
import functools

import jax
import jax.numpy as jnp
from jax import lax
from jax.experimental import pallas as pl
from jax.experimental.pallas import tpu as pltpu
from jax.sharding import Mesh
from jax.sharding import PartitionSpec as P


HD = 128
SEQ = ("seq_0", "seq_1", "seq_2")
EPS = 0.1
NEG = -1e30
F32 = jnp.float32
BF16 = jnp.bfloat16

IMG_R = 32
TXT_R = 4
ROWS = 40
REL_ROW = IMG_R + TXT_R

VMEM = pl.BlockSpec(memory_space=pltpu.VMEM)
SMEM = pl.BlockSpec(memory_space=pltpu.SMEM)


def call(body, out_shape, in_specs, mebibytes, outs=None):
    outs = outs or jax.tree.map(lambda _: VMEM, out_shape)
    return pl.pallas_call(
        body,
        out_shape=out_shape,
        in_specs=in_specs,
        out_specs=outs,
        compiler_params=pltpu.CompilerParams(vmem_limit_bytes=mebibytes << 20),
    )


def swap(value, axis):
    return lax.all_to_all(value, axis, 0, 0, tiled=True)


def spread_copies(value, count):
    return jnp.broadcast_to(value[None], (count,) + value.shape)


def split_three(value):
    high = value.astype(BF16).astype(F32)
    rest = value - high
    middle = rest.astype(BF16).astype(F32)
    return high, middle, rest - middle


def norm_body(tp_ref, x_ref, prev_ref, mod_ref, rel_ref):
    groups, rows, width = x_ref.shape
    batch = rows // ROWS
    features = groups * width
    sums = jnp.zeros((rows, 1), F32)
    for g in range(groups):
        sums = sums + jnp.sum(x_ref[g].astype(F32), axis=1, keepdims=True)
    center = sums / features
    squares = jnp.zeros((rows, 1), F32)
    for g in range(groups):
        squares = squares + jnp.sum(
            jnp.square(x_ref[g].astype(F32) - center), axis=1, keepdims=True
        )
    inv = lax.rsqrt(squares / features + EPS)
    for g in range(groups):
        normed = (x_ref[g].astype(F32) - center) * inv
        values = x_ref[g].astype(F32)
        parts = []
        for b in range(batch):
            at = b * ROWS
            shift = values[at + REL_ROW : at + REL_ROW + 1]
            scale = values[at + REL_ROW + 1 : at + REL_ROW + 2]
            parts.append(normed[at : at + ROWS] * (1.0 + scale) + shift)
        mod_ref[g] = jnp.concatenate(parts, axis=0).astype(BF16)
    own = mod_ref[tp_ref[0]].astype(F32)
    lane = lax.broadcasted_iota(jnp.int32, (8, 128), 1)
    rel = jnp.zeros((8, 128), F32)
    for b in range(batch):
        previous = prev_ref[b].astype(F32)
        gap = jnp.abs(own[b * ROWS : b * ROWS + IMG_R] - previous)
        rel = jnp.where(lane == b, jnp.sum(gap), rel)
        rel = jnp.where(lane == batch + b, jnp.sum(jnp.abs(previous)), rel)
    rel_ref[...] = rel


def project_body(core_ref, mod_ref, own_ref, other_ref, gain_ref, rel_ref, out_ref):
    @pl.when(core_ref[0] == 0)
    def _():
        project(mod_ref, (own_ref, other_ref), gain_ref, rel_ref, out_ref)

    @pl.when(core_ref[0] == 1)
    def _():
        project(mod_ref, (other_ref, own_ref), gain_ref, rel_ref, out_ref)


def project(mod_ref, w_refs, gain_ref, rel_ref, out_ref):
    groups, rows, width = mod_ref.shape
    cores = len(w_refs)
    _, ys, kinds, deep, columns = w_refs[0].shape
    batch = rows // ROWS
    heads = columns // HD
    high, middle, low = split_three(rel_ref[0:1, :])
    row = lax.broadcasted_iota(jnp.int32, (ROWS, HD), 0)
    per_group = width // (cores * deep)
    for kind in range(kinds):
        total = jnp.zeros((rows, columns), F32)
        for g in range(groups):
            pieces = []
            for step in range(per_group):
                flat = g * per_group + step
                for core in range(cores):
                    pieces.append(w_refs[core][flat // ys, flat % ys, kind])
            total = total + jnp.dot(
                mod_ref[g], jnp.concatenate(pieces, axis=0), preferred_element_type=F32
            )
        for h in range(heads):
            part = total[:, h * HD : (h + 1) * HD]
            if kind < 2:
                mean = jnp.mean(jnp.square(part), axis=1, keepdims=True)
                part = part * lax.rsqrt(mean + EPS) * gain_ref[kind : kind + 1, h * HD : (h + 1) * HD]
            for b in range(batch):
                block = part[b * ROWS : (b + 1) * ROWS]
                if kind == 1:
                    block = jnp.where(row == REL_ROW, high, block)
                    block = jnp.where(row == REL_ROW + 1, middle, block)
                    block = jnp.where(row == REL_ROW + 2, low, block)
                out_ref[b * heads + h, :, kind * HD : (kind + 1) * HD] = block.astype(BF16)


def attend_body(limit_ref, core_ref, qkv_ref, own_ref, other_ref, out_ref, rel_ref):
    ys = qkv_ref.shape[0]
    xs = own_ref.shape[0]
    count = xs * ys * ROWS
    query = jnp.concatenate([qkv_ref[y, :IMG_R, :HD] for y in range(ys)], axis=0)
    index = lax.broadcasted_iota(jnp.int32, (1, count), 1)
    slot = index % ROWS
    block = index // ROWS
    down = lax.broadcasted_iota(jnp.int32, (ROWS, HD), 0)
    held = (down >= REL_ROW) & (down < REL_ROW + 3)
    rel = jnp.zeros((1, HD), F32)
    parts = []
    for ref, core in ((own_ref, core_ref[0]), (other_ref, 1 - core_ref[0])):
        pairs = ref[...].reshape(count, 2 * HD)
        scores = lax.dot_general(
            query, pairs[:, :HD], (((1,), (1,)), ((), ())), preferred_element_type=F32
        ) * (1.0 / HD**0.5)
        text = (block * 2 + core) * TXT_R + slot - IMG_R
        valid = (slot < IMG_R) | ((slot < IMG_R + TXT_R) & (text < limit_ref[0]))
        parts.append((jnp.where(valid, scores, NEG), valid, pairs[:, HD:]))
        for x in range(xs):
            for y in range(ys):
                held_rows = jnp.where(held, ref[x, y, :, :HD].astype(F32), 0.0)
                rel = rel + jnp.sum(held_rows, axis=0, keepdims=True)
    rel_ref[...] = jnp.broadcast_to(rel, (8, HD))
    top = functools.reduce(jnp.maximum, [jnp.max(p[0], axis=1, keepdims=True) for p in parts])
    total = jnp.zeros((query.shape[0], 1), F32)
    summed = jnp.zeros(query.shape, F32)
    for scores, valid, values in parts:
        weights = jnp.where(valid, jnp.exp(scores - top), 0.0)
        total = total + jnp.sum(weights, axis=1, keepdims=True)
        summed = summed + jnp.dot(weights.astype(BF16), values, preferred_element_type=F32)
    attended = (summed / total).astype(BF16)
    for y in range(ys):
        out_ref[y] = attended[y * IMG_R : (y + 1) * IMG_R]


def mix_body(att_ref, w_ref, rel_ref, out_ref):
    pairs = att_ref.shape[0]
    groups, _, width = out_ref.shape
    heads = w_ref.shape[0] // HD
    batch = pairs // heads
    rows = batch * IMG_R
    lefts = []
    for h in range(heads):
        lefts.append(jnp.concatenate([att_ref[b * heads + h] for b in range(batch)], axis=0))
    left = jnp.concatenate(lefts, axis=1)
    high, middle, low = split_three(rel_ref[0:1, :])
    row = lax.broadcasted_iota(jnp.int32, (8, HD), 0)
    tail = jnp.where(row == 0, high, jnp.where(row == 1, middle, jnp.where(row == 2, low, 0.0)))
    tail = jnp.concatenate([tail, jnp.zeros((8, width - HD), F32)], axis=1).astype(BF16)
    for g in range(groups):
        mixed = jnp.dot(left, w_ref[:, g * width : (g + 1) * width], preferred_element_type=F32)
        out_ref[g, :rows] = mixed.astype(BF16)
        out_ref[g, rows:] = tail


def final_body(flag_ref, part_ref, cache_ref, img_ref, mod_ref, out_ref, new_ref, rel_ref):
    groups = part_ref.shape[0]
    batch = img_ref.shape[0]
    rows = batch * IMG_R
    mixed = part_ref[0, :rows].astype(F32)
    rel = part_ref[0, rows:, :HD].astype(F32)
    for g in range(1, groups):
        mixed = mixed + part_ref[g, :rows].astype(F32)
        rel = rel + part_ref[g, rows:, :HD].astype(F32)
    for b in range(batch):
        gate = mod_ref[2, b : b + 1].astype(F32)
        resid = gate * mixed[b * IMG_R : (b + 1) * IMG_R]
        fresh = jnp.where(flag_ref[b] == 1, resid, cache_ref[b])
        new_ref[b] = fresh
        out_ref[b] = img_ref[b].astype(F32) + fresh
    sums = jnp.sum(rel, axis=0, keepdims=True)
    lane = lax.broadcasted_iota(jnp.int32, (1, HD), 1)
    for b in range(batch):
        numer = jnp.sum(jnp.where(lane == b, sums, 0.0))
        denom = jnp.sum(jnp.where(lane == batch + b, sums, 0.0))
        rel_ref[b] = numer / jnp.maximum(denom, 1.0)


def local(img, txt, prev_mod, cache, modulation, w_qkv, qk_gain, output_weight, text_len, refresh):
    batch, img_rows, width = img.shape
    xs, ys, _ = (lax.axis_size(a) for a in SEQ)
    tps = lax.axis_size("tp")
    kinds, columns = w_qkv.shape[1:]
    deep = w_qkv.shape[0]
    heads = columns // HD

    pads = jnp.zeros((batch, ROWS - img_rows - txt.shape[1] - 2, width), BF16)
    joined = jnp.concatenate(
        [img, txt, modulation[0][:, None], modulation[1][:, None], pads], axis=1
    ).reshape(batch * ROWS, width)
    wide = lax.all_gather(joined, "tp", axis=0, tiled=False)

    weight = w_qkv.transpose(1, 0, 2).reshape(kinds * deep, columns)
    weight = swap(spread_copies(weight, xs * ys), ("seq_0", "seq_1"))
    weight = weight.reshape(xs, ys, kinds, deep, columns)
    other = lax.ppermute(weight, "seq_2", [(0, 1), (1, 0)])

    tp_index = lax.axis_index("tp").astype(jnp.int32)[None]
    core_index = lax.axis_index("seq_2").astype(jnp.int32)[None]
    modded, rel = call(
        norm_body,
        (
            jax.ShapeDtypeStruct((tps, batch * ROWS, width), BF16),
            jax.ShapeDtypeStruct((8, 128), F32),
        ),
        [SMEM, VMEM, VMEM],
        12,
    )(tp_index, wide, prev_mod)

    pairs = call(
        project_body,
        jax.ShapeDtypeStruct((batch * heads, ROWS, kinds * HD), BF16),
        [SMEM] + [VMEM] * 5,
        16,
    )(core_index, modded, weight, other, qk_gain, rel)

    pairs = swap(pairs, "seq_1")
    gathered = swap(spread_copies(pairs[:, :, HD:], xs), "seq_0")
    partner = lax.ppermute(gathered, "seq_2", [(0, 1), (1, 0)])

    mine = lax.axis_index("seq_1") // heads
    limit = lax.dynamic_slice_in_dim(text_len, mine, 1)
    attended, rel = call(
        attend_body,
        (
            jax.ShapeDtypeStruct((ys, IMG_R, HD), BF16),
            jax.ShapeDtypeStruct((8, HD), F32),
        ),
        [SMEM, SMEM, VMEM, VMEM, VMEM],
        24,
    )(limit, core_index, pairs, gathered, partner)

    attended = swap(attended, "seq_1")
    parts = call(
        mix_body,
        jax.ShapeDtypeStruct((tps, batch * IMG_R + 8, width), BF16),
        [VMEM] * 3,
        12,
    )(attended, output_weight, rel)
    parts = swap(parts, "tp")

    shape = jax.ShapeDtypeStruct((batch, img_rows, width), F32)
    out_img, new_cache, ratio = call(
        final_body,
        (shape, shape, jax.ShapeDtypeStruct((batch,), F32)),
        [SMEM, VMEM, VMEM, VMEM, VMEM],
        8,
        (VMEM, VMEM, SMEM),
    )(refresh, parts, cache, img, modulation)
    return (out_img, new_cache, ratio)


def solution(mesh):
    finer = Mesh(mesh.devices.reshape(4, 8, 2, mesh.shape["tp"]), ("seq_0", "seq_1", "seq_2", "tp"))
    in_specs = (
        P(None, SEQ, "tp"),
        P(None, SEQ, "tp"),
        P(None, SEQ, "tp"),
        P(None, SEQ, "tp"),
        P(None, None, "tp"),
        P(SEQ, None, "tp"),
        P(None, "tp"),
        P("tp", None),
        P(),
        P(),
    )
    out_specs = (P(None, SEQ, "tp"), P(None, SEQ, "tp"), P())

    return jax.shard_map(local, mesh=finer, in_specs=in_specs, out_specs=out_specs, check_vma=False)
```

```python
import functools

import jax
import jax.numpy as jnp
from jax import lax
from jax.experimental import pallas as pl
from jax.experimental.pallas import tpu as pltpu
from jax.sharding import Mesh
from jax.sharding import PartitionSpec as P


HD = 128
SEQ = ("seq_0", "seq_1a", "seq_1b", "seq_2")
AXIS_Y = ("seq_1a", "seq_1b")
EPS = 0.1
NEG = -1e30
F32 = jnp.float32
BF16 = jnp.bfloat16

IMG_R = 32
TXT_R = 4
ROWS = 40
REL_ROW = IMG_R + TXT_R

VMEM = pl.BlockSpec(memory_space=pltpu.VMEM)
SMEM = pl.BlockSpec(memory_space=pltpu.SMEM)


def call(body, out_shape, in_specs, mebibytes, outs=None):
    outs = outs or jax.tree.map(lambda _: VMEM, out_shape)
    return pl.pallas_call(
        body,
        out_shape=out_shape,
        in_specs=in_specs,
        out_specs=outs,
        compiler_params=pltpu.CompilerParams(vmem_limit_bytes=mebibytes << 20),
    )


def swap(value, axis):
    return lax.all_to_all(value, axis, 0, 0, tiled=True)


def spread_copies(value, count):
    return jnp.broadcast_to(value[None], (count,) + value.shape)


def split_three(value):
    high = value.astype(BF16).astype(F32)
    rest = value - high
    middle = rest.astype(BF16).astype(F32)
    return high, middle, rest - middle


def norm_body(tp_ref, x_ref, prev_ref, mod_ref, rel_ref):
    groups, rows, width = x_ref.shape
    batch = rows // ROWS
    features = groups * width
    sums = jnp.zeros((rows, 1), F32)
    for g in range(groups):
        sums = sums + jnp.sum(x_ref[g].astype(F32), axis=1, keepdims=True)
    center = sums / features
    squares = jnp.zeros((rows, 1), F32)
    for g in range(groups):
        squares = squares + jnp.sum(
            jnp.square(x_ref[g].astype(F32) - center), axis=1, keepdims=True
        )
    inv = lax.rsqrt(squares / features + EPS)
    for g in range(groups):
        normed = (x_ref[g].astype(F32) - center) * inv
        values = x_ref[g].astype(F32)
        parts = []
        for b in range(batch):
            at = b * ROWS
            shift = values[at + REL_ROW : at + REL_ROW + 1]
            scale = values[at + REL_ROW + 1 : at + REL_ROW + 2]
            parts.append(normed[at : at + ROWS] * (1.0 + scale) + shift)
        mod_ref[g] = jnp.concatenate(parts, axis=0).astype(BF16)
    own = mod_ref[tp_ref[0]].astype(F32)
    lane = lax.broadcasted_iota(jnp.int32, (8, 128), 1)
    rel = jnp.zeros((8, 128), F32)
    for b in range(batch):
        previous = prev_ref[b].astype(F32)
        gap = jnp.abs(own[b * ROWS : b * ROWS + IMG_R] - previous)
        rel = jnp.where(lane == b, jnp.sum(gap), rel)
        rel = jnp.where(lane == batch + b, jnp.sum(jnp.abs(previous)), rel)
    rel_ref[...] = rel


def project_body(core_ref, mod_ref, own_ref, other_ref, gain_ref, rel_ref, out_ref):
    @pl.when(core_ref[0] == 0)
    def _():
        project(mod_ref, (own_ref, other_ref), gain_ref, rel_ref, out_ref)

    @pl.when(core_ref[0] == 1)
    def _():
        project(mod_ref, (other_ref, own_ref), gain_ref, rel_ref, out_ref)


def project(mod_ref, w_refs, gain_ref, rel_ref, out_ref):
    groups, rows, width = mod_ref.shape
    cores = len(w_refs)
    _, near, far, kinds, deep, columns = w_refs[0].shape
    ys = near * far
    batch = rows // ROWS
    heads = columns // HD
    high, middle, low = split_three(rel_ref[0:1, :])
    row = lax.broadcasted_iota(jnp.int32, (ROWS, HD), 0)
    per_group = width // (cores * deep)
    for kind in range(kinds):
        total = jnp.zeros((rows, columns), F32)
        for g in range(groups):
            pieces = []
            for step in range(per_group):
                flat = g * per_group + step
                for core in range(cores):
                    y = flat % ys
                    pieces.append(w_refs[core][flat // ys, y % near, y // near, kind])
            total = total + jnp.dot(
                mod_ref[g], jnp.concatenate(pieces, axis=0), preferred_element_type=F32
            )
        for h in range(heads):
            part = total[:, h * HD : (h + 1) * HD]
            if kind < 2:
                mean = jnp.mean(jnp.square(part), axis=1, keepdims=True)
                part = part * lax.rsqrt(mean + EPS) * gain_ref[kind : kind + 1, h * HD : (h + 1) * HD]
            for b in range(batch):
                block = part[b * ROWS : (b + 1) * ROWS]
                if kind == 1:
                    block = jnp.where(row == REL_ROW, high, block)
                    block = jnp.where(row == REL_ROW + 1, middle, block)
                    block = jnp.where(row == REL_ROW + 2, low, block)
                out_ref[b * heads + h, :, kind * HD : (kind + 1) * HD] = block.astype(BF16)


def attend_body(limit_ref, core_ref, qkv_ref, own_ref, other_ref, out_ref, rel_ref):
    ys = qkv_ref.shape[0]
    xs = own_ref.shape[0]
    count = xs * ys * ROWS
    query = jnp.concatenate([qkv_ref[y, :IMG_R, :HD] for y in range(ys)], axis=0)
    index = lax.broadcasted_iota(jnp.int32, (1, count), 1)
    slot = index % ROWS
    block = index // ROWS
    down = lax.broadcasted_iota(jnp.int32, (ROWS, HD), 0)
    held = (down >= REL_ROW) & (down < REL_ROW + 3)
    rel = jnp.zeros((1, HD), F32)
    parts = []
    for ref, core in ((own_ref, core_ref[0]), (other_ref, 1 - core_ref[0])):
        pairs = ref[...].reshape(count, 2 * HD)
        scores = lax.dot_general(
            query, pairs[:, :HD], (((1,), (1,)), ((), ())), preferred_element_type=F32
        ) * (1.0 / HD**0.5)
        text = (block * 2 + core) * TXT_R + slot - IMG_R
        valid = (slot < IMG_R) | ((slot < IMG_R + TXT_R) & (text < limit_ref[0]))
        parts.append((jnp.where(valid, scores, NEG), valid, pairs[:, HD:]))
        for x in range(xs):
            for y in range(ys):
                held_rows = jnp.where(held, ref[x, y, :, :HD].astype(F32), 0.0)
                rel = rel + jnp.sum(held_rows, axis=0, keepdims=True)
    rel_ref[...] = jnp.broadcast_to(rel, (8, HD))
    top = functools.reduce(jnp.maximum, [jnp.max(p[0], axis=1, keepdims=True) for p in parts])
    total = jnp.zeros((query.shape[0], 1), F32)
    summed = jnp.zeros(query.shape, F32)
    for scores, valid, values in parts:
        weights = jnp.where(valid, jnp.exp(scores - top), 0.0)
        total = total + jnp.sum(weights, axis=1, keepdims=True)
        summed = summed + jnp.dot(weights.astype(BF16), values, preferred_element_type=F32)
    attended = (summed / total).astype(BF16)
    for y in range(ys):
        out_ref[y] = attended[y * IMG_R : (y + 1) * IMG_R]


def mix_body(att_ref, w_ref, rel_ref, out_ref):
    pairs = att_ref.shape[0]
    groups, _, width = out_ref.shape
    heads = w_ref.shape[0] // HD
    batch = pairs // heads
    rows = batch * IMG_R
    lefts = []
    for h in range(heads):
        lefts.append(jnp.concatenate([att_ref[b * heads + h] for b in range(batch)], axis=0))
    left = jnp.concatenate(lefts, axis=1)
    high, middle, low = split_three(rel_ref[0:1, :])
    row = lax.broadcasted_iota(jnp.int32, (8, HD), 0)
    tail = jnp.where(row == 0, high, jnp.where(row == 1, middle, jnp.where(row == 2, low, 0.0)))
    tail = jnp.concatenate([tail, jnp.zeros((8, width - HD), F32)], axis=1).astype(BF16)
    for g in range(groups):
        mixed = jnp.dot(left, w_ref[:, g * width : (g + 1) * width], preferred_element_type=F32)
        out_ref[g, :rows] = mixed.astype(BF16)
        out_ref[g, rows:] = tail


def final_body(flag_ref, part_ref, cache_ref, img_ref, mod_ref, out_ref, new_ref, rel_ref):
    groups = part_ref.shape[0]
    batch = img_ref.shape[0]
    rows = batch * IMG_R
    mixed = part_ref[0, :rows].astype(F32)
    rel = part_ref[0, rows:, :HD].astype(F32)
    for g in range(1, groups):
        mixed = mixed + part_ref[g, :rows].astype(F32)
        rel = rel + part_ref[g, rows:, :HD].astype(F32)
    for b in range(batch):
        gate = mod_ref[2, b : b + 1].astype(F32)
        resid = gate * mixed[b * IMG_R : (b + 1) * IMG_R]
        fresh = jnp.where(flag_ref[b] == 1, resid, cache_ref[b])
        new_ref[b] = fresh
        out_ref[b] = img_ref[b].astype(F32) + fresh
    sums = jnp.sum(rel, axis=0, keepdims=True)
    lane = lax.broadcasted_iota(jnp.int32, (1, HD), 1)
    for b in range(batch):
        numer = jnp.sum(jnp.where(lane == b, sums, 0.0))
        denom = jnp.sum(jnp.where(lane == batch + b, sums, 0.0))
        rel_ref[b] = numer / jnp.maximum(denom, 1.0)


def local(img, txt, prev_mod, cache, modulation, w_qkv, qk_gain, output_weight, text_len, refresh):
    batch, img_rows, width = img.shape
    xs, far, near, _ = (lax.axis_size(a) for a in SEQ)
    ys = far * near
    tps = lax.axis_size("tp")
    kinds, columns = w_qkv.shape[1:]
    deep = w_qkv.shape[0]
    heads = columns // HD

    pads = jnp.zeros((batch, ROWS - img_rows - txt.shape[1] - 2, width), BF16)
    joined = jnp.concatenate(
        [img, txt, modulation[0][:, None], modulation[1][:, None], pads], axis=1
    ).reshape(batch * ROWS, width)
    wide = lax.all_gather(joined, "tp", axis=0, tiled=False)

    weight = w_qkv.transpose(1, 0, 2).reshape(kinds * deep, columns)
    weight = swap(spread_copies(weight, far), "seq_1a")
    weight = weight.reshape(far * kinds * deep, columns)
    weight = swap(spread_copies(weight, xs * near), ("seq_0", "seq_1b"))
    weight = weight.reshape(xs, near, far, kinds, deep, columns)
    other = lax.ppermute(weight, "seq_2", [(0, 1), (1, 0)])

    tp_index = lax.axis_index("tp").astype(jnp.int32)[None]
    core_index = lax.axis_index("seq_2").astype(jnp.int32)[None]
    modded, rel = call(
        norm_body,
        (
            jax.ShapeDtypeStruct((tps, batch * ROWS, width), BF16),
            jax.ShapeDtypeStruct((8, 128), F32),
        ),
        [SMEM, VMEM, VMEM],
        12,
    )(tp_index, wide, prev_mod)

    pairs = call(
        project_body,
        jax.ShapeDtypeStruct((batch * heads, ROWS, kinds * HD), BF16),
        [SMEM] + [VMEM] * 5,
        16,
    )(core_index, modded, weight, other, qk_gain, rel)

    pairs = swap(pairs, AXIS_Y)
    gathered = swap(spread_copies(pairs[:, :, HD:], xs), "seq_0")
    partner = lax.ppermute(gathered, "seq_2", [(0, 1), (1, 0)])

    mine = lax.axis_index(AXIS_Y) // heads
    limit = lax.dynamic_slice_in_dim(text_len, mine, 1)
    attended, rel = call(
        attend_body,
        (
            jax.ShapeDtypeStruct((ys, IMG_R, HD), BF16),
            jax.ShapeDtypeStruct((8, HD), F32),
        ),
        [SMEM, SMEM, VMEM, VMEM, VMEM],
        24,
    )(limit, core_index, pairs, gathered, partner)

    attended = swap(attended, AXIS_Y)
    parts = call(
        mix_body,
        jax.ShapeDtypeStruct((tps, batch * IMG_R + 8, width), BF16),
        [VMEM] * 3,
        12,
    )(attended, output_weight, rel)
    parts = swap(parts, "tp")

    shape = jax.ShapeDtypeStruct((batch, img_rows, width), F32)
    out_img, new_cache, ratio = call(
        final_body,
        (shape, shape, jax.ShapeDtypeStruct((batch,), F32)),
        [SMEM, VMEM, VMEM, VMEM, VMEM],
        8,
        (VMEM, VMEM, SMEM),
    )(refresh, parts, cache, img, modulation)
    return (out_img, new_cache, ratio)


def solution(mesh):
    finer = Mesh(mesh.devices.reshape(4, 4, 2, 2, mesh.shape["tp"]), SEQ + ("tp",))
    in_specs = (
        P(None, SEQ, "tp"),
        P(None, SEQ, "tp"),
        P(None, SEQ, "tp"),
        P(None, SEQ, "tp"),
        P(None, None, "tp"),
        P(SEQ, None, "tp"),
        P(None, "tp"),
        P("tp", None),
        P(),
        P(),
    )
    out_specs = (P(None, SEQ, "tp"), P(None, SEQ, "tp"), P())

    return jax.shard_map(local, mesh=finer, in_specs=in_specs, out_specs=out_specs, check_vma=False)
```

```python
import functools

import jax
import jax.numpy as jnp
from jax import lax
from jax.experimental import pallas as pl
from jax.experimental.pallas import tpu as pltpu
from jax.sharding import Mesh
from jax.sharding import PartitionSpec as P


HD = 128
SEQ = ("seq_0", "seq_1a", "seq_1b", "seq_2")
AXIS_Y = ("seq_1a", "seq_1b")
EPS = 0.1
NEG = -1e30
F32 = jnp.float32
BF16 = jnp.bfloat16

IMG_R = 32
TXT_R = 4
ROWS = 40
REL_ROW = IMG_R + TXT_R

VMEM = pl.BlockSpec(memory_space=pltpu.VMEM)
SMEM = pl.BlockSpec(memory_space=pltpu.SMEM)


def call(body, out_shape, in_specs, mebibytes, outs=None):
    outs = outs or jax.tree.map(lambda _: VMEM, out_shape)
    return pl.pallas_call(
        body,
        out_shape=out_shape,
        in_specs=in_specs,
        out_specs=outs,
        compiler_params=pltpu.CompilerParams(vmem_limit_bytes=mebibytes << 20),
    )


def swap(value, axis):
    return lax.all_to_all(value, axis, 0, 0, tiled=True)


def spread_copies(value, count):
    return jnp.broadcast_to(value[None], (count,) + value.shape)


def split_three(value):
    high = value.astype(BF16).astype(F32)
    rest = value - high
    middle = rest.astype(BF16).astype(F32)
    return high, middle, rest - middle


def join_body(img_ref, txt_ref, mod_ref, out_ref):
    batch, _, width = img_ref.shape
    for b in range(batch):
        at = b * ROWS
        tail = [txt_ref[b], mod_ref[0, b : b + 1], mod_ref[1, b : b + 1]]
        tail = [t.astype(F32) for t in tail] + [jnp.zeros((ROWS - REL_ROW - 2, width), F32)]
        out_ref[at : at + IMG_R] = img_ref[b]
        out_ref[at + IMG_R : at + ROWS] = jnp.concatenate(tail, axis=0).astype(BF16)


def norm_body(tp_ref, x_ref, prev_ref, mod_ref, rel_ref):
    groups, rows, width = x_ref.shape
    batch = rows // ROWS
    features = groups * width
    sums = jnp.zeros((rows, 1), F32)
    for g in range(groups):
        sums = sums + jnp.sum(x_ref[g].astype(F32), axis=1, keepdims=True)
    center = sums / features
    squares = jnp.zeros((rows, 1), F32)
    for g in range(groups):
        squares = squares + jnp.sum(
            jnp.square(x_ref[g].astype(F32) - center), axis=1, keepdims=True
        )
    inv = lax.rsqrt(squares / features + EPS)
    for g in range(groups):
        normed = (x_ref[g].astype(F32) - center) * inv
        values = x_ref[g].astype(F32)
        parts = []
        for b in range(batch):
            at = b * ROWS
            shift = values[at + REL_ROW : at + REL_ROW + 1]
            scale = values[at + REL_ROW + 1 : at + REL_ROW + 2]
            parts.append(normed[at : at + ROWS] * (1.0 + scale) + shift)
        mod_ref[g] = jnp.concatenate(parts, axis=0).astype(BF16)
    own = mod_ref[tp_ref[0]].astype(F32)
    lane = lax.broadcasted_iota(jnp.int32, (8, 128), 1)
    rel = jnp.zeros((8, 128), F32)
    for b in range(batch):
        previous = prev_ref[b].astype(F32)
        gap = jnp.abs(own[b * ROWS : b * ROWS + IMG_R] - previous)
        rel = jnp.where(lane == b, jnp.sum(gap), rel)
        rel = jnp.where(lane == batch + b, jnp.sum(jnp.abs(previous)), rel)
    rel_ref[...] = rel


def project_body(core_ref, mod_ref, own_ref, other_ref, gain_ref, rel_ref, out_ref):
    @pl.when(core_ref[0] == 0)
    def _():
        project(mod_ref, (own_ref, other_ref), gain_ref, rel_ref, out_ref)

    @pl.when(core_ref[0] == 1)
    def _():
        project(mod_ref, (other_ref, own_ref), gain_ref, rel_ref, out_ref)


def project(mod_ref, w_refs, gain_ref, rel_ref, out_ref):
    groups, rows, width = mod_ref.shape
    cores = len(w_refs)
    _, near, far, kinds, deep, columns = w_refs[0].shape
    ys = near * far
    batch = rows // ROWS
    heads = columns // HD
    high, middle, low = split_three(rel_ref[0:1, :])
    row = lax.broadcasted_iota(jnp.int32, (ROWS, HD), 0)
    per_group = width // (cores * deep)
    for kind in range(kinds):
        total = jnp.zeros((rows, columns), F32)
        for g in range(groups):
            pieces = []
            for step in range(per_group):
                flat = g * per_group + step
                for core in range(cores):
                    y = flat % ys
                    pieces.append(w_refs[core][flat // ys, y % near, y // near, kind])
            total = total + jnp.dot(
                mod_ref[g], jnp.concatenate(pieces, axis=0), preferred_element_type=F32
            )
        for h in range(heads):
            part = total[:, h * HD : (h + 1) * HD]
            if kind < 2:
                mean = jnp.mean(jnp.square(part), axis=1, keepdims=True)
                part = part * lax.rsqrt(mean + EPS) * gain_ref[kind : kind + 1, h * HD : (h + 1) * HD]
            for b in range(batch):
                block = part[b * ROWS : (b + 1) * ROWS]
                if kind == 1:
                    block = jnp.where(row == REL_ROW, high, block)
                    block = jnp.where(row == REL_ROW + 1, middle, block)
                    block = jnp.where(row == REL_ROW + 2, low, block)
                out_ref[b * heads + h, :, kind * HD : (kind + 1) * HD] = block.astype(BF16)


def attend_body(limit_ref, flag_ref, core_ref, qkv_ref, own_ref, other_ref, out_ref):
    ys = qkv_ref.shape[0]
    xs = own_ref.shape[0]
    count = xs * ys * ROWS
    query = jnp.concatenate([qkv_ref[y, :IMG_R, :HD] for y in range(ys)], axis=0)
    index = lax.broadcasted_iota(jnp.int32, (1, count), 1)
    slot = index % ROWS
    block = index // ROWS
    down = lax.broadcasted_iota(jnp.int32, (ROWS, HD), 0)
    held = (down >= REL_ROW) & (down < REL_ROW + 3)
    rel = jnp.zeros((1, HD), F32)
    parts = []
    for ref, core in ((own_ref, core_ref[0]), (other_ref, 1 - core_ref[0])):
        pairs = ref[...].reshape(count, 2 * HD)
        scores = lax.dot_general(
            query, pairs[:, :HD], (((1,), (1,)), ((), ())), preferred_element_type=F32
        ) * (1.0 / HD**0.5)
        text = (block * 2 + core) * TXT_R + slot - IMG_R
        valid = (slot < IMG_R) | ((slot < IMG_R + TXT_R) & (text < limit_ref[0]))
        parts.append((jnp.where(valid, scores, NEG), valid, pairs[:, HD:]))
        for x in range(xs):
            for y in range(ys):
                held_rows = jnp.where(held, ref[x, y, :, :HD].astype(F32), 0.0)
                rel = rel + jnp.sum(held_rows, axis=0, keepdims=True)
    top = functools.reduce(jnp.maximum, [jnp.max(p[0], axis=1, keepdims=True) for p in parts])
    total = jnp.zeros((query.shape[0], 1), F32)
    summed = jnp.zeros(query.shape, F32)
    for scores, valid, values in parts:
        weights = jnp.where(valid, jnp.exp(scores - top), 0.0)
        total = total + jnp.sum(weights, axis=1, keepdims=True)
        summed = summed + jnp.dot(weights.astype(BF16), values, preferred_element_type=F32)
    attended = summed / total
    high, middle, low = split_three(rel)
    row = lax.broadcasted_iota(jnp.int32, (IMG_R, HD), 0)
    sums = jnp.where(row == 0, high, jnp.where(row == 1, middle, jnp.where(row == 2, low, 0.0)))
    for y in range(ys):
        block = attended[y * IMG_R : (y + 1) * IMG_R]
        block = jnp.where(flag_ref[0] == 1, block, sums).astype(BF16)
        for z in range(out_ref.shape[1]):
            out_ref[y, z] = block


def deal_body(tp_ref, w_ref, *out_refs):
    count = len(out_refs)
    width = out_refs[0].shape[1]
    for k, out_ref in enumerate(out_refs):
        target = lax.rem(tp_ref[0] + k, count)
        out_ref[...] = w_ref[:, pl.ds(pl.multiple_of(target * width, HD), width)]


def final_body(tp_ref, flag_ref, att_ref, *refs):
    *w_refs, cache_ref, img_ref, mod_ref, out_ref, new_ref, rel_ref = refs
    groups = len(w_refs)
    batch = img_ref.shape[0]
    heads = att_ref.shape[0] // batch
    rows = batch * IMG_R
    mixed = jnp.zeros((rows, img_ref.shape[2]), F32)
    for k, w_ref in enumerate(w_refs):
        source = lax.rem(tp_ref[0] + groups - k, groups)
        lefts = []
        for h in range(heads):
            lefts.append(
                jnp.concatenate([att_ref[b * heads + h, source] for b in range(batch)], axis=0)
            )
        mixed = mixed + jnp.dot(
            jnp.concatenate(lefts, axis=1), w_ref[...], preferred_element_type=F32
        )
    idle = jnp.int32(0)
    for b in range(batch - 1, -1, -1):
        idle = jnp.where(flag_ref[b] == 1, idle, b)
        gate = mod_ref[2, b : b + 1].astype(F32)
        resid = gate * mixed[b * IMG_R : (b + 1) * IMG_R]
        fresh = jnp.where(flag_ref[b] == 1, resid, cache_ref[b])
        new_ref[b] = fresh
        out_ref[b] = img_ref[b].astype(F32) + fresh
    sums = jnp.zeros((IMG_R, HD), F32)
    for z in range(groups):
        sums = sums + att_ref[idle * heads, z].astype(F32)
    sums = jnp.sum(sums, axis=0, keepdims=True)
    lane = lax.broadcasted_iota(jnp.int32, (1, HD), 1)
    for b in range(batch):
        numer = jnp.sum(jnp.where(lane == b, sums, 0.0))
        denom = jnp.sum(jnp.where(lane == batch + b, sums, 0.0))
        rel_ref[b] = numer / jnp.maximum(denom, 1.0)


def local(img, txt, prev_mod, cache, modulation, w_qkv, qk_gain, output_weight, text_len, refresh):
    batch, img_rows, width = img.shape
    xs, far, near, _ = (lax.axis_size(a) for a in SEQ)
    ys = far * near
    tps = lax.axis_size("tp")
    kinds, columns = w_qkv.shape[1:]
    deep = w_qkv.shape[0]
    heads = columns // HD

    tp_index = lax.axis_index("tp").astype(jnp.int32)[None]
    blocks = list(
        call(
            deal_body,
            (jax.ShapeDtypeStruct((output_weight.shape[0], width), BF16),) * tps,
            [SMEM, VMEM],
            12,
        )(tp_index, output_weight)
    )
    for k in range(1, tps):
        blocks[k] = lax.ppermute(blocks[k], "tp", [(i, (i + k) % tps) for i in range(tps)])

    joined = call(
        join_body,
        jax.ShapeDtypeStruct((batch * ROWS, width), BF16),
        [VMEM] * 3,
        4,
    )(img, txt, modulation)
    wide = lax.all_gather(joined, "tp", axis=0, tiled=False)

    weight = w_qkv.transpose(1, 0, 2).reshape(kinds * deep, columns)
    weight = swap(spread_copies(weight, far), "seq_1a")
    weight = weight.reshape(far * kinds * deep, columns)
    weight = swap(spread_copies(weight, xs * near), ("seq_0", "seq_1b"))
    weight = weight.reshape(xs, near, far, kinds, deep, columns)
    other = lax.ppermute(weight, "seq_2", [(0, 1), (1, 0)])

    core_index = lax.axis_index("seq_2").astype(jnp.int32)[None]
    modded, rel = call(
        norm_body,
        (
            jax.ShapeDtypeStruct((tps, batch * ROWS, width), BF16),
            jax.ShapeDtypeStruct((8, 128), F32),
        ),
        [SMEM, VMEM, VMEM],
        12,
    )(tp_index, wide, prev_mod)

    pairs = call(
        project_body,
        jax.ShapeDtypeStruct((batch * heads, ROWS, kinds * HD), BF16),
        [SMEM] + [VMEM] * 5,
        16,
    )(core_index, modded, weight, other, qk_gain, rel)

    pairs = swap(pairs, AXIS_Y)
    gathered = swap(spread_copies(pairs[:, :, HD:], xs), "seq_0")
    partner = lax.ppermute(gathered, "seq_2", [(0, 1), (1, 0)])

    mine = lax.axis_index(AXIS_Y) // heads
    limit = lax.dynamic_slice_in_dim(text_len, mine, 1)
    flag = lax.dynamic_slice_in_dim(refresh, mine, 1)
    attended = call(
        attend_body,
        jax.ShapeDtypeStruct((ys, tps, IMG_R, HD), BF16),
        [SMEM, SMEM, SMEM, VMEM, VMEM, VMEM],
        24,
    )(limit, flag, core_index, pairs, gathered, partner)

    attended = swap(attended.reshape(ys * tps, IMG_R, HD), AXIS_Y + ("tp",))
    attended = attended.reshape(ys, tps, IMG_R, HD)

    shape = jax.ShapeDtypeStruct((batch, img_rows, width), F32)
    return call(
        final_body,
        (shape, shape, jax.ShapeDtypeStruct((batch,), F32)),
        [SMEM, SMEM] + [VMEM] * (tps + 4),
        12,
        (VMEM, VMEM, SMEM),
    )(tp_index, refresh, attended, *blocks, cache, img, modulation)


def solution(mesh):
    finer = Mesh(mesh.devices.reshape(4, 4, 2, 2, mesh.shape["tp"]), SEQ + ("tp",))
    in_specs = (
        P(None, SEQ, "tp"),
        P(None, SEQ, "tp"),
        P(None, SEQ, "tp"),
        P(None, SEQ, "tp"),
        P(None, None, "tp"),
        P(SEQ, None, "tp"),
        P(None, "tp"),
        P("tp", None),
        P(),
        P(),
    )
    out_specs = (P(None, SEQ, "tp"), P(None, SEQ, "tp"), P())

    return jax.shard_map(local, mesh=finer, in_specs=in_specs, out_specs=out_specs, check_vma=False)
```

```python
import functools

import jax
import jax.numpy as jnp
from jax import lax
from jax.experimental import pallas as pl
from jax.experimental.pallas import tpu as pltpu
from jax.sharding import Mesh
from jax.sharding import PartitionSpec as P


X, FAR, NEAR, CORE, TP = "seq_0", "seq_1a", "seq_1b", "seq_2", "tp"
SEQ = (X, FAR, NEAR, CORE)
HD = 128
EPS = 0.1
NEG = -1e30
F32 = jnp.float32
BF16 = jnp.bfloat16

VMEM = pl.BlockSpec(memory_space=pltpu.VMEM)
SMEM = pl.BlockSpec(memory_space=pltpu.SMEM)


def call(body, out_shape, in_specs, mebibytes, outs=None):
    outs = outs or jax.tree.map(lambda _: VMEM, out_shape)
    return pl.pallas_call(
        body,
        out_shape=out_shape,
        in_specs=in_specs,
        out_specs=outs,
        compiler_params=pltpu.CompilerParams(vmem_limit_bytes=mebibytes << 20),
    )


def shaped(*shape, dtype=BF16):
    return jax.ShapeDtypeStruct(shape, dtype)


def swap(value, axis):
    return lax.all_to_all(value, axis, 0, 0, tiled=True)


def split_three(value):
    high = value.astype(BF16).astype(F32)
    rest = value - high
    middle = rest.astype(BF16).astype(F32)
    return high, middle, rest - middle


def stacked_parts(value, rows):
    row = lax.broadcasted_iota(jnp.int32, (rows, value.shape[1]), 0)
    high, middle, low = split_three(value)
    return jnp.where(row == 0, high, jnp.where(row == 1, middle, jnp.where(row == 2, low, 0.0)))


def pack_body(w_ref, img_ref, prev_ref, txt_ref, out_ref):
    kinds, deep, columns = w_ref.shape
    batch, img_rows, width = img_ref.shape
    cores = columns // HD
    img_half = img_rows // cores
    txt_half = txt_ref.shape[1] // cores
    for b in range(batch):
        for c in range(cores):
            to = b * cores + c
            for kind in range(kinds):
                out_ref[to, :deep, kind * HD : (kind + 1) * HD] = w_ref[
                    kind, :, c * HD : (c + 1) * HD
                ]
            at = deep
            for ref in (img_ref, prev_ref):
                out_ref[to, at : at + img_half] = ref[b, c * img_half : (c + 1) * img_half]
                at += img_half
            text = txt_ref[b].astype(F32)[c * txt_half : (c + 1) * txt_half]
            text = jnp.concatenate([text, jnp.zeros((8 - txt_half, width), F32)], axis=0)
            out_ref[to, at : at + 8] = text.astype(BF16)


def spread_body(got_ref, out_ref):
    copies = out_ref.shape[0]
    sources = got_ref.shape[0]
    deep = out_ref.shape[1] // sources
    for copy in range(copies):
        for source in range(sources):
            out_ref[copy, source * deep : (source + 1) * deep] = got_ref[source, :deep]


def join_body(deep, img_half, txt_half, far_ref, got_ref, mod_ref, out_ref):
    sources = got_ref.shape[0]
    width = got_ref.shape[2]
    for source in range(sources):
        out_ref[source * img_half : (source + 1) * img_half] = got_ref[
            source, deep : deep + img_half
        ]
    at = deep + 2 * img_half
    texts = [got_ref[source, at : at + 8].astype(F32)[:txt_half] for source in range(sources)]
    vectors = []
    for which in range(2):
        chosen = mod_ref[which, 0:1].astype(F32)
        for b in range(1, mod_ref.shape[1]):
            chosen = jnp.where(far_ref[0] == b, mod_ref[which, b : b + 1].astype(F32), chosen)
        vectors.append(chosen)
    tail = jnp.concatenate(texts + vectors + [jnp.zeros((6, width), F32)], axis=0)
    out_ref[sources * img_half :] = tail.astype(BF16)


def norm_body(deep, place_ref, x_ref, got_ref, mod_ref):
    groups, rows, width = x_ref.shape
    sources = got_ref.shape[0]
    vectors = rows - 8
    features = groups * width
    sums = jnp.zeros((rows, 1), F32)
    for g in range(groups):
        sums = sums + jnp.sum(x_ref[g].astype(F32), axis=1, keepdims=True)
    center = sums / features
    squares = jnp.zeros((rows, 1), F32)
    for g in range(groups):
        squares = squares + jnp.sum(
            jnp.square(x_ref[g].astype(F32) - center), axis=1, keepdims=True
        )
    inv = lax.rsqrt(squares / features + EPS)
    for g in range(groups):
        values = x_ref[g].astype(F32)
        shift = values[vectors : vectors + 1]
        scale = values[vectors + 1 : vectors + 2]
        mod_ref[g] = ((values - center) * inv * (1.0 + scale) + shift).astype(BF16)
    far = place_ref[0]
    own = mod_ref.at[place_ref[1]]
    img_half = (got_ref.shape[1] - deep - 8) // 2
    numer = jnp.zeros((img_half, width), F32)
    denom = jnp.zeros((img_half, width), F32)
    for source in range(sources):
        at = deep + img_half
        previous = got_ref[source, at : at + img_half].astype(F32)
        current = own[source * img_half : (source + 1) * img_half].astype(F32)
        numer = numer + jnp.abs(current - previous)
        denom = denom + jnp.abs(previous)
    lane = lax.broadcasted_iota(jnp.int32, (1, width), 1)
    line = jnp.where(lane == far, jnp.sum(numer), 0.0)
    line = jnp.where(lane == 4 + far, jnp.sum(denom), line)
    mod_ref[0, vectors:] = stacked_parts(line, 8).astype(BF16)


def project_body(core_ref, own_ref, other_ref, w_ref, gain_ref, query_ref, pair_ref):
    groups, rows, width = own_ref.shape
    _, sources, deep, columns = w_ref.shape
    near = cores = 2
    ys = near * sources // cores
    per_group = width // deep
    total = jnp.zeros((2 * rows, columns), F32)
    for g in range(groups):
        pieces = []
        for step in range(per_group):
            flat = g * per_group + step
            core = flat % cores
            y = flat // cores % ys
            x = flat // cores // ys
            pieces.append(w_ref[x * near + y % near, y // near * cores + core])
        left = jnp.concatenate([own_ref[g], other_ref[g]], axis=0)
        total = total + jnp.dot(
            left, jnp.concatenate(pieces, axis=0), preferred_element_type=F32
        )
    parts = []
    for kind in range(2):
        part = total[:, kind * HD : (kind + 1) * HD]
        gain = jnp.where(
            core_ref[0] == 0, gain_ref[kind : kind + 1, :HD], gain_ref[kind : kind + 1, HD:]
        )
        mean = jnp.mean(jnp.square(part), axis=1, keepdims=True)
        parts.append(part * lax.rsqrt(mean + EPS) * gain)
    query, keyed = parts
    valued = total[:, 2 * HD :].astype(BF16)
    img = query_ref.shape[1]
    for half, ref in enumerate((own_ref, other_ref)):
        at = half * rows
        query_ref[half] = query[at : at + img].astype(BF16)
        carried = ref[0, rows - 8 :, :HD]
        keys = keyed[at : at + rows - 8].astype(BF16)
        for copy in range(pair_ref.shape[0]):
            pair_ref[copy, half, : rows - 8, :HD] = keys
            pair_ref[copy, half, rows - 8 :, :HD] = carried
            pair_ref[copy, half, :, HD:] = valued[at : at + rows]


def attend_body(img_half, txt_half, limit_ref, place_ref, query_ref, pair_ref, out_ref):
    blocks, halves, rows, _ = pair_ref.shape
    sources = out_ref.shape[0]
    img = sources * img_half
    txt = sources * txt_half
    count = blocks * rows
    far, core = place_ref[0], place_ref[2]
    query = query_ref[...].reshape(2 * img, HD)
    index = lax.broadcasted_iota(jnp.int32, (1, count), 1)
    slot = index % rows
    block = index // rows
    source = (slot - img) // txt_half
    y = source // 2 * 2 + block % 2
    device = (block // 2 * 8 + y) * 2 + source % 2
    scores_of, valid_of = [], []
    rel = jnp.zeros((1, HD), F32)
    for half in range(halves):
        actual = jnp.where(half == 0, core, 1 - core)
        keys = pair_ref[:, half, :, :HD].reshape(count, HD)
        scores = lax.dot_general(
            query, keys, (((1,), (1,)), ((), ())), preferred_element_type=F32
        ) * (1.0 / HD**0.5)
        text = device * 4 + actual * txt_half + (slot - img) % txt_half
        valid = (slot < img) | ((slot < img + txt) & (text < limit_ref[far]))
        scores_of.append(jnp.where(valid, scores, NEG))
        valid_of.append(valid)
        for b in range(blocks):
            carried = pair_ref[b, half, rows - 8 :, :HD].astype(F32)
            rel = rel + jnp.sum(carried, axis=0, keepdims=True)
    top = functools.reduce(
        jnp.maximum, [jnp.max(s, axis=1, keepdims=True) for s in scores_of]
    )
    total = jnp.zeros((2 * img, 1), F32)
    summed = jnp.zeros((2 * img, HD), F32)
    for half in range(halves):
        weights = jnp.where(valid_of[half], jnp.exp(scores_of[half] - top), 0.0)
        total = total + jnp.sum(weights, axis=1, keepdims=True)
        values = pair_ref[:, half, :, HD:].reshape(count, HD)
        summed = summed + jnp.dot(weights.astype(BF16), values, preferred_element_type=F32)
    attended = (summed / total).astype(BF16)
    tail = stacked_parts(rel, 8).astype(BF16)
    for half in range(halves):
        actual = jnp.where(half == 0, core, 1 - core)
        at = pl.multiple_of(actual * img_half, img_half)
        for source in range(sources):
            start = half * img + source * img_half
            out_ref[source, pl.ds(at, img_half)] = attended[start : start + img_half]
    for source in range(sources):
        out_ref[source, 2 * img_half :] = tail


def slots_of(flag_ref, batch, count):
    order = [jnp.int32(0)] * count
    seen = jnp.int32(0)
    slot = []
    for b in range(batch):
        on = flag_ref[b] == 1
        slot.append(seen)
        for i in range(count):
            order[i] = jnp.where(on & (seen == i), jnp.int32(b), order[i])
        seen = seen + jnp.where(on, 1, 0)
    return order, slot


def mix_body(img_rows, flag_ref, att_ref, w_ref, out_ref):
    groups, rows, width = out_ref.shape
    heads = w_ref.shape[0] // HD
    batch = att_ref.shape[0] // heads
    slots = (rows - 8) // img_rows
    order, _ = slots_of(flag_ref, batch, slots)
    lefts = []
    for h in range(heads):
        lefts.append(
            jnp.concatenate([att_ref[order[i] * heads + h, :img_rows] for i in range(slots)], axis=0)
        )
    left = jnp.concatenate(lefts, axis=1)
    rel = jnp.zeros((8, HD), F32)
    for b in range(batch):
        rel = rel + att_ref[b * heads, img_rows:].astype(F32)
    tail = stacked_parts(jnp.sum(rel, axis=0, keepdims=True), 8)
    tail = jnp.concatenate([tail, jnp.zeros((8, width - HD), F32)], axis=1).astype(BF16)
    for g in range(groups):
        mixed = jnp.dot(left, w_ref[:, g * width : (g + 1) * width], preferred_element_type=F32)
        out_ref[g, : rows - 8] = mixed.astype(BF16)
        out_ref[g, rows - 8 :] = tail


def final_body(flag_ref, part_ref, cache_ref, img_ref, mod_ref, out_ref, new_ref, rel_ref, sum_ref):
    groups, rows, _ = part_ref.shape
    batch, img_rows, _ = img_ref.shape
    slots = (rows - 8) // img_rows
    mixed = part_ref[0].astype(F32)
    for g in range(1, groups):
        mixed = mixed + part_ref[g].astype(F32)
    sum_ref[...] = mixed
    _, slot = slots_of(flag_ref, batch, slots)
    for b in range(batch):
        gate = mod_ref[2, b : b + 1].astype(F32)
        at = pl.multiple_of(jnp.minimum(slot[b], slots - 1) * img_rows, img_rows)
        resid = gate * sum_ref[pl.ds(at, img_rows)]
        fresh = jnp.where(flag_ref[b] == 1, resid, cache_ref[b])
        new_ref[b] = fresh
        out_ref[b] = img_ref[b].astype(F32) + fresh
    sums = jnp.sum(mixed[rows - 8 :, :HD], axis=0, keepdims=True)
    lane = lax.broadcasted_iota(jnp.int32, (1, HD), 1)
    for b in range(batch):
        numer = jnp.sum(jnp.where(lane == b, sums, 0.0))
        denom = jnp.sum(jnp.where(lane == 4 + b, sums, 0.0))
        rel_ref[b] = numer / jnp.maximum(denom, 1.0)


def local(img, txt, prev_mod, cache, modulation, w_qkv, qk_gain, output_weight, text_len, refresh):
    batch, img_rows, width = img.shape
    xs, fars, nears, cores = (lax.axis_size(a) for a in SEQ)
    tps = lax.axis_size(TP)
    deep, kinds, _ = w_qkv.shape
    sources = fars * cores
    around = xs * nears
    img_half, txt_half = img_rows // cores, txt.shape[1] // cores
    rows = sources * (img_half + txt_half) + 8
    place = jnp.stack([lax.axis_index(a) for a in (FAR, TP, CORE)]).astype(jnp.int32)
    core_index = lax.axis_index(CORE).astype(jnp.int32)[None]
    far_index = lax.axis_index(FAR).astype(jnp.int32)[None]

    got = call(
        pack_body, shaped(sources, deep + 2 * img_half + 8, width), [VMEM] * 4, 8
    )(w_qkv.transpose(1, 0, 2), img, prev_mod, txt)
    got = swap(got, (FAR, CORE))
    weight = call(spread_body, shaped(around, sources * deep, kinds * HD), [VMEM], 8)(got)
    weight = swap(weight, (X, NEAR)).reshape(around, sources, deep, kinds * HD)

    joined = call(
        functools.partial(join_body, deep, img_half, txt_half),
        shaped(rows, width),
        [SMEM, VMEM, VMEM],
        8,
    )(far_index, got, modulation)
    wide = lax.all_gather(joined, TP, axis=0, tiled=False)
    own = call(
        functools.partial(norm_body, deep), shaped(tps, rows, width), [SMEM, VMEM, VMEM], 12
    )(place, wide, got)
    other = lax.ppermute(own, CORE, [(0, 1), (1, 0)])

    query, pairs = call(
        project_body,
        (shaped(2, sources * img_half, HD), shaped(around, 2, rows, 2 * HD)),
        [SMEM] + [VMEM] * 4,
        16,
    )(core_index, own, other, weight, qk_gain)
    pairs = swap(pairs, (X, NEAR))
    attended = call(
        functools.partial(attend_body, img_half, txt_half),
        shaped(sources, img_rows + 8, HD),
        [SMEM, SMEM, VMEM, VMEM],
        24,
    )(text_len, place, query, pairs)
    attended = swap(attended, (FAR, CORE))

    slots = batch - 1
    parts = call(
        functools.partial(mix_body, img_rows),
        shaped(tps, slots * img_rows + 8, width),
        [SMEM, VMEM, VMEM],
        12,
    )(refresh, attended, output_weight)
    parts = swap(parts, TP)

    whole = shaped(batch, img_rows, width, dtype=F32)
    return pl.pallas_call(
        final_body,
        out_shape=(whole, whole, shaped(batch, dtype=F32)),
        in_specs=[SMEM] + [VMEM] * 4,
        out_specs=(VMEM, VMEM, SMEM),
        scratch_shapes=[pltpu.VMEM((slots * img_rows + 8, width), F32)],
        compiler_params=pltpu.CompilerParams(vmem_limit_bytes=8 << 20),
    )(refresh, parts, cache, img, modulation)


def solution(mesh):
    finer = Mesh(mesh.devices.reshape(4, 4, 2, 2, mesh.shape["tp"]), SEQ + (TP,))
    in_specs = (
        P(None, SEQ, TP),
        P(None, SEQ, TP),
        P(None, SEQ, TP),
        P(None, SEQ, TP),
        P(None, None, TP),
        P(SEQ, None, TP),
        P(None, TP),
        P(TP, None),
        P(),
        P(),
    )
    out_specs = (P(None, SEQ, TP), P(None, SEQ, TP), P())

    return jax.shard_map(local, mesh=finer, in_specs=in_specs, out_specs=out_specs, check_vma=False)
```

```python
import functools

import jax
import jax.numpy as jnp
from jax import lax
from jax.experimental import pallas as pl
from jax.experimental.pallas import tpu as pltpu
from jax.sharding import Mesh
from jax.sharding import PartitionSpec as P


X, FAR, NEAR, CORE, TP = "seq_0", "seq_1a", "seq_1b", "seq_2", "tp"
SEQ = (X, FAR, NEAR, CORE)
HD = 128
EPS = 0.1
NEG = -1e30
F32 = jnp.float32
BF16 = jnp.bfloat16

VMEM = pl.BlockSpec(memory_space=pltpu.VMEM)
SMEM = pl.BlockSpec(memory_space=pltpu.SMEM)
HBM = pl.BlockSpec(memory_space=pltpu.HBM)


def call(body, out_shape, in_specs, mebibytes, outs=None, scratch=()):
    outs = outs or jax.tree.map(lambda _: VMEM, out_shape)
    return pl.pallas_call(
        body,
        out_shape=out_shape,
        in_specs=in_specs,
        out_specs=outs,
        scratch_shapes=scratch,
        compiler_params=pltpu.CompilerParams(vmem_limit_bytes=mebibytes << 20),
    )


def shaped(*shape, dtype=BF16):
    return jax.ShapeDtypeStruct(shape, dtype)


def swap(value, axis):
    return lax.all_to_all(value, axis, 0, 0, tiled=True)


def split_three(value):
    high = value.astype(BF16).astype(F32)
    rest = value - high
    middle = rest.astype(BF16).astype(F32)
    return high, middle, rest - middle


def stacked_parts(value, rows):
    row = lax.broadcasted_iota(jnp.int32, (rows, value.shape[1]), 0)
    high, middle, low = split_three(value)
    return jnp.where(row == 0, high, jnp.where(row == 1, middle, jnp.where(row == 2, low, 0.0)))


def pack_body(w_hbm, img_hbm, prev_hbm, txt_hbm, out_ref, w_ref, img_ref, prev_ref, txt_ref, sems):
    copies = [
        pltpu.make_async_copy(source, target, sems.at[i])
        for i, (source, target) in enumerate(
            ((w_hbm, w_ref), (img_hbm, img_ref), (prev_hbm, prev_ref), (txt_hbm, txt_ref))
        )
    ]
    for copy in copies:
        copy.start()
    for copy in copies:
        copy.wait()
    kinds, deep, columns = w_ref.shape
    batch, img_rows, width = img_ref.shape
    cores = columns // HD
    img_half = img_rows // cores
    txt_half = txt_ref.shape[1] // cores
    for b in range(batch):
        for c in range(cores):
            to = b * cores + c
            for kind in range(kinds):
                out_ref[to, :deep, kind * HD : (kind + 1) * HD] = w_ref[
                    kind, :, c * HD : (c + 1) * HD
                ]
            at = deep
            for ref in (img_ref, prev_ref):
                out_ref[to, at : at + img_half] = ref[b, c * img_half : (c + 1) * img_half]
                at += img_half
            text = txt_ref[b].astype(F32)[c * txt_half : (c + 1) * txt_half]
            text = jnp.concatenate([text, jnp.zeros((8 - txt_half, width), F32)], axis=0)
            out_ref[to, at : at + 8] = text.astype(BF16)


def spread_body(got_ref, out_hbm, sems):
    copies = []
    sources = got_ref.shape[0]
    deep = out_hbm.shape[1] // sources
    for copy in range(out_hbm.shape[0]):
        for source in range(sources):
            copies.append(
                pltpu.make_async_copy(
                    got_ref.at[source, pl.ds(0, deep)],
                    out_hbm.at[copy, pl.ds(source * deep, deep)],
                    sems.at[copy, source],
                )
            )
    for copy in copies:
        copy.start()
    for copy in copies:
        copy.wait()


def join_body(deep, img_half, txt_half, far_ref, got_ref, mod_ref, out_ref, prev_ref):
    sources = got_ref.shape[0]
    width = got_ref.shape[2]
    for source in range(sources):
        out_ref[source * img_half : (source + 1) * img_half] = got_ref[
            source, deep : deep + img_half
        ]
        prev_ref[source * img_half : (source + 1) * img_half] = got_ref[
            source, deep + img_half : deep + 2 * img_half
        ]
    at = deep + 2 * img_half
    texts = [got_ref[source, at : at + 8].astype(F32)[:txt_half] for source in range(sources)]
    vectors = []
    for which in range(2):
        chosen = mod_ref[which, 0:1].astype(F32)
        for b in range(1, mod_ref.shape[1]):
            chosen = jnp.where(far_ref[0] == b, mod_ref[which, b : b + 1].astype(F32), chosen)
        vectors.append(chosen)
    tail = jnp.concatenate(texts + vectors + [jnp.zeros((6, width), F32)], axis=0)
    out_ref[sources * img_half :] = tail.astype(BF16)


def norm_body(place_ref, x_ref, prev_ref, mod_ref):
    groups, rows, width = x_ref.shape
    vectors = rows - 8
    features = groups * width
    sums = jnp.zeros((rows, 1), F32)
    for g in range(groups):
        sums = sums + jnp.sum(x_ref[g].astype(F32), axis=1, keepdims=True)
    center = sums / features
    squares = jnp.zeros((rows, 1), F32)
    for g in range(groups):
        squares = squares + jnp.sum(
            jnp.square(x_ref[g].astype(F32) - center), axis=1, keepdims=True
        )
    inv = lax.rsqrt(squares / features + EPS)
    for g in range(groups):
        values = x_ref[g].astype(F32)
        shift = values[vectors : vectors + 1]
        scale = values[vectors + 1 : vectors + 2]
        mod_ref[g] = ((values - center) * inv * (1.0 + scale) + shift).astype(BF16)
    far = place_ref[0]
    own = mod_ref.at[place_ref[1]]
    previous = prev_ref[...].astype(F32)
    numer = jnp.abs(own[: prev_ref.shape[0]].astype(F32) - previous)
    denom = jnp.abs(previous)
    lane = lax.broadcasted_iota(jnp.int32, (1, width), 1)
    line = jnp.where(lane == far, jnp.sum(numer), 0.0)
    line = jnp.where(lane == 4 + far, jnp.sum(denom), line)
    mod_ref[0, vectors:] = stacked_parts(line, 8).astype(BF16)


def project_body(core_ref, own_ref, other_ref, w_ref, gain_ref, query_ref, pair_ref):
    groups, rows, width = own_ref.shape
    _, sources, deep, columns = w_ref.shape
    near = cores = 2
    ys = near * sources // cores
    per_group = width // deep
    total = jnp.zeros((2 * rows, columns), F32)
    for g in range(groups):
        pieces = []
        for step in range(per_group):
            flat = g * per_group + step
            core = flat % cores
            y = flat // cores % ys
            x = flat // cores // ys
            pieces.append(w_ref[x * near + y % near, y // near * cores + core])
        left = jnp.concatenate([own_ref[g], other_ref[g]], axis=0)
        total = total + jnp.dot(
            left, jnp.concatenate(pieces, axis=0), preferred_element_type=F32
        )
    parts = []
    for kind in range(2):
        part = total[:, kind * HD : (kind + 1) * HD]
        gain = jnp.where(
            core_ref[0] == 0, gain_ref[kind : kind + 1, :HD], gain_ref[kind : kind + 1, HD:]
        )
        mean = jnp.mean(jnp.square(part), axis=1, keepdims=True)
        parts.append(part * lax.rsqrt(mean + EPS) * gain)
    query, keyed = parts
    valued = total[:, 2 * HD :].astype(BF16)
    img = query_ref.shape[1]
    for half, ref in enumerate((own_ref, other_ref)):
        at = half * rows
        query_ref[half] = query[at : at + img].astype(BF16)
        carried = ref[0, rows - 8 :, :HD]
        keys = keyed[at : at + rows - 8].astype(BF16)
        for copy in range(pair_ref.shape[0]):
            pair_ref[copy, half, : rows - 8, :HD] = keys
            pair_ref[copy, half, rows - 8 :, :HD] = carried
            pair_ref[copy, half, :, HD:] = valued[at : at + rows]


def attend_body(img_half, txt_half, limit_ref, place_ref, query_ref, pair_ref, out_ref):
    blocks, halves, rows, _ = pair_ref.shape
    sources = out_ref.shape[0]
    img = sources * img_half
    txt = sources * txt_half
    count = blocks * rows
    far, core = place_ref[0], place_ref[2]
    query = query_ref[...].reshape(2 * img, HD)
    index = lax.broadcasted_iota(jnp.int32, (1, count), 1)
    slot = index % rows
    block = index // rows
    source = (slot - img) // txt_half
    y = source // 2 * 2 + block % 2
    device = (block // 2 * 8 + y) * 2 + source % 2
    scores_of, valid_of = [], []
    rel = jnp.zeros((1, HD), F32)
    for half in range(halves):
        actual = jnp.where(half == 0, core, 1 - core)
        keys = pair_ref[:, half, :, :HD].reshape(count, HD)
        scores = lax.dot_general(
            query, keys, (((1,), (1,)), ((), ())), preferred_element_type=F32
        ) * (1.0 / HD**0.5)
        text = device * 4 + actual * txt_half + (slot - img) % txt_half
        valid = (slot < img) | ((slot < img + txt) & (text < limit_ref[far]))
        scores_of.append(jnp.where(valid, scores, NEG))
        valid_of.append(valid)
        for b in range(blocks):
            carried = pair_ref[b, half, rows - 8 :, :HD].astype(F32)
            rel = rel + jnp.sum(carried, axis=0, keepdims=True)
    top = functools.reduce(
        jnp.maximum, [jnp.max(s, axis=1, keepdims=True) for s in scores_of]
    )
    total = jnp.zeros((2 * img, 1), F32)
    summed = jnp.zeros((2 * img, HD), F32)
    for half in range(halves):
        weights = jnp.where(valid_of[half], jnp.exp(scores_of[half] - top), 0.0)
        total = total + jnp.sum(weights, axis=1, keepdims=True)
        values = pair_ref[:, half, :, HD:].reshape(count, HD)
        summed = summed + jnp.dot(weights.astype(BF16), values, preferred_element_type=F32)
    attended = (summed / total).astype(BF16)
    tail = stacked_parts(rel, 8).astype(BF16)
    for half in range(halves):
        actual = jnp.where(half == 0, core, 1 - core)
        at = pl.multiple_of(actual * img_half, img_half)
        for source in range(sources):
            start = half * img + source * img_half
            out_ref[source, pl.ds(at, img_half)] = attended[start : start + img_half]
    for source in range(sources):
        out_ref[source, 2 * img_half :] = tail


def slots_of(flag_ref, batch, count):
    order = [jnp.int32(0)] * count
    seen = jnp.int32(0)
    slot = []
    for b in range(batch):
        on = flag_ref[b] == 1
        slot.append(seen)
        for i in range(count):
            order[i] = jnp.where(on & (seen == i), jnp.int32(b), order[i])
        seen = seen + jnp.where(on, 1, 0)
    return order, slot


def mix_body(img_rows, flag_ref, att_ref, w_ref, out_ref):
    groups, rows, width = out_ref.shape
    heads = w_ref.shape[0] // HD
    batch = att_ref.shape[0] // heads
    slots = (rows - 8) // img_rows
    order, _ = slots_of(flag_ref, batch, slots)
    lefts = []
    for h in range(heads):
        lefts.append(
            jnp.concatenate([att_ref[order[i] * heads + h, :img_rows] for i in range(slots)], axis=0)
        )
    left = jnp.concatenate(lefts, axis=1)
    rel = jnp.zeros((8, HD), F32)
    for b in range(batch):
        rel = rel + att_ref[b * heads, img_rows:].astype(F32)
    tail = stacked_parts(jnp.sum(rel, axis=0, keepdims=True), 8)
    tail = jnp.concatenate([tail, jnp.zeros((8, width - HD), F32)], axis=1).astype(BF16)
    for g in range(groups):
        mixed = jnp.dot(left, w_ref[:, g * width : (g + 1) * width], preferred_element_type=F32)
        out_ref[g, : rows - 8] = mixed.astype(BF16)
        out_ref[g, rows - 8 :] = tail


def final_body(flag_ref, part_ref, cache_ref, img_ref, mod_ref, out_ref, new_ref, rel_ref, sum_ref):
    groups, rows, _ = part_ref.shape
    batch, img_rows, _ = img_ref.shape
    slots = (rows - 8) // img_rows
    mixed = part_ref[0].astype(F32)
    for g in range(1, groups):
        mixed = mixed + part_ref[g].astype(F32)
    sum_ref[...] = mixed
    _, slot = slots_of(flag_ref, batch, slots)
    for b in range(batch):
        gate = mod_ref[2, b : b + 1].astype(F32)
        at = pl.multiple_of(jnp.minimum(slot[b], slots - 1) * img_rows, img_rows)
        resid = gate * sum_ref[pl.ds(at, img_rows)]
        fresh = jnp.where(flag_ref[b] == 1, resid, cache_ref[b])
        new_ref[b] = fresh
        out_ref[b] = img_ref[b].astype(F32) + fresh
    sums = jnp.sum(mixed[rows - 8 :, :HD], axis=0, keepdims=True)
    lane = lax.broadcasted_iota(jnp.int32, (1, HD), 1)
    for b in range(batch):
        numer = jnp.sum(jnp.where(lane == b, sums, 0.0))
        denom = jnp.sum(jnp.where(lane == 4 + b, sums, 0.0))
        rel_ref[b] = numer / jnp.maximum(denom, 1.0)


def local(img, txt, prev_mod, cache, modulation, w_qkv, qk_gain, output_weight, text_len, refresh):
    batch, img_rows, width = img.shape
    xs, fars, nears, cores = (lax.axis_size(a) for a in SEQ)
    tps = lax.axis_size(TP)
    deep, kinds, _ = w_qkv.shape
    sources = fars * cores
    around = xs * nears
    img_half, txt_half = img_rows // cores, txt.shape[1] // cores
    rows = sources * (img_half + txt_half) + 8
    place = jnp.stack([lax.axis_index(a) for a in (FAR, TP, CORE)]).astype(jnp.int32)
    core_index = lax.axis_index(CORE).astype(jnp.int32)[None]
    far_index = lax.axis_index(FAR).astype(jnp.int32)[None]

    arrays = (w_qkv.transpose(1, 0, 2), img, prev_mod, txt)
    got = call(
        pack_body,
        shaped(sources, deep + 2 * img_half + 8, width),
        [HBM] * 4,
        8,
        scratch=[pltpu.VMEM(a.shape, a.dtype) for a in arrays]
        + [pltpu.SemaphoreType.DMA((len(arrays),))],
    )(*(pltpu.with_memory_space_constraint(a, pltpu.HBM) for a in arrays))
    got = swap(got, (FAR, CORE))
    weight = call(
        spread_body,
        pltpu.HBM((around, sources * deep, kinds * HD), BF16),
        [VMEM],
        8,
        outs=HBM,
        scratch=[pltpu.SemaphoreType.DMA((around, sources))],
    )(got)
    weight = swap(weight, (X, NEAR)).reshape(around, sources, deep, kinds * HD)

    joined, previous = call(
        functools.partial(join_body, deep, img_half, txt_half),
        (shaped(rows, width), shaped(sources * img_half, width)),
        [SMEM, VMEM, VMEM],
        8,
    )(far_index, got, modulation)
    wide = lax.all_gather(joined, TP, axis=0, tiled=False)
    own = call(norm_body, shaped(tps, rows, width), [SMEM, VMEM, VMEM], 12)(place, wide, previous)
    other = lax.ppermute(own, CORE, [(0, 1), (1, 0)])

    query, pairs = call(
        project_body,
        (shaped(2, sources * img_half, HD), shaped(around, 2, rows, 2 * HD)),
        [SMEM] + [VMEM] * 4,
        16,
    )(core_index, own, other, weight, qk_gain)
    pairs = swap(pairs, (X, NEAR))
    attended = call(
        functools.partial(attend_body, img_half, txt_half),
        shaped(sources, img_rows + 8, HD),
        [SMEM, SMEM, VMEM, VMEM],
        24,
    )(text_len, place, query, pairs)
    attended = swap(attended, (FAR, CORE))

    slots = batch - 1
    parts = call(
        functools.partial(mix_body, img_rows),
        shaped(tps, slots * img_rows + 8, width),
        [SMEM, VMEM, VMEM],
        12,
    )(refresh, attended, output_weight)
    parts = swap(parts, TP)

    whole = shaped(batch, img_rows, width, dtype=F32)
    return pl.pallas_call(
        final_body,
        out_shape=(whole, whole, shaped(batch, dtype=F32)),
        in_specs=[SMEM] + [VMEM] * 4,
        out_specs=(VMEM, VMEM, SMEM),
        scratch_shapes=[pltpu.VMEM((slots * img_rows + 8, width), F32)],
        compiler_params=pltpu.CompilerParams(vmem_limit_bytes=8 << 20),
    )(refresh, parts, cache, img, modulation)


def solution(mesh):
    finer = Mesh(mesh.devices.reshape(4, 4, 2, 2, mesh.shape["tp"]), SEQ + (TP,))
    in_specs = (
        P(None, SEQ, TP),
        P(None, SEQ, TP),
        P(None, SEQ, TP),
        P(None, SEQ, TP),
        P(None, None, TP),
        P(SEQ, None, TP),
        P(None, TP),
        P(TP, None),
        P(),
        P(),
    )
    out_specs = (P(None, SEQ, TP), P(None, SEQ, TP), P())

    return jax.shard_map(local, mesh=finer, in_specs=in_specs, out_specs=out_specs, check_vma=False)
```

```python
import functools

import jax
import jax.numpy as jnp
from jax import lax
from jax.experimental import pallas as pl
from jax.experimental.pallas import tpu as pltpu
from jax.sharding import Mesh
from jax.sharding import PartitionSpec as P


X, FAR, NEAR, CORE, TP = "seq_0", "seq_1a", "seq_1b", "seq_2", "tp"
SEQ = (X, FAR, NEAR, CORE)
HD = 128
EPS = 0.1
NEG = -1e30
F32 = jnp.float32
BF16 = jnp.bfloat16

VMEM = pl.BlockSpec(memory_space=pltpu.VMEM)
SMEM = pl.BlockSpec(memory_space=pltpu.SMEM)
HBM = pl.BlockSpec(memory_space=pltpu.HBM)


def call(body, out_shape, in_specs, mebibytes, outs=None, scratch=()):
    outs = outs or jax.tree.map(lambda _: VMEM, out_shape)
    return pl.pallas_call(
        body,
        out_shape=out_shape,
        in_specs=in_specs,
        out_specs=outs,
        scratch_shapes=scratch,
        compiler_params=pltpu.CompilerParams(vmem_limit_bytes=mebibytes << 20),
    )


def shaped(*shape, dtype=BF16):
    return jax.ShapeDtypeStruct(shape, dtype)


def swap(value, axis):
    return lax.all_to_all(value, axis, 0, 0, tiled=True)


def split_three(value):
    high = value.astype(BF16).astype(F32)
    rest = value - high
    middle = rest.astype(BF16).astype(F32)
    return high, middle, rest - middle


def stacked_parts(value, rows):
    row = lax.broadcasted_iota(jnp.int32, (rows, value.shape[1]), 0)
    high, middle, low = split_three(value)
    return jnp.where(row == 0, high, jnp.where(row == 1, middle, jnp.where(row == 2, low, 0.0)))


def pack_body(
    w_hbm, img_hbm, prev_hbm, txt_hbm, out_hbm, w_ref, img_ref, prev_ref, txt_ref, out_ref, sems
):
    copies = [
        pltpu.make_async_copy(source, target, sems.at[i])
        for i, (source, target) in enumerate(
            ((w_hbm, w_ref), (img_hbm, img_ref), (prev_hbm, prev_ref), (txt_hbm, txt_ref))
        )
    ]
    for copy in copies:
        copy.start()
    for copy in copies:
        copy.wait()
    kinds, deep, columns = w_ref.shape
    batch, img_rows, width = img_ref.shape
    cores = columns // HD
    img_half = img_rows // cores
    txt_half = txt_ref.shape[1] // cores
    for b in range(batch):
        for c in range(cores):
            to = b * cores + c
            for kind in range(kinds):
                out_ref[to, :deep, kind * HD : (kind + 1) * HD] = w_ref[
                    kind, :, c * HD : (c + 1) * HD
                ]
            at = deep
            for ref in (img_ref, prev_ref):
                out_ref[to, at : at + img_half] = ref[b, c * img_half : (c + 1) * img_half]
                at += img_half
            text = txt_ref[b].astype(F32)[c * txt_half : (c + 1) * txt_half]
            text = jnp.concatenate([text, jnp.zeros((8 - txt_half, width), F32)], axis=0)
            out_ref[to, at : at + 8] = text.astype(BF16)
    whole = pltpu.make_async_copy(out_ref, out_hbm, sems.at[0])
    whole.start()
    whole.wait()


def spread_body(got_ref, out_hbm, block_ref, sems):
    sources = got_ref.shape[0]
    deep = block_ref.shape[0] // sources
    for source in range(sources):
        block_ref[source * deep : (source + 1) * deep] = got_ref[source, :deep]
    copies = [
        pltpu.make_async_copy(block_ref, out_hbm.at[copy], sems.at[copy])
        for copy in range(out_hbm.shape[0])
    ]
    for copy in copies:
        copy.start()
    for copy in copies:
        copy.wait()


def deal_body(tp_ref, w_hbm, *refs):
    *out_refs, sems = refs
    width = out_refs[0].shape[1]
    copies = []
    for k, out_ref in enumerate(out_refs):
        target = lax.rem(tp_ref[0] + k, len(out_refs))
        columns = pl.ds(pl.multiple_of(target * width, HD), width)
        copies.append(pltpu.make_async_copy(w_hbm.at[:, columns], out_ref, sems.at[k]))
    for copy in copies:
        copy.start()
    for copy in copies:
        copy.wait()


def join_body(deep, img_half, txt_half, far_ref, got_ref, mod_ref, out_ref, prev_ref):
    sources = got_ref.shape[0]
    width = got_ref.shape[2]
    for source in range(sources):
        out_ref[source * img_half : (source + 1) * img_half] = got_ref[
            source, deep : deep + img_half
        ]
        prev_ref[source * img_half : (source + 1) * img_half] = got_ref[
            source, deep + img_half : deep + 2 * img_half
        ]
    at = deep + 2 * img_half
    texts = [got_ref[source, at : at + 8].astype(F32)[:txt_half] for source in range(sources)]
    vectors = []
    for which in range(2):
        chosen = mod_ref[which, 0:1].astype(F32)
        for b in range(1, mod_ref.shape[1]):
            chosen = jnp.where(far_ref[0] == b, mod_ref[which, b : b + 1].astype(F32), chosen)
        vectors.append(chosen)
    tail = jnp.concatenate(texts + vectors + [jnp.zeros((6, width), F32)], axis=0)
    out_ref[sources * img_half :] = tail.astype(BF16)


def norm_body(place_ref, x_ref, prev_ref, mod_ref):
    groups, rows, width = x_ref.shape
    vectors = rows - 8
    features = groups * width
    sums = jnp.zeros((rows, 1), F32)
    for g in range(groups):
        sums = sums + jnp.sum(x_ref[g].astype(F32), axis=1, keepdims=True)
    center = sums / features
    squares = jnp.zeros((rows, 1), F32)
    for g in range(groups):
        squares = squares + jnp.sum(
            jnp.square(x_ref[g].astype(F32) - center), axis=1, keepdims=True
        )
    inv = lax.rsqrt(squares / features + EPS)
    for g in range(groups):
        values = x_ref[g].astype(F32)
        shift = values[vectors : vectors + 1]
        scale = values[vectors + 1 : vectors + 2]
        mod_ref[g] = ((values - center) * inv * (1.0 + scale) + shift).astype(BF16)
    far = place_ref[0]
    own = mod_ref.at[place_ref[1]]
    previous = prev_ref[...].astype(F32)
    numer = jnp.abs(own[: prev_ref.shape[0]].astype(F32) - previous)
    denom = jnp.abs(previous)
    lane = lax.broadcasted_iota(jnp.int32, (1, width), 1)
    line = jnp.where(lane == far, jnp.sum(numer), 0.0)
    line = jnp.where(lane == 4 + far, jnp.sum(denom), line)
    mod_ref[0, vectors:] = stacked_parts(line, 8).astype(BF16)


def project_body(
    core_ref, own_ref, other_ref, w_ref, gain_ref, query_ref, pair_hbm, pair_ref, sems
):
    groups, rows, width = own_ref.shape
    _, sources, deep, columns = w_ref.shape
    near = cores = 2
    ys = near * sources // cores
    per_group = width // deep
    total = jnp.zeros((2 * rows, columns), F32)
    for g in range(groups):
        pieces = []
        for step in range(per_group):
            flat = g * per_group + step
            core = flat % cores
            y = flat // cores % ys
            x = flat // cores // ys
            pieces.append(w_ref[x * near + y % near, y // near * cores + core])
        left = jnp.concatenate([own_ref[g], other_ref[g]], axis=0)
        total = total + jnp.dot(
            left, jnp.concatenate(pieces, axis=0), preferred_element_type=F32
        )
    parts = []
    for kind in range(2):
        part = total[:, kind * HD : (kind + 1) * HD]
        gain = jnp.where(
            core_ref[0] == 0, gain_ref[kind : kind + 1, :HD], gain_ref[kind : kind + 1, HD:]
        )
        mean = jnp.mean(jnp.square(part), axis=1, keepdims=True)
        parts.append(part * lax.rsqrt(mean + EPS) * gain)
    query, keyed = parts
    valued = total[:, 2 * HD :].astype(BF16)
    img = query_ref.shape[1]
    for half, ref in enumerate((own_ref, other_ref)):
        at = half * rows
        query_ref[half] = query[at : at + img].astype(BF16)
        carried = ref[0, rows - 8 :, :HD]
        keys = keyed[at : at + rows - 8].astype(BF16)
        pair_ref[half, : rows - 8, :HD] = keys
        pair_ref[half, rows - 8 :, :HD] = carried
        pair_ref[half, :, HD:] = valued[at : at + rows]
    copies = [
        pltpu.make_async_copy(pair_ref, pair_hbm.at[copy], sems.at[copy])
        for copy in range(pair_hbm.shape[0])
    ]
    for copy in copies:
        copy.start()
    for copy in copies:
        copy.wait()


def attend_body(img_half, txt_half, limit_ref, place_ref, query_ref, pair_ref, out_ref):
    blocks, halves, rows, _ = pair_ref.shape
    sources = out_ref.shape[0]
    img = sources * img_half
    txt = sources * txt_half
    count = blocks * rows
    far, core = place_ref[0], place_ref[2]
    query = query_ref[...].reshape(2 * img, HD)
    index = lax.broadcasted_iota(jnp.int32, (1, count), 1)
    slot = index % rows
    block = index // rows
    source = (slot - img) // txt_half
    y = source // 2 * 2 + block % 2
    device = (block // 2 * 8 + y) * 2 + source % 2
    scores_of, valid_of = [], []
    rel = jnp.zeros((1, HD), F32)
    for half in range(halves):
        actual = jnp.where(half == 0, core, 1 - core)
        keys = pair_ref[:, half, :, :HD].reshape(count, HD)
        scores = lax.dot_general(
            query, keys, (((1,), (1,)), ((), ())), preferred_element_type=F32
        ) * (1.0 / HD**0.5)
        text = device * 4 + actual * txt_half + (slot - img) % txt_half
        valid = (slot < img) | ((slot < img + txt) & (text < limit_ref[far]))
        scores_of.append(jnp.where(valid, scores, NEG))
        valid_of.append(valid)
        for b in range(blocks):
            carried = pair_ref[b, half, rows - 8 :, :HD].astype(F32)
            rel = rel + jnp.sum(carried, axis=0, keepdims=True)
    top = functools.reduce(
        jnp.maximum, [jnp.max(s, axis=1, keepdims=True) for s in scores_of]
    )
    total = jnp.zeros((2 * img, 1), F32)
    summed = jnp.zeros((2 * img, HD), F32)
    for half in range(halves):
        weights = jnp.where(valid_of[half], jnp.exp(scores_of[half] - top), 0.0)
        total = total + jnp.sum(weights, axis=1, keepdims=True)
        values = pair_ref[:, half, :, HD:].reshape(count, HD)
        summed = summed + jnp.dot(weights.astype(BF16), values, preferred_element_type=F32)
    attended = (summed / total).astype(BF16)
    tail = stacked_parts(rel, 8).astype(BF16)
    for half in range(halves):
        actual = jnp.where(half == 0, core, 1 - core)
        at = pl.multiple_of(actual * img_half, img_half)
        for source in range(sources):
            start = half * img + source * img_half
            for z in range(out_ref.shape[1]):
                out_ref[source, z, pl.ds(at, img_half)] = attended[start : start + img_half]
    for source in range(sources):
        for z in range(out_ref.shape[1]):
            out_ref[source, z, 2 * img_half :] = tail


def final_body(tp_ref, flag_ref, att_ref, *refs):
    *w_refs, cache_ref, img_ref, mod_ref, out_ref, new_ref, rel_ref = refs
    groups = len(w_refs)
    batch, img_rows, width = img_ref.shape
    heads = att_ref.shape[0] // batch
    mixed = jnp.zeros((batch * img_rows, width), F32)
    rel = jnp.zeros((8, HD), F32)
    for k, w_ref in enumerate(w_refs):
        source = lax.rem(tp_ref[0] + groups - k, groups)
        lefts = []
        for h in range(heads):
            blocks = [att_ref[b * heads + h, source, :img_rows] for b in range(batch)]
            lefts.append(jnp.concatenate(blocks, axis=0))
        mixed = mixed + jnp.dot(
            jnp.concatenate(lefts, axis=1), w_ref[...], preferred_element_type=F32
        )
        for b in range(batch):
            rel = rel + att_ref[b * heads, k, img_rows:].astype(F32)
    for b in range(batch):
        gate = mod_ref[2, b : b + 1].astype(F32)
        resid = gate * mixed[b * img_rows : (b + 1) * img_rows]
        fresh = jnp.where(flag_ref[b] == 1, resid, cache_ref[b])
        new_ref[b] = fresh
        out_ref[b] = img_ref[b].astype(F32) + fresh
    sums = jnp.sum(rel, axis=0, keepdims=True)
    lane = lax.broadcasted_iota(jnp.int32, (1, HD), 1)
    for b in range(batch):
        numer = jnp.sum(jnp.where(lane == b, sums, 0.0))
        denom = jnp.sum(jnp.where(lane == 4 + b, sums, 0.0))
        rel_ref[b] = numer / jnp.maximum(denom, 1.0)


def local(img, txt, prev_mod, cache, modulation, w_qkv, qk_gain, output_weight, text_len, refresh):
    batch, img_rows, width = img.shape
    xs, fars, nears, cores = (lax.axis_size(a) for a in SEQ)
    tps = lax.axis_size(TP)
    deep, kinds, _ = w_qkv.shape
    sources = fars * cores
    around = xs * nears
    img_half, txt_half = img_rows // cores, txt.shape[1] // cores
    rows = sources * (img_half + txt_half) + 8
    place = jnp.stack([lax.axis_index(a) for a in (FAR, TP, CORE)]).astype(jnp.int32)
    core_index = lax.axis_index(CORE).astype(jnp.int32)[None]
    far_index = lax.axis_index(FAR).astype(jnp.int32)[None]

    arrays = (w_qkv.transpose(1, 0, 2), img, prev_mod, txt)
    packed = (sources, deep + 2 * img_half + 8, width)
    got = call(
        pack_body,
        pltpu.HBM(packed, BF16),
        [HBM] * 4,
        8,
        outs=HBM,
        scratch=[pltpu.VMEM(a.shape, a.dtype) for a in arrays]
        + [pltpu.VMEM(packed, BF16), pltpu.SemaphoreType.DMA((len(arrays),))],
    )(*(pltpu.with_memory_space_constraint(a, pltpu.HBM) for a in arrays))
    blocks = list(
        call(
            deal_body,
            (pltpu.HBM((output_weight.shape[0], width), BF16),) * tps,
            [SMEM, HBM],
            4,
            outs=(HBM,) * tps,
            scratch=[pltpu.SemaphoreType.DMA((tps,))],
        )(place[1:2], pltpu.with_memory_space_constraint(output_weight, pltpu.HBM))
    )
    for k in range(1, tps):
        blocks[k] = lax.ppermute(blocks[k], TP, [(i, (i + k) % tps) for i in range(tps)])
    got = swap(got, (FAR, CORE))
    weight = call(
        spread_body,
        pltpu.HBM((around, sources * deep, kinds * HD), BF16),
        [VMEM],
        8,
        outs=HBM,
        scratch=[
            pltpu.VMEM((sources * deep, kinds * HD), BF16),
            pltpu.SemaphoreType.DMA((around,)),
        ],
    )(got)
    weight = swap(weight, (X, NEAR)).reshape(around, sources, deep, kinds * HD)

    joined, previous = call(
        functools.partial(join_body, deep, img_half, txt_half),
        (shaped(rows, width), shaped(sources * img_half, width)),
        [SMEM, VMEM, VMEM],
        8,
    )(far_index, got, modulation)
    wide = lax.all_gather(joined, TP, axis=0, tiled=False)
    own = call(norm_body, shaped(tps, rows, width), [SMEM, VMEM, VMEM], 12)(place, wide, previous)
    other = lax.ppermute(own, CORE, [(0, 1), (1, 0)])

    query, pairs = call(
        project_body,
        (shaped(2, sources * img_half, HD), pltpu.HBM((around, 2, rows, 2 * HD), BF16)),
        [SMEM] + [VMEM] * 4,
        16,
        outs=(VMEM, HBM),
        scratch=[
            pltpu.VMEM((2, rows, 2 * HD), BF16),
            pltpu.SemaphoreType.DMA((around,)),
        ],
    )(core_index, own, other, weight, qk_gain)
    pairs = swap(pairs, (X, NEAR))
    attended = call(
        functools.partial(attend_body, img_half, txt_half),
        shaped(sources, tps, img_rows + 8, HD),
        [SMEM, SMEM, VMEM, VMEM],
        24,
    )(text_len, place, query, pairs)
    flat = attended.reshape(sources * tps, img_rows + 8, HD)
    attended = swap(flat, (FAR, CORE, TP)).reshape(attended.shape)

    whole = shaped(batch, img_rows, width, dtype=F32)
    return call(
        final_body,
        (whole, whole, shaped(batch, dtype=F32)),
        [SMEM, SMEM] + [VMEM] * (tps + 4),
        12,
        outs=(VMEM, VMEM, SMEM),
    )(place[1:2], refresh, attended, *blocks, cache, img, modulation)


def solution(mesh):
    finer = Mesh(mesh.devices.reshape(4, 4, 2, 2, mesh.shape["tp"]), SEQ + (TP,))
    in_specs = (
        P(None, SEQ, TP),
        P(None, SEQ, TP),
        P(None, SEQ, TP),
        P(None, SEQ, TP),
        P(None, None, TP),
        P(SEQ, None, TP),
        P(None, TP),
        P(TP, None),
        P(),
        P(),
    )
    out_specs = (P(None, SEQ, TP), P(None, SEQ, TP), P())

    return jax.shard_map(local, mesh=finer, in_specs=in_specs, out_specs=out_specs, check_vma=False)
```

```python
import functools

import jax
import jax.numpy as jnp
from jax import lax
from jax.experimental import pallas as pl
from jax.experimental.pallas import tpu as pltpu
from jax.sharding import Mesh
from jax.sharding import PartitionSpec as P


X, FAR, NEAR, CORE, TP = "seq_0", "seq_1a", "seq_1b", "seq_2", "tp"
SEQ = (X, FAR, NEAR, CORE)
HD = 128
EPS = 0.1
NEG = -1e30
F32 = jnp.float32
BF16 = jnp.bfloat16

VMEM = pl.BlockSpec(memory_space=pltpu.VMEM)
SMEM = pl.BlockSpec(memory_space=pltpu.SMEM)
HBM = pl.BlockSpec(memory_space=pltpu.HBM)


def call(body, out_shape, in_specs, mebibytes, outs=None, scratch=()):
    outs = outs or jax.tree.map(lambda _: VMEM, out_shape)
    return pl.pallas_call(
        body,
        out_shape=out_shape,
        in_specs=in_specs,
        out_specs=outs,
        scratch_shapes=scratch,
        compiler_params=pltpu.CompilerParams(vmem_limit_bytes=mebibytes << 20),
    )


def shaped(*shape, dtype=BF16):
    return jax.ShapeDtypeStruct(shape, dtype)


def swap(value, axis):
    return lax.all_to_all(value, axis, 0, 0, tiled=True)


def split_three(value):
    high = value.astype(BF16).astype(F32)
    rest = value - high
    middle = rest.astype(BF16).astype(F32)
    return high, middle, rest - middle


def stacked_parts(value, rows):
    row = lax.broadcasted_iota(jnp.int32, (rows, value.shape[1]), 0)
    high, middle, low = split_three(value)
    return jnp.where(row == 0, high, jnp.where(row == 1, middle, jnp.where(row == 2, low, 0.0)))


def pack_body(w_hbm, img_hbm, prev_hbm, txt_hbm, out_ref, w_ref, img_ref, prev_ref, txt_ref, sems):
    copies = [
        pltpu.make_async_copy(source, target, sems.at[i])
        for i, (source, target) in enumerate(
            ((w_hbm, w_ref), (img_hbm, img_ref), (prev_hbm, prev_ref), (txt_hbm, txt_ref))
        )
    ]
    for copy in copies:
        copy.start()
    for copy in copies:
        copy.wait()
    kinds, deep, columns = w_ref.shape
    batch, img_rows, width = img_ref.shape
    cores = columns // HD
    img_half = img_rows // cores
    txt_half = txt_ref.shape[1] // cores
    for b in range(batch):
        for c in range(cores):
            to = b * cores + c
            for kind in range(kinds):
                out_ref[to, :deep, kind * HD : (kind + 1) * HD] = w_ref[
                    kind, :, c * HD : (c + 1) * HD
                ]
            at = deep
            for ref in (img_ref, prev_ref):
                out_ref[to, at : at + img_half] = ref[b, c * img_half : (c + 1) * img_half]
                at += img_half
            text = txt_ref[b].astype(F32)[c * txt_half : (c + 1) * txt_half]
            text = jnp.concatenate([text, jnp.zeros((8 - txt_half, width), F32)], axis=0)
            out_ref[to, at : at + 8] = text.astype(BF16)


def spread_body(got_ref, out_hbm, block_ref, sems):
    sources = got_ref.shape[0]
    deep = block_ref.shape[0] // sources
    for source in range(sources):
        block_ref[source * deep : (source + 1) * deep] = got_ref[source, :deep]
    copies = [
        pltpu.make_async_copy(block_ref, out_hbm.at[copy], sems.at[copy])
        for copy in range(out_hbm.shape[0])
    ]
    for copy in copies:
        copy.start()
    for copy in copies:
        copy.wait()


def join_body(deep, img_half, txt_half, far_ref, got_ref, mod_ref, out_ref, prev_ref):
    sources = got_ref.shape[0]
    width = got_ref.shape[2]
    for source in range(sources):
        out_ref[source * img_half : (source + 1) * img_half] = got_ref[
            source, deep : deep + img_half
        ]
        prev_ref[source * img_half : (source + 1) * img_half] = got_ref[
            source, deep + img_half : deep + 2 * img_half
        ]
    at = deep + 2 * img_half
    texts = [got_ref[source, at : at + 8].astype(F32)[:txt_half] for source in range(sources)]
    vectors = []
    for which in range(2):
        chosen = mod_ref[which, 0:1].astype(F32)
        for b in range(1, mod_ref.shape[1]):
            chosen = jnp.where(far_ref[0] == b, mod_ref[which, b : b + 1].astype(F32), chosen)
        vectors.append(chosen)
    tail = jnp.concatenate(texts + vectors + [jnp.zeros((6, width), F32)], axis=0)
    out_ref[sources * img_half :] = tail.astype(BF16)


def norm_body(place_ref, x_ref, prev_ref, mod_ref):
    groups, rows, width = x_ref.shape
    vectors = rows - 8
    features = groups * width
    sums = jnp.zeros((rows, 1), F32)
    for g in range(groups):
        sums = sums + jnp.sum(x_ref[g].astype(F32), axis=1, keepdims=True)
    center = sums / features
    squares = jnp.zeros((rows, 1), F32)
    for g in range(groups):
        squares = squares + jnp.sum(
            jnp.square(x_ref[g].astype(F32) - center), axis=1, keepdims=True
        )
    inv = lax.rsqrt(squares / features + EPS)
    for g in range(groups):
        values = x_ref[g].astype(F32)
        shift = values[vectors : vectors + 1]
        scale = values[vectors + 1 : vectors + 2]
        mod_ref[g] = ((values - center) * inv * (1.0 + scale) + shift).astype(BF16)
    far = place_ref[0]
    own = mod_ref.at[place_ref[1]]
    previous = prev_ref[...].astype(F32)
    numer = jnp.abs(own[: prev_ref.shape[0]].astype(F32) - previous)
    denom = jnp.abs(previous)
    lane = lax.broadcasted_iota(jnp.int32, (1, width), 1)
    line = jnp.where(lane == far, jnp.sum(numer), 0.0)
    line = jnp.where(lane == 4 + far, jnp.sum(denom), line)
    mod_ref[0, vectors:] = stacked_parts(line, 8).astype(BF16)


def project_body(
    core_ref, own_ref, other_ref, w_hbm, gain_ref, query_ref, pair_ref, w_ref, sems
):
    groups, rows, width = own_ref.shape
    _, sources, deep, columns = w_ref.shape
    near = cores = 2
    fetches = []
    for x in range(w_ref.shape[0] // near):
        at = pl.ds(x * near, near)
        fetches.append(pltpu.make_async_copy(w_hbm.at[at], w_ref.at[at], sems.at[x]))
        fetches[-1].start()
    ys = near * sources // cores
    per_group = width // deep
    total = jnp.zeros((2 * rows, columns), F32)
    for g in range(groups):
        pieces = []
        if g % 2 == 0:
            fetches[g // 2].wait()
        for step in range(per_group):
            flat = g * per_group + step
            core = flat % cores
            y = flat // cores % ys
            x = flat // cores // ys
            pieces.append(w_ref[x * near + y % near, y // near * cores + core])
        left = jnp.concatenate([own_ref[g], other_ref[g]], axis=0)
        total = total + jnp.dot(
            left, jnp.concatenate(pieces, axis=0), preferred_element_type=F32
        )
    parts = []
    for kind in range(2):
        part = total[:, kind * HD : (kind + 1) * HD]
        gain = jnp.where(
            core_ref[0] == 0, gain_ref[kind : kind + 1, :HD], gain_ref[kind : kind + 1, HD:]
        )
        mean = jnp.mean(jnp.square(part), axis=1, keepdims=True)
        parts.append(part * lax.rsqrt(mean + EPS) * gain)
    query, keyed = parts
    valued = total[:, 2 * HD :].astype(BF16)
    img = query_ref.shape[1]
    for half, ref in enumerate((own_ref, other_ref)):
        at = half * rows
        query_ref[half] = query[at : at + img].astype(BF16)
        carried = ref[0, rows - 8 :, :HD]
        keys = keyed[at : at + rows - 8].astype(BF16)
        for copy in range(pair_ref.shape[0]):
            pair_ref[copy, half, : rows - 8, :HD] = keys
            pair_ref[copy, half, rows - 8 :, :HD] = carried
            pair_ref[copy, half, :, HD:] = valued[at : at + rows]


def attend_body(img_half, txt_half, limit_ref, place_ref, query_ref, pair_ref, out_ref):
    blocks, halves, rows, _ = pair_ref.shape
    sources = out_ref.shape[0]
    img = sources * img_half
    txt = sources * txt_half
    count = blocks * rows
    far, core = place_ref[0], place_ref[2]
    query = query_ref[...].reshape(2 * img, HD)
    index = lax.broadcasted_iota(jnp.int32, (1, count), 1)
    slot = index % rows
    block = index // rows
    source = (slot - img) // txt_half
    y = source // 2 * 2 + block % 2
    device = (block // 2 * 8 + y) * 2 + source % 2
    scores_of, valid_of = [], []
    rel = jnp.zeros((1, HD), F32)
    for half in range(halves):
        actual = jnp.where(half == 0, core, 1 - core)
        keys = pair_ref[:, half, :, :HD].reshape(count, HD)
        scores = lax.dot_general(
            query, keys, (((1,), (1,)), ((), ())), preferred_element_type=F32
        ) * (1.0 / HD**0.5)
        text = device * 4 + actual * txt_half + (slot - img) % txt_half
        valid = (slot < img) | ((slot < img + txt) & (text < limit_ref[far]))
        scores_of.append(jnp.where(valid, scores, NEG))
        valid_of.append(valid)
        for b in range(blocks):
            carried = pair_ref[b, half, rows - 8 :, :HD].astype(F32)
            rel = rel + jnp.sum(carried, axis=0, keepdims=True)
    top = functools.reduce(
        jnp.maximum, [jnp.max(s, axis=1, keepdims=True) for s in scores_of]
    )
    total = jnp.zeros((2 * img, 1), F32)
    summed = jnp.zeros((2 * img, HD), F32)
    for half in range(halves):
        weights = jnp.where(valid_of[half], jnp.exp(scores_of[half] - top), 0.0)
        total = total + jnp.sum(weights, axis=1, keepdims=True)
        values = pair_ref[:, half, :, HD:].reshape(count, HD)
        summed = summed + jnp.dot(weights.astype(BF16), values, preferred_element_type=F32)
    attended = (summed / total).astype(BF16)
    tail = stacked_parts(rel, 8).astype(BF16)
    for half in range(halves):
        actual = jnp.where(half == 0, core, 1 - core)
        at = pl.multiple_of(actual * img_half, img_half)
        for source in range(sources):
            start = half * img + source * img_half
            out_ref[source, pl.ds(at, img_half)] = attended[start : start + img_half]
    for source in range(sources):
        out_ref[source, 2 * img_half :] = tail


def slots_of(flag_ref, batch, count):
    order = [jnp.int32(0)] * count
    seen = jnp.int32(0)
    slot = []
    for b in range(batch):
        on = flag_ref[b] == 1
        slot.append(seen)
        for i in range(count):
            order[i] = jnp.where(on & (seen == i), jnp.int32(b), order[i])
        seen = seen + jnp.where(on, 1, 0)
    return order, slot


def mix_body(img_rows, flag_ref, att_ref, w_ref, out_ref):
    groups, rows, width = out_ref.shape
    heads = w_ref.shape[0] // HD
    batch = att_ref.shape[0] // heads
    slots = (rows - 8) // img_rows
    order, _ = slots_of(flag_ref, batch, slots)
    lefts = []
    for h in range(heads):
        lefts.append(
            jnp.concatenate([att_ref[order[i] * heads + h, :img_rows] for i in range(slots)], axis=0)
        )
    left = jnp.concatenate(lefts, axis=1)
    rel = jnp.zeros((8, HD), F32)
    for b in range(batch):
        rel = rel + att_ref[b * heads, img_rows:].astype(F32)
    tail = stacked_parts(jnp.sum(rel, axis=0, keepdims=True), 8)
    tail = jnp.concatenate([tail, jnp.zeros((8, width - HD), F32)], axis=1).astype(BF16)
    for g in range(groups):
        mixed = jnp.dot(left, w_ref[:, g * width : (g + 1) * width], preferred_element_type=F32)
        out_ref[g, : rows - 8] = mixed.astype(BF16)
        out_ref[g, rows - 8 :] = tail


def final_body(flag_ref, part_ref, cache_ref, img_ref, mod_ref, out_ref, new_ref, rel_ref, sum_ref):
    groups, rows, _ = part_ref.shape
    batch, img_rows, _ = img_ref.shape
    slots = (rows - 8) // img_rows
    mixed = part_ref[0].astype(F32)
    for g in range(1, groups):
        mixed = mixed + part_ref[g].astype(F32)
    sum_ref[...] = mixed
    _, slot = slots_of(flag_ref, batch, slots)
    for b in range(batch):
        gate = mod_ref[2, b : b + 1].astype(F32)
        at = pl.multiple_of(jnp.minimum(slot[b], slots - 1) * img_rows, img_rows)
        resid = gate * sum_ref[pl.ds(at, img_rows)]
        fresh = jnp.where(flag_ref[b] == 1, resid, cache_ref[b])
        new_ref[b] = fresh
        out_ref[b] = img_ref[b].astype(F32) + fresh
    sums = jnp.sum(mixed[rows - 8 :, :HD], axis=0, keepdims=True)
    lane = lax.broadcasted_iota(jnp.int32, (1, HD), 1)
    for b in range(batch):
        numer = jnp.sum(jnp.where(lane == b, sums, 0.0))
        denom = jnp.sum(jnp.where(lane == 4 + b, sums, 0.0))
        rel_ref[b] = numer / jnp.maximum(denom, 1.0)


def local(img, txt, prev_mod, cache, modulation, w_qkv, qk_gain, output_weight, text_len, refresh):
    batch, img_rows, width = img.shape
    xs, fars, nears, cores = (lax.axis_size(a) for a in SEQ)
    tps = lax.axis_size(TP)
    deep, kinds, _ = w_qkv.shape
    sources = fars * cores
    around = xs * nears
    img_half, txt_half = img_rows // cores, txt.shape[1] // cores
    rows = sources * (img_half + txt_half) + 8
    place = jnp.stack([lax.axis_index(a) for a in (FAR, TP, CORE)]).astype(jnp.int32)
    core_index = lax.axis_index(CORE).astype(jnp.int32)[None]
    far_index = lax.axis_index(FAR).astype(jnp.int32)[None]

    arrays = (w_qkv.transpose(1, 0, 2), img, prev_mod, txt)
    got = call(
        pack_body,
        shaped(sources, deep + 2 * img_half + 8, width),
        [HBM] * 4,
        8,
        scratch=[pltpu.VMEM(a.shape, a.dtype) for a in arrays]
        + [pltpu.SemaphoreType.DMA((len(arrays),))],
    )(*(pltpu.with_memory_space_constraint(a, pltpu.HBM) for a in arrays))
    got = swap(got, (FAR, CORE))
    weight = call(
        spread_body,
        pltpu.HBM((around, sources * deep, kinds * HD), BF16),
        [VMEM],
        8,
        outs=HBM,
        scratch=[
            pltpu.VMEM((sources * deep, kinds * HD), BF16),
            pltpu.SemaphoreType.DMA((around,)),
        ],
    )(got)
    weight = swap(weight, (X, NEAR)).reshape(around, sources, deep, kinds * HD)

    joined, previous = call(
        functools.partial(join_body, deep, img_half, txt_half),
        (shaped(rows, width), shaped(sources * img_half, width)),
        [SMEM, VMEM, VMEM],
        8,
    )(far_index, got, modulation)
    wide = lax.all_gather(joined, TP, axis=0, tiled=False)
    own = call(norm_body, shaped(tps, rows, width), [SMEM, VMEM, VMEM], 12)(place, wide, previous)
    other = lax.ppermute(own, CORE, [(0, 1), (1, 0)])

    query, pairs = call(
        project_body,
        (shaped(2, sources * img_half, HD), shaped(around, 2, rows, 2 * HD)),
        [SMEM, VMEM, VMEM, HBM, VMEM],
        16,
        scratch=[
            pltpu.VMEM((around, sources, deep, kinds * HD), BF16),
            pltpu.SemaphoreType.DMA((xs,)),
        ],
    )(core_index, own, other, pltpu.with_memory_space_constraint(weight, pltpu.HBM), qk_gain)
    pairs = swap(pairs, (X, NEAR))
    attended = call(
        functools.partial(attend_body, img_half, txt_half),
        shaped(sources, img_rows + 8, HD),
        [SMEM, SMEM, VMEM, VMEM],
        24,
    )(text_len, place, query, pairs)
    attended = swap(attended, (FAR, CORE))

    slots = batch - 1
    parts = call(
        functools.partial(mix_body, img_rows),
        shaped(tps, slots * img_rows + 8, width),
        [SMEM, VMEM, VMEM],
        12,
    )(refresh, attended, output_weight)
    parts = swap(parts, TP)

    whole = shaped(batch, img_rows, width, dtype=F32)
    return pl.pallas_call(
        final_body,
        out_shape=(whole, whole, shaped(batch, dtype=F32)),
        in_specs=[SMEM] + [VMEM] * 4,
        out_specs=(VMEM, VMEM, SMEM),
        scratch_shapes=[pltpu.VMEM((slots * img_rows + 8, width), F32)],
        compiler_params=pltpu.CompilerParams(vmem_limit_bytes=8 << 20),
    )(refresh, parts, cache, img, modulation)


def solution(mesh):
    finer = Mesh(mesh.devices.reshape(4, 4, 2, 2, mesh.shape["tp"]), SEQ + (TP,))
    in_specs = (
        P(None, SEQ, TP),
        P(None, SEQ, TP),
        P(None, SEQ, TP),
        P(None, SEQ, TP),
        P(None, None, TP),
        P(SEQ, None, TP),
        P(None, TP),
        P(TP, None),
        P(),
        P(),
    )
    out_specs = (P(None, SEQ, TP), P(None, SEQ, TP), P())

    return jax.shard_map(local, mesh=finer, in_specs=in_specs, out_specs=out_specs, check_vma=False)
```

```python
import functools

import jax
import jax.numpy as jnp
from jax import lax
from jax.experimental import pallas as pl
from jax.experimental.pallas import tpu as pltpu
from jax.sharding import Mesh
from jax.sharding import PartitionSpec as P


X, FAR, NEAR, CORE, TP = "seq_0", "seq_1a", "seq_1b", "seq_2", "tp"
SEQ = (X, FAR, NEAR, CORE)
HD = 128
EPS = 0.1
NEG = -1e30
F32 = jnp.float32
BF16 = jnp.bfloat16

VMEM = pl.BlockSpec(memory_space=pltpu.VMEM)
SMEM = pl.BlockSpec(memory_space=pltpu.SMEM)
HBM = pl.BlockSpec(memory_space=pltpu.HBM)


def call(body, out_shape, in_specs, mebibytes, outs=None, scratch=()):
    outs = outs or jax.tree.map(lambda _: VMEM, out_shape)
    return pl.pallas_call(
        body,
        out_shape=out_shape,
        in_specs=in_specs,
        out_specs=outs,
        scratch_shapes=scratch,
        compiler_params=pltpu.CompilerParams(vmem_limit_bytes=mebibytes << 20),
    )


def shaped(*shape, dtype=BF16):
    return jax.ShapeDtypeStruct(shape, dtype)


def swap(value, axis):
    return lax.all_to_all(value, axis, 0, 0, tiled=True)


def split_three(value):
    high = value.astype(BF16).astype(F32)
    rest = value - high
    middle = rest.astype(BF16).astype(F32)
    return high, middle, rest - middle


def stacked_parts(value, rows):
    row = lax.broadcasted_iota(jnp.int32, (rows, value.shape[1]), 0)
    high, middle, low = split_three(value)
    return jnp.where(row == 0, high, jnp.where(row == 1, middle, jnp.where(row == 2, low, 0.0)))


def pack_body(w_hbm, img_hbm, prev_hbm, txt_hbm, out_ref, w_ref, img_ref, prev_ref, txt_ref, sems):
    copies = [
        pltpu.make_async_copy(source, target, sems.at[i])
        for i, (source, target) in enumerate(
            ((w_hbm, w_ref), (img_hbm, img_ref), (prev_hbm, prev_ref), (txt_hbm, txt_ref))
        )
    ]
    for copy in copies:
        copy.start()
    for copy in copies:
        copy.wait()
    kinds, deep, columns = w_ref.shape
    batch, img_rows, width = img_ref.shape
    cores = columns // HD
    img_half = img_rows // cores
    txt_half = txt_ref.shape[1] // cores
    for b in range(batch):
        for c in range(cores):
            to = b * cores + c
            for kind in range(kinds):
                out_ref[to, :deep, kind * HD : (kind + 1) * HD] = w_ref[
                    kind, :, c * HD : (c + 1) * HD
                ]
            at = deep
            for ref in (img_ref, prev_ref):
                out_ref[to, at : at + img_half] = ref[b, c * img_half : (c + 1) * img_half]
                at += img_half
            text = txt_ref[b].astype(F32)[c * txt_half : (c + 1) * txt_half]
            text = jnp.concatenate([text, jnp.zeros((8 - txt_half, width), F32)], axis=0)
            out_ref[to, at : at + 8] = text.astype(BF16)


def spread_body(got_ref, out_hbm, block_ref, sems):
    sources = got_ref.shape[0]
    deep = block_ref.shape[0] // sources
    for source in range(sources):
        block_ref[source * deep : (source + 1) * deep] = got_ref[source, :deep]
    copies = [
        pltpu.make_async_copy(block_ref, out_hbm.at[copy], sems.at[copy])
        for copy in range(out_hbm.shape[0])
    ]
    for copy in copies:
        copy.start()
    for copy in copies:
        copy.wait()


def join_body(
    deep, img_half, txt_half, far_ref, flag_ref, got_ref, mod_ref, out_ref, prev_ref, tail_ref
):
    tail_no = jnp.int32(-1)
    for b in range(mod_ref.shape[1]):
        tail_no = tail_no + jnp.where(flag_ref[b] == 1, 1, 0)
    tail_ref[0] = tail_no
    sources = got_ref.shape[0]
    width = got_ref.shape[2]
    for source in range(sources):
        out_ref[source * img_half : (source + 1) * img_half] = got_ref[
            source, deep : deep + img_half
        ]
        prev_ref[source * img_half : (source + 1) * img_half] = got_ref[
            source, deep + img_half : deep + 2 * img_half
        ]
    at = deep + 2 * img_half
    texts = [got_ref[source, at : at + 8].astype(F32)[:txt_half] for source in range(sources)]
    vectors = []
    for which in range(2):
        chosen = mod_ref[which, 0:1].astype(F32)
        for b in range(1, mod_ref.shape[1]):
            chosen = jnp.where(far_ref[0] == b, mod_ref[which, b : b + 1].astype(F32), chosen)
        vectors.append(chosen)
    tail = jnp.concatenate(texts + vectors + [jnp.zeros((6, width), F32)], axis=0)
    out_ref[sources * img_half :] = tail.astype(BF16)


def norm_body(place_ref, x_ref, prev_ref, mod_ref):
    groups, rows, width = x_ref.shape
    vectors = rows - 8
    features = groups * width
    sums = jnp.zeros((rows, 1), F32)
    for g in range(groups):
        sums = sums + jnp.sum(x_ref[g].astype(F32), axis=1, keepdims=True)
    center = sums / features
    squares = jnp.zeros((rows, 1), F32)
    for g in range(groups):
        squares = squares + jnp.sum(
            jnp.square(x_ref[g].astype(F32) - center), axis=1, keepdims=True
        )
    inv = lax.rsqrt(squares / features + EPS)
    for g in range(groups):
        values = x_ref[g].astype(F32)
        shift = values[vectors : vectors + 1]
        scale = values[vectors + 1 : vectors + 2]
        mod_ref[g] = ((values - center) * inv * (1.0 + scale) + shift).astype(BF16)
    far = place_ref[0]
    own = mod_ref.at[place_ref[1]]
    previous = prev_ref[...].astype(F32)
    numer = jnp.abs(own[: prev_ref.shape[0]].astype(F32) - previous)
    denom = jnp.abs(previous)
    lane = lax.broadcasted_iota(jnp.int32, (1, width), 1)
    line = jnp.where(lane == far, jnp.sum(numer), 0.0)
    line = jnp.where(lane == 4 + far, jnp.sum(denom), line)
    mod_ref[0, vectors:] = stacked_parts(line, 8).astype(BF16)


def project_body(core_ref, own_ref, other_ref, w_ref, gain_ref, query_ref, pair_ref):
    groups, rows, width = own_ref.shape
    _, sources, deep, columns = w_ref.shape
    near = cores = 2
    ys = near * sources // cores
    per_group = width // deep
    total = jnp.zeros((2 * rows, columns), F32)
    for g in range(groups):
        pieces = []
        for step in range(per_group):
            flat = g * per_group + step
            core = flat % cores
            y = flat // cores % ys
            x = flat // cores // ys
            pieces.append(w_ref[x * near + y % near, y // near * cores + core])
        left = jnp.concatenate([own_ref[g], other_ref[g]], axis=0)
        total = total + jnp.dot(
            left, jnp.concatenate(pieces, axis=0), preferred_element_type=F32
        )
    parts = []
    for kind in range(2):
        part = total[:, kind * HD : (kind + 1) * HD]
        gain = jnp.where(
            core_ref[0] == 0, gain_ref[kind : kind + 1, :HD], gain_ref[kind : kind + 1, HD:]
        )
        mean = jnp.mean(jnp.square(part), axis=1, keepdims=True)
        parts.append(part * lax.rsqrt(mean + EPS) * gain)
    query, keyed = parts
    valued = total[:, 2 * HD :].astype(BF16)
    img = query_ref.shape[1]
    for half, ref in enumerate((own_ref, other_ref)):
        at = half * rows
        query_ref[half] = query[at : at + img].astype(BF16)
        carried = ref[0, rows - 8 :, :HD]
        keys = keyed[at : at + rows - 8].astype(BF16)
        for copy in range(pair_ref.shape[0]):
            pair_ref[copy, half, : rows - 8, :HD] = keys
            pair_ref[copy, half, rows - 8 :, :HD] = carried
            pair_ref[copy, half, :, HD:] = valued[at : at + rows]


def attend_body(img_half, txt_half, limit_ref, place_ref, query_ref, pair_ref, out_ref):
    blocks, halves, rows, _ = pair_ref.shape
    sources = out_ref.shape[0]
    img = sources * img_half
    txt = sources * txt_half
    count = blocks * rows
    far, core = place_ref[0], place_ref[2]
    query = query_ref[...].reshape(2 * img, HD)
    index = lax.broadcasted_iota(jnp.int32, (1, count), 1)
    slot = index % rows
    block = index // rows
    source = (slot - img) // txt_half
    y = source // 2 * 2 + block % 2
    device = (block // 2 * 8 + y) * 2 + source % 2
    scores_of, valid_of = [], []
    rel = jnp.zeros((1, HD), F32)
    for half in range(halves):
        actual = jnp.where(half == 0, core, 1 - core)
        keys = pair_ref[:, half, :, :HD].reshape(count, HD)
        scores = lax.dot_general(
            query, keys, (((1,), (1,)), ((), ())), preferred_element_type=F32
        ) * (1.0 / HD**0.5)
        text = device * 4 + actual * txt_half + (slot - img) % txt_half
        valid = (slot < img) | ((slot < img + txt) & (text < limit_ref[far]))
        scores_of.append(jnp.where(valid, scores, NEG))
        valid_of.append(valid)
        for b in range(blocks):
            carried = pair_ref[b, half, rows - 8 :, :HD].astype(F32)
            rel = rel + jnp.sum(carried, axis=0, keepdims=True)
    top = functools.reduce(
        jnp.maximum, [jnp.max(s, axis=1, keepdims=True) for s in scores_of]
    )
    total = jnp.zeros((2 * img, 1), F32)
    summed = jnp.zeros((2 * img, HD), F32)
    for half in range(halves):
        weights = jnp.where(valid_of[half], jnp.exp(scores_of[half] - top), 0.0)
        total = total + jnp.sum(weights, axis=1, keepdims=True)
        values = pair_ref[:, half, :, HD:].reshape(count, HD)
        summed = summed + jnp.dot(weights.astype(BF16), values, preferred_element_type=F32)
    attended = (summed / total).astype(BF16)
    tail = stacked_parts(rel, 8).astype(BF16)
    for half in range(halves):
        actual = jnp.where(half == 0, core, 1 - core)
        at = pl.multiple_of(actual * img_half, img_half)
        for source in range(sources):
            start = half * img + source * img_half
            out_ref[source, pl.ds(at, img_half)] = attended[start : start + img_half]
    for source in range(sources):
        out_ref[source, 2 * img_half :] = tail


def slots_of(flag_ref, batch, count):
    order = [jnp.int32(0)] * count
    seen = jnp.int32(0)
    slot = []
    for b in range(batch):
        on = flag_ref[b] == 1
        slot.append(seen)
        for i in range(count):
            order[i] = jnp.where(on & (seen == i), jnp.int32(b), order[i])
        seen = seen + jnp.where(on, 1, 0)
    return order, slot


def mix_body(img_rows, flag_ref, att_ref, w_ref, out_ref):
    groups, rows, width = out_ref.shape
    heads = w_ref.shape[0] // HD
    batch = att_ref.shape[0] // heads
    slots = (rows - 8) // img_rows
    order, _ = slots_of(flag_ref, batch, slots)
    lefts = []
    for h in range(heads):
        lefts.append(
            jnp.concatenate([att_ref[order[i] * heads + h, :img_rows] for i in range(slots)], axis=0)
        )
    left = jnp.concatenate(lefts, axis=1)
    rel = jnp.zeros((8, HD), F32)
    for b in range(batch):
        rel = rel + att_ref[b * heads, img_rows:].astype(F32)
    tail = stacked_parts(jnp.sum(rel, axis=0, keepdims=True), 8)
    tail = jnp.concatenate([tail, jnp.zeros((8, width - HD), F32)], axis=1).astype(BF16)
    for g in range(groups):
        mixed = jnp.dot(left, w_ref[:, g * width : (g + 1) * width], preferred_element_type=F32)
        out_ref[g, : rows - 8] = mixed.astype(BF16)
        out_ref[g, rows - 8 :] = tail


def final_body(flag_ref, part_ref, cache_ref, img_ref, mod_ref, out_ref, new_ref, rel_ref, sum_ref):
    groups, rows, _ = part_ref.shape
    batch, img_rows, _ = img_ref.shape
    slots = (rows - 8) // img_rows
    mixed = part_ref[0].astype(F32)
    for g in range(1, groups):
        mixed = mixed + part_ref[g].astype(F32)
    sum_ref[...] = mixed
    _, slot = slots_of(flag_ref, batch, slots)
    for b in range(batch):
        gate = mod_ref[2, b : b + 1].astype(F32)
        at = pl.multiple_of(jnp.minimum(slot[b], slots - 1) * img_rows, img_rows)
        resid = gate * sum_ref[pl.ds(at, img_rows)]
        fresh = jnp.where(flag_ref[b] == 1, resid, cache_ref[b])
        new_ref[b] = fresh
        out_ref[b] = img_ref[b].astype(F32) + fresh
    sums = jnp.sum(mixed[rows - 8 :, :HD], axis=0, keepdims=True)
    lane = lax.broadcasted_iota(jnp.int32, (1, HD), 1)
    for b in range(batch):
        numer = jnp.sum(jnp.where(lane == b, sums, 0.0))
        denom = jnp.sum(jnp.where(lane == 4 + b, sums, 0.0))
        rel_ref[b] = numer / jnp.maximum(denom, 1.0)


def local(img, txt, prev_mod, cache, modulation, w_qkv, qk_gain, output_weight, text_len, refresh):
    batch, img_rows, width = img.shape
    xs, fars, nears, cores = (lax.axis_size(a) for a in SEQ)
    tps = lax.axis_size(TP)
    deep, kinds, _ = w_qkv.shape
    sources = fars * cores
    around = xs * nears
    img_half, txt_half = img_rows // cores, txt.shape[1] // cores
    rows = sources * (img_half + txt_half) + 8
    place = jnp.stack([lax.axis_index(a) for a in (FAR, TP, CORE)]).astype(jnp.int32)
    core_index = lax.axis_index(CORE).astype(jnp.int32)[None]
    far_index = lax.axis_index(FAR).astype(jnp.int32)[None]

    arrays = (w_qkv.transpose(1, 0, 2), img, prev_mod, txt)
    got = call(
        pack_body,
        shaped(sources, deep + 2 * img_half + 8, width),
        [HBM] * 4,
        8,
        scratch=[pltpu.VMEM(a.shape, a.dtype) for a in arrays]
        + [pltpu.SemaphoreType.DMA((len(arrays),))],
    )(*(pltpu.with_memory_space_constraint(a, pltpu.HBM) for a in arrays))
    got = swap(got, (FAR, CORE))
    weight = call(
        spread_body,
        pltpu.HBM((around, sources * deep, kinds * HD), BF16),
        [VMEM],
        8,
        outs=HBM,
        scratch=[
            pltpu.VMEM((sources * deep, kinds * HD), BF16),
            pltpu.SemaphoreType.DMA((around,)),
        ],
    )(got)
    weight = swap(weight, (X, NEAR)).reshape(around, sources, deep, kinds * HD)

    joined, previous, tail_no = call(
        functools.partial(join_body, deep, img_half, txt_half),
        (
            shaped(rows, width),
            shaped(sources * img_half, width),
            shaped(1, dtype=jnp.int32),
        ),
        [SMEM, SMEM, VMEM, VMEM],
        8,
        outs=(VMEM, VMEM, SMEM),
    )(far_index, refresh, got, modulation)
    wide = lax.all_gather(joined, TP, axis=0, tiled=False)
    own = call(norm_body, shaped(tps, rows, width), [SMEM, VMEM, VMEM], 12)(place, wide, previous)
    other = lax.ppermute(own, CORE, [(0, 1), (1, 0)])

    query, pairs = call(
        project_body,
        (shaped(2, sources * img_half, HD), shaped(around, 2, rows, 2 * HD)),
        [SMEM] + [VMEM] * 4,
        16,
    )(core_index, own, other, weight, qk_gain)
    pairs = swap(pairs, (X, NEAR))
    attended = call(
        functools.partial(attend_body, img_half, txt_half),
        shaped(sources, img_rows + 8, HD),
        [SMEM, SMEM, VMEM, VMEM],
        24,
    )(text_len, place, query, pairs)
    attended = swap(attended, (FAR, CORE))

    tails = [functools.partial(finish, slots) for slots in range(1, batch)]
    return lax.switch(tail_no[0], tails, refresh, attended, output_weight, cache, img, modulation)


def finish(slots, refresh, attended, output_weight, cache, img, modulation):
    batch, img_rows, width = img.shape
    rows = slots * img_rows + 8
    parts = call(
        functools.partial(mix_body, img_rows),
        shaped(lax.axis_size(TP), rows, width),
        [SMEM, VMEM, VMEM],
        12,
    )(refresh, attended, output_weight)
    parts = swap(parts, TP)
    whole = shaped(batch, img_rows, width, dtype=F32)
    return call(
        final_body,
        (whole, whole, shaped(batch, dtype=F32)),
        [SMEM] + [VMEM] * 4,
        8,
        outs=(VMEM, VMEM, SMEM),
        scratch=[pltpu.VMEM((rows, width), F32)],
    )(refresh, parts, cache, img, modulation)


def solution(mesh):
    finer = Mesh(mesh.devices.reshape(4, 4, 2, 2, mesh.shape["tp"]), SEQ + (TP,))
    in_specs = (
        P(None, SEQ, TP),
        P(None, SEQ, TP),
        P(None, SEQ, TP),
        P(None, SEQ, TP),
        P(None, None, TP),
        P(SEQ, None, TP),
        P(None, TP),
        P(TP, None),
        P(),
        P(),
    )
    out_specs = (P(None, SEQ, TP), P(None, SEQ, TP), P())

    return jax.shard_map(local, mesh=finer, in_specs=in_specs, out_specs=out_specs, check_vma=False)
```

```python
import functools

import jax
import jax.numpy as jnp
from jax import lax
from jax.experimental import pallas as pl
from jax.experimental.pallas import tpu as pltpu
from jax.sharding import Mesh
from jax.sharding import PartitionSpec as P


X, FAR, NEAR, CORE, TP = "seq_0", "seq_1a", "seq_1b", "seq_2", "tp"
SEQ = (X, FAR, NEAR, CORE)
HD = 128
EPS = 0.1
NEG = -1e30
F32 = jnp.float32
BF16 = jnp.bfloat16

VMEM = pl.BlockSpec(memory_space=pltpu.VMEM)
SMEM = pl.BlockSpec(memory_space=pltpu.SMEM)
HBM = pl.BlockSpec(memory_space=pltpu.HBM)


def call(body, out_shape, in_specs, mebibytes, outs=None, scratch=()):
    outs = outs or jax.tree.map(lambda _: VMEM, out_shape)
    return pl.pallas_call(
        body,
        out_shape=out_shape,
        in_specs=in_specs,
        out_specs=outs,
        scratch_shapes=scratch,
        compiler_params=pltpu.CompilerParams(vmem_limit_bytes=mebibytes << 20),
    )


def shaped(*shape, dtype=BF16):
    return jax.ShapeDtypeStruct(shape, dtype)


def swap(value, axis):
    return lax.all_to_all(value, axis, 0, 0, tiled=True)


def split_three(value):
    high = value.astype(BF16).astype(F32)
    rest = value - high
    middle = rest.astype(BF16).astype(F32)
    return high, middle, rest - middle


def stacked_parts(value, rows):
    row = lax.broadcasted_iota(jnp.int32, (rows, value.shape[1]), 0)
    high, middle, low = split_three(value)
    return jnp.where(row == 0, high, jnp.where(row == 1, middle, jnp.where(row == 2, low, 0.0)))


def pack_body(
    w_hbm, img_hbm, prev_hbm, txt_hbm, flag_hbm, out_ref, tail_hbm,
    w_ref, img_ref, prev_ref, txt_ref, flag_ref, tail_ref, sems,
):
    copies = [
        pltpu.make_async_copy(source, target, sems.at[i])
        for i, (source, target) in enumerate(
            (
                (flag_hbm, flag_ref),
                (w_hbm, w_ref),
                (img_hbm, img_ref),
                (prev_hbm, prev_ref),
                (txt_hbm, txt_ref),
            )
        )
    ]
    for copy in copies:
        copy.start()
    copies[0].wait()
    tail_no = jnp.int32(-1)
    for b in range(img_ref.shape[0]):
        tail_no = tail_no + jnp.where(flag_ref[b] == 1, 1, 0)
    tail_ref[0] = tail_no
    tell = pltpu.make_async_copy(tail_ref, tail_hbm, sems.at[len(copies)])
    tell.start()
    for copy in copies[1:]:
        copy.wait()
    kinds, deep, columns = w_ref.shape
    batch, img_rows, width = img_ref.shape
    cores = columns // HD
    img_half = img_rows // cores
    txt_half = txt_ref.shape[1] // cores
    for b in range(batch):
        for c in range(cores):
            to = b * cores + c
            for kind in range(kinds):
                out_ref[to, :deep, kind * HD : (kind + 1) * HD] = w_ref[
                    kind, :, c * HD : (c + 1) * HD
                ]
            at = deep
            for ref in (img_ref, prev_ref):
                out_ref[to, at : at + img_half] = ref[b, c * img_half : (c + 1) * img_half]
                at += img_half
            text = txt_ref[b].astype(F32)[c * txt_half : (c + 1) * txt_half]
            text = jnp.concatenate([text, jnp.zeros((8 - txt_half, width), F32)], axis=0)
            out_ref[to, at : at + 8] = text.astype(BF16)
    tell.wait()


def spread_body(got_ref, out_hbm, block_ref, sems):
    sources = got_ref.shape[0]
    deep = block_ref.shape[0] // sources
    for source in range(sources):
        block_ref[source * deep : (source + 1) * deep] = got_ref[source, :deep]
    copies = [
        pltpu.make_async_copy(block_ref, out_hbm.at[copy], sems.at[copy])
        for copy in range(out_hbm.shape[0])
    ]
    for copy in copies:
        copy.start()
    for copy in copies:
        copy.wait()


def join_body(deep, img_half, txt_half, got_ref, mod_ref, out_ref, prev_ref):
    far = lax.axis_index(FAR)
    sources = got_ref.shape[0]
    width = got_ref.shape[2]
    for source in range(sources):
        out_ref[source * img_half : (source + 1) * img_half] = got_ref[
            source, deep : deep + img_half
        ]
        prev_ref[source * img_half : (source + 1) * img_half] = got_ref[
            source, deep + img_half : deep + 2 * img_half
        ]
    at = deep + 2 * img_half
    texts = [got_ref[source, at : at + 8].astype(F32)[:txt_half] for source in range(sources)]
    vectors = []
    for which in range(2):
        chosen = mod_ref[which, 0:1].astype(F32)
        for b in range(1, mod_ref.shape[1]):
            chosen = jnp.where(far == b, mod_ref[which, b : b + 1].astype(F32), chosen)
        vectors.append(chosen)
    tail = jnp.concatenate(texts + vectors + [jnp.zeros((6, width), F32)], axis=0)
    out_ref[sources * img_half :] = tail.astype(BF16)


def norm_body(x_ref, prev_ref, mod_ref):
    groups, rows, width = x_ref.shape
    vectors = rows - 8
    features = groups * width
    sums = x_ref[0].astype(F32)
    for g in range(1, groups):
        sums = sums + x_ref[g].astype(F32)
    center = jnp.sum(sums, axis=1, keepdims=True) / features
    squares = jnp.square(x_ref[0].astype(F32) - center)
    for g in range(1, groups):
        squares = squares + jnp.square(x_ref[g].astype(F32) - center)
    squares = jnp.sum(squares, axis=1, keepdims=True)
    inv = lax.rsqrt(squares / features + EPS)
    for g in range(groups):
        values = x_ref[g].astype(F32)
        shift = values[vectors : vectors + 1]
        scale = values[vectors + 1 : vectors + 2]
        mod_ref[g] = ((values - center) * inv * (1.0 + scale) + shift).astype(BF16)
    far = lax.axis_index(FAR)
    own = mod_ref.at[lax.axis_index(TP)]
    previous = prev_ref[...].astype(F32)
    numer = jnp.abs(own[: prev_ref.shape[0]].astype(F32) - previous)
    denom = jnp.abs(previous)
    lane = lax.broadcasted_iota(jnp.int32, (1, width), 1)
    line = jnp.where(lane == far, jnp.sum(numer), 0.0)
    line = jnp.where(lane == 4 + far, jnp.sum(denom), line)
    mod_ref[0, vectors:] = stacked_parts(line, 8).astype(BF16)


def project_body(own_ref, other_ref, w_ref, gain_ref, query_ref, pair_ref):
    groups, rows, width = own_ref.shape
    _, sources, deep, columns = w_ref.shape
    near = cores = 2
    ys = near * sources // cores
    per_group = width // deep
    total = jnp.zeros((2 * rows, columns), F32)
    for g in range(groups):
        pieces = []
        for step in range(per_group):
            flat = g * per_group + step
            core = flat % cores
            y = flat // cores % ys
            x = flat // cores // ys
            pieces.append(w_ref[x * near + y % near, y // near * cores + core])
        left = jnp.concatenate([own_ref[g], other_ref[g]], axis=0)
        total = total + jnp.dot(
            left, jnp.concatenate(pieces, axis=0), preferred_element_type=F32
        )
    parts = []
    for kind in range(2):
        part = total[:, kind * HD : (kind + 1) * HD]
        gain = jnp.where(
            lax.axis_index(CORE) == 0, gain_ref[kind : kind + 1, :HD], gain_ref[kind : kind + 1, HD:]
        )
        mean = jnp.mean(jnp.square(part), axis=1, keepdims=True)
        parts.append(part * lax.rsqrt(mean + EPS) * gain)
    query, keyed = parts
    valued = total[:, 2 * HD :].astype(BF16)
    img = query_ref.shape[1]
    for half, ref in enumerate((own_ref, other_ref)):
        at = half * rows
        query_ref[half] = query[at : at + img].astype(BF16)
        carried = ref[0, rows - 8 :, :HD]
        keys = keyed[at : at + rows - 8].astype(BF16)
        for copy in range(pair_ref.shape[0]):
            pair_ref[copy, half, : rows - 8, :HD] = keys
            pair_ref[copy, half, rows - 8 :, :HD] = carried
            pair_ref[copy, half, :, HD:] = valued[at : at + rows]


def attend_body(img_half, txt_half, limit_ref, query_ref, pair_ref, out_ref):
    blocks, halves, rows, _ = pair_ref.shape
    sources = out_ref.shape[0]
    img = sources * img_half
    txt = sources * txt_half
    count = blocks * rows
    far, core = lax.axis_index(FAR), lax.axis_index(CORE)
    query = query_ref[...].reshape(2 * img, HD)
    index = lax.broadcasted_iota(jnp.int32, (1, count), 1)
    slot = index % rows
    block = index // rows
    source = (slot - img) // txt_half
    y = source // 2 * 2 + block % 2
    device = (block // 2 * 8 + y) * 2 + source % 2
    scores_of, valid_of = [], []
    rel = jnp.zeros((1, HD), F32)
    for half in range(halves):
        actual = jnp.where(half == 0, core, 1 - core)
        keys = pair_ref[:, half, :, :HD].reshape(count, HD)
        scores = lax.dot_general(
            query, keys, (((1,), (1,)), ((), ())), preferred_element_type=F32
        ) * (1.0 / HD**0.5)
        text = device * 4 + actual * txt_half + (slot - img) % txt_half
        valid = (slot < img) | ((slot < img + txt) & (text < limit_ref[far]))
        scores_of.append(jnp.where(valid, scores, NEG))
        valid_of.append(valid)
        for b in range(blocks):
            carried = pair_ref[b, half, rows - 8 :, :HD].astype(F32)
            rel = rel + jnp.sum(carried, axis=0, keepdims=True)
    top = functools.reduce(
        jnp.maximum, [jnp.max(s, axis=1, keepdims=True) for s in scores_of]
    )
    total = jnp.zeros((2 * img, 1), F32)
    summed = jnp.zeros((2 * img, HD), F32)
    for half in range(halves):
        weights = jnp.where(valid_of[half], jnp.exp(scores_of[half] - top), 0.0)
        total = total + jnp.sum(weights, axis=1, keepdims=True)
        values = pair_ref[:, half, :, HD:].reshape(count, HD)
        summed = summed + jnp.dot(weights.astype(BF16), values, preferred_element_type=F32)
    attended = (summed / total).astype(BF16)
    tail = stacked_parts(rel, 8).astype(BF16)
    for half in range(halves):
        actual = jnp.where(half == 0, core, 1 - core)
        at = pl.multiple_of(actual * img_half, img_half)
        for source in range(sources):
            start = half * img + source * img_half
            out_ref[source, pl.ds(at, img_half)] = attended[start : start + img_half]
    for source in range(sources):
        out_ref[source, 2 * img_half :] = tail


def slots_of(flag_ref, batch, count):
    order = [jnp.int32(0)] * count
    seen = jnp.int32(0)
    slot = []
    for b in range(batch):
        on = flag_ref[b] == 1
        slot.append(seen)
        for i in range(count):
            order[i] = jnp.where(on & (seen == i), jnp.int32(b), order[i])
        seen = seen + jnp.where(on, 1, 0)
    return order, slot


def mix_body(img_rows, flag_ref, att_ref, w_ref, out_ref):
    groups, rows, width = out_ref.shape
    heads = w_ref.shape[0] // HD
    batch = att_ref.shape[0] // heads
    slots = (rows - 8) // img_rows
    order, _ = slots_of(flag_ref, batch, slots)
    lefts = []
    for h in range(heads):
        lefts.append(
            jnp.concatenate([att_ref[order[i] * heads + h, :img_rows] for i in range(slots)], axis=0)
        )
    left = jnp.concatenate(lefts, axis=1)
    rel = jnp.zeros((8, HD), F32)
    for b in range(batch):
        rel = rel + att_ref[b * heads, img_rows:].astype(F32)
    tail = stacked_parts(jnp.sum(rel, axis=0, keepdims=True), 8)
    tail = jnp.concatenate([tail, jnp.zeros((8, width - HD), F32)], axis=1).astype(BF16)
    for g in range(groups):
        mixed = jnp.dot(left, w_ref[:, g * width : (g + 1) * width], preferred_element_type=F32)
        out_ref[g, : rows - 8] = mixed.astype(BF16)
        out_ref[g, rows - 8 :] = tail


def final_body(flag_ref, part_ref, cache_ref, img_ref, mod_ref, out_ref, new_ref, rel_ref, sum_ref):
    groups, rows, _ = part_ref.shape
    batch, img_rows, _ = img_ref.shape
    slots = (rows - 8) // img_rows
    mixed = part_ref[0].astype(F32)
    for g in range(1, groups):
        mixed = mixed + part_ref[g].astype(F32)
    sum_ref[...] = mixed
    _, slot = slots_of(flag_ref, batch, slots)
    for b in range(batch):
        gate = mod_ref[2, b : b + 1].astype(F32)
        at = pl.multiple_of(jnp.minimum(slot[b], slots - 1) * img_rows, img_rows)
        resid = gate * sum_ref[pl.ds(at, img_rows)]
        fresh = jnp.where(flag_ref[b] == 1, resid, cache_ref[b])
        new_ref[b] = fresh
        out_ref[b] = img_ref[b].astype(F32) + fresh
    sums = jnp.sum(mixed[rows - 8 :, :HD], axis=0, keepdims=True)
    lane = lax.broadcasted_iota(jnp.int32, (1, HD), 1)
    for b in range(batch):
        numer = jnp.sum(jnp.where(lane == b, sums, 0.0))
        denom = jnp.sum(jnp.where(lane == 4 + b, sums, 0.0))
        rel_ref[b] = numer / jnp.maximum(denom, 1.0)


def local(img, txt, prev_mod, cache, modulation, w_qkv, qk_gain, output_weight, text_len, refresh):
    batch, img_rows, width = img.shape
    xs, fars, nears, cores = (lax.axis_size(a) for a in SEQ)
    tps = lax.axis_size(TP)
    deep, kinds, _ = w_qkv.shape
    sources = fars * cores
    around = xs * nears
    img_half, txt_half = img_rows // cores, txt.shape[1] // cores
    rows = sources * (img_half + txt_half) + 8
    arrays = (w_qkv.transpose(1, 0, 2), img, prev_mod, txt)
    smem = lambda *shape: pltpu.SMEM(shape, jnp.int32)
    got, tail_no = call(
        pack_body,
        (
            shaped(sources, deep + 2 * img_half + 8, width),
            pltpu.HBM((1,), jnp.int32),
        ),
        [HBM] * 5,
        8,
        outs=(VMEM, HBM),
        scratch=[pltpu.VMEM(a.shape, a.dtype) for a in arrays]
        + [smem(batch), smem(1), pltpu.SemaphoreType.DMA((len(arrays) + 2,))],
    )(*(pltpu.with_memory_space_constraint(a, pltpu.HBM) for a in arrays + (refresh,)))
    got = swap(got, (FAR, CORE))
    weight = call(
        spread_body,
        pltpu.HBM((around, sources * deep, kinds * HD), BF16),
        [VMEM],
        8,
        outs=HBM,
        scratch=[
            pltpu.VMEM((sources * deep, kinds * HD), BF16),
            pltpu.SemaphoreType.DMA((around,)),
        ],
    )(got)
    weight = swap(weight, (X, NEAR)).reshape(around, sources, deep, kinds * HD)

    joined, previous = call(
        functools.partial(join_body, deep, img_half, txt_half),
        (shaped(rows, width), shaped(sources * img_half, width)),
        [VMEM] * 2,
        8,
    )(got, modulation)
    wide = lax.all_gather(joined, TP, axis=0, tiled=False)
    own = call(norm_body, shaped(tps, rows, width), [VMEM] * 2, 12)(wide, previous)
    other = lax.ppermute(own, CORE, [(0, 1), (1, 0)])

    query, pairs = call(
        project_body,
        (shaped(2, sources * img_half, HD), shaped(around, 2, rows, 2 * HD)),
        [VMEM] * 4,
        16,
    )(own, other, weight, qk_gain)
    pairs = swap(pairs, (X, NEAR))
    attended = call(
        functools.partial(attend_body, img_half, txt_half),
        shaped(sources, img_rows + 8, HD),
        [SMEM, VMEM, VMEM],
        24,
    )(text_len, query, pairs)
    attended = swap(attended, (FAR, CORE))

    tails = [functools.partial(finish, slots) for slots in range(1, batch)]
    return lax.switch(tail_no[0], tails, refresh, attended, output_weight, cache, img, modulation)


def finish(slots, refresh, attended, output_weight, cache, img, modulation):
    batch, img_rows, width = img.shape
    rows = slots * img_rows + 8
    parts = call(
        functools.partial(mix_body, img_rows),
        shaped(lax.axis_size(TP), rows, width),
        [SMEM, VMEM, VMEM],
        12,
    )(refresh, attended, output_weight)
    parts = swap(parts, TP)
    whole = shaped(batch, img_rows, width, dtype=F32)
    return call(
        final_body,
        (whole, whole, shaped(batch, dtype=F32)),
        [SMEM] + [VMEM] * 4,
        8,
        outs=(VMEM, VMEM, SMEM),
        scratch=[pltpu.VMEM((rows, width), F32)],
    )(refresh, parts, cache, img, modulation)


def solution(mesh):
    finer = Mesh(mesh.devices.reshape(4, 4, 2, 2, mesh.shape["tp"]), SEQ + (TP,))
    in_specs = (
        P(None, SEQ, TP),
        P(None, SEQ, TP),
        P(None, SEQ, TP),
        P(None, SEQ, TP),
        P(None, None, TP),
        P(SEQ, None, TP),
        P(None, TP),
        P(TP, None),
        P(),
        P(),
    )
    out_specs = (P(None, SEQ, TP), P(None, SEQ, TP), P())

    return jax.shard_map(local, mesh=finer, in_specs=in_specs, out_specs=out_specs, check_vma=False)
```

```python
import functools

import jax
import jax.numpy as jnp
from jax import lax
from jax.experimental import pallas as pl
from jax.experimental.pallas import tpu as pltpu
from jax.sharding import Mesh
from jax.sharding import PartitionSpec as P


X, FAR, NEAR, CORE, TP = "seq_0", "seq_1a", "seq_1b", "seq_2", "tp"
SEQ = (X, FAR, NEAR, CORE)
HD = 128
EPS = 0.1
NEG = -1e30
F32 = jnp.float32
BF16 = jnp.bfloat16

VMEM = pl.BlockSpec(memory_space=pltpu.VMEM)
SMEM = pl.BlockSpec(memory_space=pltpu.SMEM)
HBM = pl.BlockSpec(memory_space=pltpu.HBM)


def call(body, out_shape, in_specs, mebibytes, outs=None, scratch=()):
    outs = outs or jax.tree.map(lambda _: VMEM, out_shape)
    return pl.pallas_call(
        body,
        out_shape=out_shape,
        in_specs=in_specs,
        out_specs=outs,
        scratch_shapes=scratch,
        compiler_params=pltpu.CompilerParams(vmem_limit_bytes=mebibytes << 20),
    )


def shaped(*shape, dtype=BF16):
    return jax.ShapeDtypeStruct(shape, dtype)


def swap(value, axis):
    return lax.all_to_all(value, axis, 0, 0, tiled=True)


def split_three(value):
    high = value.astype(BF16).astype(F32)
    rest = value - high
    middle = rest.astype(BF16).astype(F32)
    return high, middle, rest - middle


def stacked_parts(value, rows):
    row = lax.broadcasted_iota(jnp.int32, (rows, value.shape[1]), 0)
    high, middle, low = split_three(value)
    return jnp.where(row == 0, high, jnp.where(row == 1, middle, jnp.where(row == 2, low, 0.0)))


def pack_body(
    w_hbm, img_hbm, prev_hbm, txt_hbm, flag_hbm, out_ref, tail_hbm,
    w_ref, img_ref, prev_ref, txt_ref, flag_ref, tail_ref, sems,
):
    copies = [
        pltpu.make_async_copy(source, target, sems.at[i])
        for i, (source, target) in enumerate(
            (
                (flag_hbm, flag_ref),
                (w_hbm, w_ref),
                (img_hbm, img_ref),
                (prev_hbm, prev_ref),
                (txt_hbm, txt_ref),
            )
        )
    ]
    for copy in copies:
        copy.start()
    copies[0].wait()
    tail_no = jnp.int32(-1)
    for b in range(img_ref.shape[0]):
        tail_no = tail_no + jnp.where(flag_ref[b] == 1, 1, 0)
    tail_ref[0] = tail_no
    tell = pltpu.make_async_copy(tail_ref, tail_hbm, sems.at[len(copies)])
    tell.start()
    for copy in copies[1:]:
        copy.wait()
    kinds, deep, columns = w_ref.shape
    batch, img_rows, width = img_ref.shape
    cores = columns // HD
    img_half = img_rows // cores
    txt_half = txt_ref.shape[1] // cores
    for b in range(batch):
        for c in range(cores):
            to = b * cores + c
            for kind in range(kinds):
                out_ref[to, :deep, kind * HD : (kind + 1) * HD] = w_ref[
                    kind, :, c * HD : (c + 1) * HD
                ]
            at = deep
            for ref in (img_ref, prev_ref):
                out_ref[to, at : at + img_half] = ref[b, c * img_half : (c + 1) * img_half]
                at += img_half
            text = txt_ref[b].astype(F32)[c * txt_half : (c + 1) * txt_half]
            text = jnp.concatenate([text, jnp.zeros((8 - txt_half, width), F32)], axis=0)
            out_ref[to, at : at + 8] = text.astype(BF16)
    tell.wait()


def spread_body(got_ref, out_hbm, block_ref, sems):
    sources = got_ref.shape[0]
    deep = block_ref.shape[0] // sources
    for source in range(sources):
        block_ref[source * deep : (source + 1) * deep] = got_ref[source, :deep]
    copies = [
        pltpu.make_async_copy(block_ref, out_hbm.at[copy], sems.at[copy])
        for copy in range(out_hbm.shape[0])
    ]
    for copy in copies:
        copy.start()
    for copy in copies:
        copy.wait()


def join_body(deep, img_half, txt_half, got_ref, mod_ref, out_ref, prev_ref):
    far = lax.axis_index(FAR)
    sources = got_ref.shape[0]
    width = got_ref.shape[2]
    for source in range(sources):
        out_ref[source * img_half : (source + 1) * img_half] = got_ref[
            source, deep : deep + img_half
        ]
        prev_ref[source * img_half : (source + 1) * img_half] = got_ref[
            source, deep + img_half : deep + 2 * img_half
        ]
    at = deep + 2 * img_half
    texts = [got_ref[source, at : at + 8].astype(F32)[:txt_half] for source in range(sources)]
    vectors = []
    for which in range(2):
        chosen = mod_ref[which, 0:1].astype(F32)
        for b in range(1, mod_ref.shape[1]):
            chosen = jnp.where(far == b, mod_ref[which, b : b + 1].astype(F32), chosen)
        vectors.append(chosen)
    tail = jnp.concatenate(texts + vectors + [jnp.zeros((6, width), F32)], axis=0)
    out_ref[sources * img_half :] = tail.astype(BF16)


def norm_body(x_ref, prev_ref, mod_ref):
    groups, rows, width = x_ref.shape
    vectors = rows - 8
    features = groups * width
    sums = x_ref[0].astype(F32)
    for g in range(1, groups):
        sums = sums + x_ref[g].astype(F32)
    center = jnp.sum(sums, axis=1, keepdims=True) / features
    squares = jnp.square(x_ref[0].astype(F32) - center)
    for g in range(1, groups):
        squares = squares + jnp.square(x_ref[g].astype(F32) - center)
    squares = jnp.sum(squares, axis=1, keepdims=True)
    inv = lax.rsqrt(squares / features + EPS)
    for g in range(groups):
        values = x_ref[g].astype(F32)
        shift = values[vectors : vectors + 1]
        scale = values[vectors + 1 : vectors + 2]
        mod_ref[g] = ((values - center) * inv * (1.0 + scale) + shift).astype(BF16)
    far = lax.axis_index(FAR)
    own = mod_ref.at[lax.axis_index(TP)]
    previous = prev_ref[...].astype(F32)
    numer = jnp.abs(own[: prev_ref.shape[0]].astype(F32) - previous)
    denom = jnp.abs(previous)
    lane = lax.broadcasted_iota(jnp.int32, (1, width), 1)
    line = jnp.where(lane == far, jnp.sum(numer), 0.0)
    line = jnp.where(lane == 4 + far, jnp.sum(denom), line)
    mod_ref[0, vectors:] = stacked_parts(line, 8).astype(BF16)


def project_body(own_ref, other_ref, w_ref, gain_ref, query_ref, pair_ref):
    groups, rows, width = own_ref.shape
    _, sources, deep, columns = w_ref.shape
    near = cores = 2
    xs = w_ref.shape[0] // near
    ys = near * sources // cores
    per_group = width // deep
    total = jnp.zeros((2 * rows, columns), F32)
    for g in range(groups):
        pieces = []
        for step in range(per_group):
            flat = g * per_group + step
            core = flat % cores
            y = flat // cores % ys
            x = flat // cores // ys
            pieces.append(w_ref[y % near * xs + x, y // near * cores + core])
        left = jnp.concatenate([own_ref[g], other_ref[g]], axis=0)
        total = total + jnp.dot(
            left, jnp.concatenate(pieces, axis=0), preferred_element_type=F32
        )
    parts = []
    for kind in range(2):
        part = total[:, kind * HD : (kind + 1) * HD]
        gain = jnp.where(
            lax.axis_index(CORE) == 0, gain_ref[kind : kind + 1, :HD], gain_ref[kind : kind + 1, HD:]
        )
        mean = jnp.mean(jnp.square(part), axis=1, keepdims=True)
        parts.append(part * lax.rsqrt(mean + EPS) * gain)
    query, keyed = parts
    valued = total[:, 2 * HD :].astype(BF16)
    img = query_ref.shape[1]
    for half, ref in enumerate((own_ref, other_ref)):
        at = half * rows
        query_ref[half] = query[at : at + img].astype(BF16)
        carried = ref[0, rows - 8 :, :HD]
        keys = keyed[at : at + rows - 8].astype(BF16)
        for copy in range(pair_ref.shape[0]):
            pair_ref[copy, half, : rows - 8, :HD] = keys
            pair_ref[copy, half, rows - 8 :, :HD] = carried
            pair_ref[copy, half, :, HD:] = valued[at : at + rows]


def attend_body(img_half, txt_half, limit_ref, query_ref, pair_ref, out_ref):
    blocks, halves, rows, _ = pair_ref.shape
    sources = out_ref.shape[0]
    img = sources * img_half
    txt = sources * txt_half
    count = blocks * rows
    far, core = lax.axis_index(FAR), lax.axis_index(CORE)
    query = query_ref[...].reshape(2 * img, HD)
    index = lax.broadcasted_iota(jnp.int32, (1, count), 1)
    slot = index % rows
    block = index // rows
    source = (slot - img) // txt_half
    y = source // 2 * 2 + block // 4
    device = (block % 4 * 8 + y) * 2 + source % 2
    scores_of, valid_of = [], []
    rel = jnp.zeros((1, HD), F32)
    for half in range(halves):
        actual = jnp.where(half == 0, core, 1 - core)
        keys = pair_ref[:, half, :, :HD].reshape(count, HD)
        scores = lax.dot_general(
            query, keys, (((1,), (1,)), ((), ())), preferred_element_type=F32
        ) * (1.0 / HD**0.5)
        text = device * 4 + actual * txt_half + (slot - img) % txt_half
        valid = (slot < img) | ((slot < img + txt) & (text < limit_ref[far]))
        scores_of.append(jnp.where(valid, scores, NEG))
        valid_of.append(valid)
        for b in range(blocks):
            carried = pair_ref[b, half, rows - 8 :, :HD].astype(F32)
            rel = rel + jnp.sum(carried, axis=0, keepdims=True)
    top = functools.reduce(
        jnp.maximum, [jnp.max(s, axis=1, keepdims=True) for s in scores_of]
    )
    total = jnp.zeros((2 * img, 1), F32)
    summed = jnp.zeros((2 * img, HD), F32)
    for half in range(halves):
        weights = jnp.where(valid_of[half], jnp.exp(scores_of[half] - top), 0.0)
        total = total + jnp.sum(weights, axis=1, keepdims=True)
        values = pair_ref[:, half, :, HD:].reshape(count, HD)
        summed = summed + jnp.dot(weights.astype(BF16), values, preferred_element_type=F32)
    attended = (summed / total).astype(BF16)
    tail = stacked_parts(rel, 8).astype(BF16)
    for half in range(halves):
        actual = jnp.where(half == 0, core, 1 - core)
        at = pl.multiple_of(actual * img_half, img_half)
        for source in range(sources):
            start = half * img + source * img_half
            out_ref[source, pl.ds(at, img_half)] = attended[start : start + img_half]
    for source in range(sources):
        out_ref[source, 2 * img_half :] = tail


def slots_of(flag_ref, batch, count):
    order = [jnp.int32(0)] * count
    seen = jnp.int32(0)
    slot = []
    for b in range(batch):
        on = flag_ref[b] == 1
        slot.append(seen)
        for i in range(count):
            order[i] = jnp.where(on & (seen == i), jnp.int32(b), order[i])
        seen = seen + jnp.where(on, 1, 0)
    return order, slot


def mix_body(img_rows, flag_ref, att_ref, w_ref, out_ref):
    groups, rows, width = out_ref.shape
    heads = w_ref.shape[0] // HD
    batch = att_ref.shape[0] // heads
    slots = (rows - 8) // img_rows
    order, _ = slots_of(flag_ref, batch, slots)
    lefts = []
    for h in range(heads):
        lefts.append(
            jnp.concatenate([att_ref[order[i] * heads + h, :img_rows] for i in range(slots)], axis=0)
        )
    left = jnp.concatenate(lefts, axis=1)
    rel = jnp.zeros((8, HD), F32)
    for b in range(batch):
        rel = rel + att_ref[b * heads, img_rows:].astype(F32)
    tail = stacked_parts(jnp.sum(rel, axis=0, keepdims=True), 8)
    tail = jnp.concatenate([tail, jnp.zeros((8, width - HD), F32)], axis=1).astype(BF16)
    for g in range(groups):
        mixed = jnp.dot(left, w_ref[:, g * width : (g + 1) * width], preferred_element_type=F32)
        out_ref[g, : rows - 8] = mixed.astype(BF16)
        out_ref[g, rows - 8 :] = tail


def final_body(flag_ref, part_ref, cache_ref, img_ref, mod_ref, out_ref, new_ref, rel_ref, sum_ref):
    groups, rows, _ = part_ref.shape
    batch, img_rows, _ = img_ref.shape
    slots = (rows - 8) // img_rows
    mixed = part_ref[0].astype(F32)
    for g in range(1, groups):
        mixed = mixed + part_ref[g].astype(F32)
    sum_ref[...] = mixed
    _, slot = slots_of(flag_ref, batch, slots)
    for b in range(batch):
        gate = mod_ref[2, b : b + 1].astype(F32)
        at = pl.multiple_of(jnp.minimum(slot[b], slots - 1) * img_rows, img_rows)
        resid = gate * sum_ref[pl.ds(at, img_rows)]
        fresh = jnp.where(flag_ref[b] == 1, resid, cache_ref[b])
        new_ref[b] = fresh
        out_ref[b] = img_ref[b].astype(F32) + fresh
    sums = jnp.sum(mixed[rows - 8 :, :HD], axis=0, keepdims=True)
    lane = lax.broadcasted_iota(jnp.int32, (1, HD), 1)
    for b in range(batch):
        numer = jnp.sum(jnp.where(lane == b, sums, 0.0))
        denom = jnp.sum(jnp.where(lane == 4 + b, sums, 0.0))
        rel_ref[b] = numer / jnp.maximum(denom, 1.0)


def local(img, txt, prev_mod, cache, modulation, w_qkv, qk_gain, output_weight, text_len, refresh):
    batch, img_rows, width = img.shape
    xs, fars, nears, cores = (lax.axis_size(a) for a in SEQ)
    tps = lax.axis_size(TP)
    deep, kinds, _ = w_qkv.shape
    sources = fars * cores
    around = xs * nears
    img_half, txt_half = img_rows // cores, txt.shape[1] // cores
    rows = sources * (img_half + txt_half) + 8
    arrays = (w_qkv.transpose(1, 0, 2), img, prev_mod, txt)
    smem = lambda *shape: pltpu.SMEM(shape, jnp.int32)
    got, tail_no = call(
        pack_body,
        (
            shaped(sources, deep + 2 * img_half + 8, width),
            pltpu.HBM((1,), jnp.int32),
        ),
        [HBM] * 5,
        8,
        outs=(VMEM, HBM),
        scratch=[pltpu.VMEM(a.shape, a.dtype) for a in arrays]
        + [smem(batch), smem(1), pltpu.SemaphoreType.DMA((len(arrays) + 2,))],
    )(*(pltpu.with_memory_space_constraint(a, pltpu.HBM) for a in arrays + (refresh,)))
    got = swap(got, (FAR, CORE))
    weight = call(
        spread_body,
        pltpu.HBM((around, sources * deep, kinds * HD), BF16),
        [VMEM],
        8,
        outs=HBM,
        scratch=[
            pltpu.VMEM((sources * deep, kinds * HD), BF16),
            pltpu.SemaphoreType.DMA((around,)),
        ],
    )(got)
    weight = swap(weight, (NEAR, X)).reshape(around, sources, deep, kinds * HD)

    joined, previous = call(
        functools.partial(join_body, deep, img_half, txt_half),
        (shaped(rows, width), shaped(sources * img_half, width)),
        [VMEM] * 2,
        8,
    )(got, modulation)
    wide = lax.all_gather(joined, TP, axis=0, tiled=False)
    own = call(norm_body, shaped(tps, rows, width), [VMEM] * 2, 12)(wide, previous)
    other = lax.ppermute(own, CORE, [(0, 1), (1, 0)])

    query, pairs = call(
        project_body,
        (shaped(2, sources * img_half, HD), shaped(around, 2, rows, 2 * HD)),
        [VMEM] * 4,
        16,
    )(own, other, weight, qk_gain)
    pairs = swap(pairs, (NEAR, X))
    attended = call(
        functools.partial(attend_body, img_half, txt_half),
        shaped(sources, img_rows + 8, HD),
        [SMEM, VMEM, VMEM],
        24,
    )(text_len, query, pairs)
    attended = swap(attended, (FAR, CORE))

    tails = [functools.partial(finish, slots) for slots in range(1, batch)]
    return lax.switch(tail_no[0], tails, refresh, attended, output_weight, cache, img, modulation)


def finish(slots, refresh, attended, output_weight, cache, img, modulation):
    batch, img_rows, width = img.shape
    rows = slots * img_rows + 8
    parts = call(
        functools.partial(mix_body, img_rows),
        shaped(lax.axis_size(TP), rows, width),
        [SMEM, VMEM, VMEM],
        12,
    )(refresh, attended, output_weight)
    parts = swap(parts, TP)
    whole = shaped(batch, img_rows, width, dtype=F32)
    return call(
        final_body,
        (whole, whole, shaped(batch, dtype=F32)),
        [SMEM] + [VMEM] * 4,
        8,
        outs=(VMEM, VMEM, SMEM),
        scratch=[pltpu.VMEM((rows, width), F32)],
    )(refresh, parts, cache, img, modulation)


def solution(mesh):
    finer = Mesh(mesh.devices.reshape(4, 4, 2, 2, mesh.shape["tp"]), SEQ + (TP,))
    in_specs = (
        P(None, SEQ, TP),
        P(None, SEQ, TP),
        P(None, SEQ, TP),
        P(None, SEQ, TP),
        P(None, None, TP),
        P(SEQ, None, TP),
        P(None, TP),
        P(TP, None),
        P(),
        P(),
    )
    out_specs = (P(None, SEQ, TP), P(None, SEQ, TP), P())

    return jax.shard_map(local, mesh=finer, in_specs=in_specs, out_specs=out_specs, check_vma=False)
```

```python
import functools
import math

import jax
import jax.numpy as jnp
from jax import lax
from jax.experimental import pallas as pl
from jax.experimental.pallas import tpu as pltpu
from jax.sharding import Mesh
from jax.sharding import PartitionSpec as P


X, FAR, NEAR, CORE, TP = "seq_0", "seq_1a", "seq_1b", "seq_2", "tp"
SEQ = (X, FAR, NEAR, CORE)
HD = 128
EPS = 0.1
NEG = -1e30
F32 = jnp.float32
BF16 = jnp.bfloat16

VMEM = pl.BlockSpec(memory_space=pltpu.VMEM)
SMEM = pl.BlockSpec(memory_space=pltpu.SMEM)
HBM = pl.BlockSpec(memory_space=pltpu.HBM)


def call(body, out_shape, in_specs, mebibytes, outs=None, scratch=()):
    outs = outs or jax.tree.map(lambda _: VMEM, out_shape)
    return pl.pallas_call(
        body,
        out_shape=out_shape,
        in_specs=in_specs,
        out_specs=outs,
        scratch_shapes=scratch,
        compiler_params=pltpu.CompilerParams(vmem_limit_bytes=mebibytes << 20),
    )


def shaped(*shape, dtype=BF16):
    return jax.ShapeDtypeStruct(shape, dtype)


def swap(value, axis):
    return lax.all_to_all(value, axis, 0, 0, tiled=True)


def split_three(value):
    high = value.astype(BF16).astype(F32)
    rest = value - high
    middle = rest.astype(BF16).astype(F32)
    return high, middle, rest - middle


def stacked_parts(value, rows):
    row = lax.broadcasted_iota(jnp.int32, (rows, value.shape[1]), 0)
    high, middle, low = split_three(value)
    return jnp.where(row == 0, high, jnp.where(row == 1, middle, jnp.where(row == 2, low, 0.0)))


def pack_body(
    w_hbm, img_hbm, prev_hbm, txt_hbm, flag_hbm, out_ref, tail_hbm,
    w_ref, img_ref, prev_ref, txt_ref, flag_ref, tail_ref, sems,
):
    copies = [
        pltpu.make_async_copy(source, target, sems.at[i])
        for i, (source, target) in enumerate(
            (
                (flag_hbm, flag_ref),
                (w_hbm, w_ref),
                (img_hbm, img_ref),
                (prev_hbm, prev_ref),
                (txt_hbm, txt_ref),
            )
        )
    ]
    for copy in copies:
        copy.start()
    copies[0].wait()
    tail_no = jnp.int32(-1)
    for b in range(img_ref.shape[0]):
        tail_no = tail_no + jnp.where(flag_ref[b] == 1, 1, 0)
    tail_ref[0] = tail_no
    tell = pltpu.make_async_copy(tail_ref, tail_hbm, sems.at[len(copies)])
    tell.start()
    for copy in copies[1:]:
        copy.wait()
    kinds, deep, columns = w_ref.shape
    batch, img_rows, width = img_ref.shape
    cores = columns // HD
    img_half = img_rows // cores
    txt_half = txt_ref.shape[1] // cores
    for b in range(batch):
        for c in range(cores):
            to = b * cores + c
            for kind in range(kinds):
                out_ref[to, :deep, kind * HD : (kind + 1) * HD] = w_ref[
                    kind, :, c * HD : (c + 1) * HD
                ]
            at = deep
            for ref in (img_ref, prev_ref):
                out_ref[to, at : at + img_half] = ref[b, c * img_half : (c + 1) * img_half]
                at += img_half
            text = txt_ref[b].astype(F32)[c * txt_half : (c + 1) * txt_half]
            text = jnp.concatenate([text, jnp.zeros((8 - txt_half, width), F32)], axis=0)
            out_ref[to, at : at + 8] = text.astype(BF16)
    tell.wait()


def spread_body(got_ref, out_hbm, block_ref, sems):
    sources = got_ref.shape[0]
    deep = block_ref.shape[0] // sources
    for source in range(sources):
        block_ref[source * deep : (source + 1) * deep] = got_ref[source, :deep]
    copies = [
        pltpu.make_async_copy(block_ref, out_hbm.at[copy], sems.at[copy])
        for copy in range(out_hbm.shape[0])
    ]
    for copy in copies:
        copy.start()
    for copy in copies:
        copy.wait()


def join_body(deep, img_half, txt_half, got_ref, mod_ref, out_ref, prev_ref):
    far = lax.axis_index(FAR)
    sources = got_ref.shape[0]
    width = got_ref.shape[2]
    for source in range(sources):
        out_ref[source * img_half : (source + 1) * img_half] = got_ref[
            source, deep : deep + img_half
        ]
        prev_ref[source * img_half : (source + 1) * img_half] = got_ref[
            source, deep + img_half : deep + 2 * img_half
        ]
    at = deep + 2 * img_half
    texts = [got_ref[source, at : at + 8].astype(F32)[:txt_half] for source in range(sources)]
    vectors = []
    for which in range(2):
        chosen = mod_ref[which, 0:1].astype(F32)
        for b in range(1, mod_ref.shape[1]):
            chosen = jnp.where(far == b, mod_ref[which, b : b + 1].astype(F32), chosen)
        vectors.append(chosen)
    tail = jnp.concatenate(texts + vectors + [jnp.zeros((6, width), F32)], axis=0)
    out_ref[sources * img_half :] = tail.astype(BF16)


def norm_body(x_ref, prev_ref, mod_ref):
    groups, rows, width = x_ref.shape
    vectors = rows - 8
    features = groups * width
    sums = x_ref[0].astype(F32)
    for g in range(1, groups):
        sums = sums + x_ref[g].astype(F32)
    center = jnp.sum(sums, axis=1, keepdims=True) / features
    squares = jnp.square(x_ref[0].astype(F32) - center)
    for g in range(1, groups):
        squares = squares + jnp.square(x_ref[g].astype(F32) - center)
    squares = jnp.sum(squares, axis=1, keepdims=True)
    inv = lax.rsqrt(squares / features + EPS)
    for g in range(groups):
        values = x_ref[g].astype(F32)
        shift = values[vectors : vectors + 1]
        scale = values[vectors + 1 : vectors + 2]
        mod_ref[g] = ((values - center) * inv * (1.0 + scale) + shift).astype(BF16)
    far = lax.axis_index(FAR)
    own = mod_ref.at[lax.axis_index(TP)]
    previous = prev_ref[...].astype(F32)
    numer = jnp.abs(own[: prev_ref.shape[0]].astype(F32) - previous)
    denom = jnp.abs(previous)
    lane = lax.broadcasted_iota(jnp.int32, (1, width), 1)
    line = jnp.where(lane == far, jnp.sum(numer), 0.0)
    line = jnp.where(lane == 4 + far, jnp.sum(denom), line)
    mod_ref[0, vectors:] = stacked_parts(line, 8).astype(BF16)


def project_body(own_ref, other_ref, w_ref, gain_ref, query_ref, pair_ref):
    groups, rows, width = own_ref.shape
    _, sources, deep, columns = w_ref.shape
    near = cores = 2
    xs = w_ref.shape[0] // near
    ys = near * sources // cores
    per_group = width // deep
    total = jnp.zeros((2 * rows, columns), F32)
    for g in range(groups):
        pieces = []
        for step in range(per_group):
            flat = g * per_group + step
            core = flat % cores
            y = flat // cores % ys
            x = flat // cores // ys
            pieces.append(w_ref[y % near * xs + x, y // near * cores + core])
        left = jnp.concatenate([own_ref[g], other_ref[g]], axis=0)
        total = total + jnp.dot(
            left, jnp.concatenate(pieces, axis=0), preferred_element_type=F32
        )
    parts = []
    for kind in range(2):
        part = total[:, kind * HD : (kind + 1) * HD]
        gain = jnp.where(
            lax.axis_index(CORE) == 0, gain_ref[kind : kind + 1, :HD], gain_ref[kind : kind + 1, HD:]
        )
        mean = jnp.mean(jnp.square(part), axis=1, keepdims=True)
        parts.append(part * lax.rsqrt(mean + EPS) * gain)
    query, keyed = parts
    valued = total[:, 2 * HD :].astype(BF16)
    img = query_ref.shape[1]
    for half, ref in enumerate((own_ref, other_ref)):
        at = half * rows
        query_ref[half] = query[at : at + img].astype(BF16)
        carried = ref[0, rows - 8 :, :HD]
        keys = keyed[at : at + rows - 8].astype(BF16)
        for copy in range(pair_ref.shape[0]):
            pair_ref[copy, half, : rows - 8, :HD] = keys
            pair_ref[copy, half, rows - 8 :, :HD] = carried
            pair_ref[copy, half, :, HD:] = valued[at : at + rows]


def attend_body(img_half, txt_half, limit_ref, query_ref, pair_ref, out_ref):
    blocks, halves, rows, _ = pair_ref.shape
    sources = out_ref.shape[0]
    img = sources * img_half
    txt = sources * txt_half
    count = blocks * rows
    far, core = lax.axis_index(FAR), lax.axis_index(CORE)
    query = query_ref[...].reshape(2 * img, HD)
    index = lax.broadcasted_iota(jnp.int32, (1, count), 1)
    slot = index % rows
    block = index // rows
    source = (slot - img) // txt_half
    y = source // 2 * 2 + block // 4
    device = (block % 4 * 8 + y) * 2 + source % 2
    raw_of = []
    rel = jnp.zeros((1, HD), F32)
    for half in range(halves):
        actual = jnp.where(half == 0, core, 1 - core)
        keys = pair_ref[:, half, :, :HD].reshape(count, HD)
        raw = lax.dot_general(
            query, keys, (((1,), (1,)), ((), ())), preferred_element_type=F32
        )
        text = device * 4 + actual * txt_half + (slot - img) % txt_half
        valid = (slot < img) | ((slot < img + txt) & (text < limit_ref[far]))
        raw_of.append(raw + jnp.where(valid, 0.0, NEG))
        for b in range(blocks):
            carried = pair_ref[b, half, rows - 8 :, :HD].astype(F32)
            rel = rel + jnp.sum(carried, axis=0, keepdims=True)
    factor = math.log2(math.e) / HD**0.5
    top = functools.reduce(jnp.maximum, [jnp.max(r, axis=1, keepdims=True) for r in raw_of])
    total = jnp.zeros((2 * img, 1), F32)
    summed = jnp.zeros((2 * img, HD), F32)
    for half in range(halves):
        weights = jnp.exp2((raw_of[half] - top) * factor)
        total = total + jnp.sum(weights, axis=1, keepdims=True)
        values = pair_ref[:, half, :, HD:].reshape(count, HD)
        summed = summed + jnp.dot(weights.astype(BF16), values, preferred_element_type=F32)
    attended = (summed / total).astype(BF16)
    tail = stacked_parts(rel, 8).astype(BF16)
    for half in range(halves):
        actual = jnp.where(half == 0, core, 1 - core)
        at = pl.multiple_of(actual * img_half, img_half)
        for source in range(sources):
            start = half * img + source * img_half
            out_ref[source, pl.ds(at, img_half)] = attended[start : start + img_half]
    for source in range(sources):
        out_ref[source, 2 * img_half :] = tail


def slots_of(flag_ref, batch, count):
    order = [jnp.int32(0)] * count
    seen = jnp.int32(0)
    slot = []
    for b in range(batch):
        on = flag_ref[b] == 1
        slot.append(seen)
        for i in range(count):
            order[i] = jnp.where(on & (seen == i), jnp.int32(b), order[i])
        seen = seen + jnp.where(on, 1, 0)
    return order, slot


def mix_body(img_rows, flag_ref, att_ref, w_ref, out_ref):
    groups, rows, width = out_ref.shape
    heads = w_ref.shape[0] // HD
    batch = att_ref.shape[0] // heads
    slots = (rows - 8) // img_rows
    order, _ = slots_of(flag_ref, batch, slots)
    lefts = []
    for h in range(heads):
        lefts.append(
            jnp.concatenate([att_ref[order[i] * heads + h, :img_rows] for i in range(slots)], axis=0)
        )
    left = jnp.concatenate(lefts, axis=1)
    rel = jnp.zeros((8, HD), F32)
    for b in range(batch):
        rel = rel + att_ref[b * heads, img_rows:].astype(F32)
    tail = stacked_parts(jnp.sum(rel, axis=0, keepdims=True), 8)
    tail = jnp.concatenate([tail, jnp.zeros((8, width - HD), F32)], axis=1).astype(BF16)
    for g in range(groups):
        mixed = jnp.dot(left, w_ref[:, g * width : (g + 1) * width], preferred_element_type=F32)
        out_ref[g, : rows - 8] = mixed.astype(BF16)
        out_ref[g, rows - 8 :] = tail


def final_body(
    flag_ref, part_ref, cache_ref, img_ref, mod_ref, out_hbm, new_hbm, rel_ref,
    sum_ref, out_ref, new_ref, sems,
):
    groups, rows, _ = part_ref.shape
    batch, img_rows, _ = img_ref.shape
    slots = (rows - 8) // img_rows
    mixed = part_ref[0].astype(F32)
    for g in range(1, groups):
        mixed = mixed + part_ref[g].astype(F32)
    sum_ref[...] = mixed
    _, slot = slots_of(flag_ref, batch, slots)
    copies = []
    for b in range(batch):
        gate = mod_ref[2, b : b + 1].astype(F32)
        at = pl.multiple_of(jnp.minimum(slot[b], slots - 1) * img_rows, img_rows)
        resid = gate * sum_ref[pl.ds(at, img_rows)]
        fresh = jnp.where(flag_ref[b] == 1, resid, cache_ref[b])
        new_ref[b] = fresh
        out_ref[b] = img_ref[b].astype(F32) + fresh
        for i, (source, target) in enumerate(((new_ref, new_hbm), (out_ref, out_hbm))):
            copies.append(pltpu.make_async_copy(source.at[b], target.at[b], sems.at[i, b]))
            copies[-1].start()
    sums = jnp.sum(mixed[rows - 8 :, :HD], axis=0, keepdims=True)
    lane = lax.broadcasted_iota(jnp.int32, (1, HD), 1)
    for b in range(batch):
        numer = jnp.sum(jnp.where(lane == b, sums, 0.0))
        denom = jnp.sum(jnp.where(lane == 4 + b, sums, 0.0))
        rel_ref[b] = numer / jnp.maximum(denom, 1.0)
    for copy in copies:
        copy.wait()


def local(img, txt, prev_mod, cache, modulation, w_qkv, qk_gain, output_weight, text_len, refresh):
    batch, img_rows, width = img.shape
    xs, fars, nears, cores = (lax.axis_size(a) for a in SEQ)
    tps = lax.axis_size(TP)
    deep, kinds, _ = w_qkv.shape
    sources = fars * cores
    around = xs * nears
    img_half, txt_half = img_rows // cores, txt.shape[1] // cores
    rows = sources * (img_half + txt_half) + 8
    arrays = (w_qkv.transpose(1, 0, 2), img, prev_mod, txt)
    smem = lambda *shape: pltpu.SMEM(shape, jnp.int32)
    got, tail_no = call(
        pack_body,
        (
            shaped(sources, deep + 2 * img_half + 8, width),
            pltpu.HBM((1,), jnp.int32),
        ),
        [HBM] * 5,
        8,
        outs=(VMEM, HBM),
        scratch=[pltpu.VMEM(a.shape, a.dtype) for a in arrays]
        + [smem(batch), smem(1), pltpu.SemaphoreType.DMA((len(arrays) + 2,))],
    )(*(pltpu.with_memory_space_constraint(a, pltpu.HBM) for a in arrays + (refresh,)))
    got = swap(got, (FAR, CORE))
    weight = call(
        spread_body,
        pltpu.HBM((around, sources * deep, kinds * HD), BF16),
        [VMEM],
        8,
        outs=HBM,
        scratch=[
            pltpu.VMEM((sources * deep, kinds * HD), BF16),
            pltpu.SemaphoreType.DMA((around,)),
        ],
    )(got)
    weight = swap(weight, (NEAR, X)).reshape(around, sources, deep, kinds * HD)

    joined, previous = call(
        functools.partial(join_body, deep, img_half, txt_half),
        (shaped(rows, width), shaped(sources * img_half, width)),
        [VMEM] * 2,
        8,
    )(got, modulation)
    wide = lax.all_gather(joined, TP, axis=0, tiled=False)
    own = call(norm_body, shaped(tps, rows, width), [VMEM] * 2, 12)(wide, previous)
    other = lax.ppermute(own, CORE, [(0, 1), (1, 0)])

    query, pairs = call(
        project_body,
        (shaped(2, sources * img_half, HD), shaped(around, 2, rows, 2 * HD)),
        [VMEM] * 4,
        16,
    )(own, other, weight, qk_gain)
    pairs = swap(pairs, (NEAR, X))
    attended = call(
        functools.partial(attend_body, img_half, txt_half),
        shaped(sources, img_rows + 8, HD),
        [SMEM, VMEM, VMEM],
        24,
    )(text_len, query, pairs)
    attended = swap(attended, (FAR, CORE))

    tails = [functools.partial(finish, slots) for slots in range(1, batch)]
    return lax.switch(tail_no[0], tails, refresh, attended, output_weight, cache, img, modulation)


def finish(slots, refresh, attended, output_weight, cache, img, modulation):
    batch, img_rows, width = img.shape
    rows = slots * img_rows + 8
    parts = call(
        functools.partial(mix_body, img_rows),
        shaped(lax.axis_size(TP), rows, width),
        [SMEM, VMEM, VMEM],
        12,
    )(refresh, attended, output_weight)
    parts = swap(parts, TP)
    whole = pltpu.HBM((batch, img_rows, width), F32)
    return call(
        final_body,
        (whole, whole, shaped(batch, dtype=F32)),
        [SMEM] + [VMEM] * 4,
        8,
        outs=(HBM, HBM, SMEM),
        scratch=[pltpu.VMEM((rows, width), F32)]
        + [pltpu.VMEM((batch, img_rows, width), F32)] * 2
        + [pltpu.SemaphoreType.DMA((2, batch))],
    )(refresh, parts, cache, img, modulation)


def solution(mesh):
    finer = Mesh(mesh.devices.reshape(4, 4, 2, 2, mesh.shape["tp"]), SEQ + (TP,))
    in_specs = (
        P(None, SEQ, TP),
        P(None, SEQ, TP),
        P(None, SEQ, TP),
        P(None, SEQ, TP),
        P(None, None, TP),
        P(SEQ, None, TP),
        P(None, TP),
        P(TP, None),
        P(),
        P(),
    )
    out_specs = (P(None, SEQ, TP), P(None, SEQ, TP), P())

    return jax.shard_map(local, mesh=finer, in_specs=in_specs, out_specs=out_specs, check_vma=False)
```

```python
import functools
import math

import jax
import jax.numpy as jnp
from jax import lax
from jax.experimental import pallas as pl
from jax.experimental.pallas import tpu as pltpu
from jax.sharding import Mesh
from jax.sharding import PartitionSpec as P


X, FAR, NEAR, CORE, TP = "seq_0", "seq_1a", "seq_1b", "seq_2", "tp"
SEQ = (X, FAR, NEAR, CORE)
HD = 128
EPS = 0.1
NEG = -1e30
F32 = jnp.float32
BF16 = jnp.bfloat16

VMEM = pl.BlockSpec(memory_space=pltpu.VMEM)
SMEM = pl.BlockSpec(memory_space=pltpu.SMEM)
HBM = pl.BlockSpec(memory_space=pltpu.HBM)


def call(body, out_shape, in_specs, mebibytes, outs=None, scratch=()):
    outs = outs or jax.tree.map(lambda _: VMEM, out_shape)
    return pl.pallas_call(
        body,
        out_shape=out_shape,
        in_specs=in_specs,
        out_specs=outs,
        scratch_shapes=scratch,
        compiler_params=pltpu.CompilerParams(vmem_limit_bytes=mebibytes << 20),
    )


def shaped(*shape, dtype=BF16):
    return jax.ShapeDtypeStruct(shape, dtype)


def swap(value, axis):
    return lax.all_to_all(value, axis, 0, 0, tiled=True)


def split_three(value):
    high = value.astype(BF16).astype(F32)
    rest = value - high
    middle = rest.astype(BF16).astype(F32)
    return high, middle, rest - middle


def stacked_parts(value, rows):
    row = lax.broadcasted_iota(jnp.int32, (rows, value.shape[1]), 0)
    high, middle, low = split_three(value)
    return jnp.where(row == 0, high, jnp.where(row == 1, middle, jnp.where(row == 2, low, 0.0)))


def pack_body(
    w_hbm, img_hbm, prev_hbm, txt_hbm, flag_hbm, out_ref, tail_hbm,
    w_ref, img_ref, prev_ref, txt_ref, flag_ref, tail_ref, sems,
):
    copies = [
        pltpu.make_async_copy(source, target, sems.at[i])
        for i, (source, target) in enumerate(
            (
                (flag_hbm, flag_ref),
                (w_hbm, w_ref),
                (img_hbm, img_ref),
                (prev_hbm, prev_ref),
                (txt_hbm, txt_ref),
            )
        )
    ]
    for copy in copies:
        copy.start()
    copies[0].wait()
    tail_no = jnp.int32(-1)
    for b in range(img_ref.shape[0]):
        tail_no = tail_no + jnp.where(flag_ref[b] == 1, 1, 0)
    tail_ref[0] = tail_no
    tell = pltpu.make_async_copy(tail_ref, tail_hbm, sems.at[len(copies)])
    tell.start()
    for copy in copies[1:]:
        copy.wait()
    kinds, deep, columns = w_ref.shape
    batch, img_rows, width = img_ref.shape
    cores = columns // HD
    img_half = img_rows // cores
    txt_half = txt_ref.shape[1] // cores
    for b in range(batch):
        for c in range(cores):
            to = b * cores + c
            for kind in range(kinds):
                out_ref[to, :deep, kind * HD : (kind + 1) * HD] = w_ref[
                    kind, :, c * HD : (c + 1) * HD
                ]
            at = deep
            for ref in (img_ref, prev_ref):
                out_ref[to, at : at + img_half] = ref[b, c * img_half : (c + 1) * img_half]
                at += img_half
            text = txt_ref[b].astype(F32)[c * txt_half : (c + 1) * txt_half]
            text = jnp.concatenate([text, jnp.zeros((8 - txt_half, width), F32)], axis=0)
            out_ref[to, at : at + 8] = text.astype(BF16)
    tell.wait()


def spread_body(got_ref, out_hbm, block_ref, sems):
    sources = got_ref.shape[0]
    deep = block_ref.shape[0] // sources
    for source in range(sources):
        block_ref[source * deep : (source + 1) * deep] = got_ref[source, :deep]
    copies = [
        pltpu.make_async_copy(block_ref, out_hbm.at[copy], sems.at[copy])
        for copy in range(out_hbm.shape[0])
    ]
    for copy in copies:
        copy.start()
    for copy in copies:
        copy.wait()


def join_body(deep, img_half, txt_half, got_ref, mod_ref, out_ref, prev_ref):
    far = lax.axis_index(FAR)
    sources = got_ref.shape[0]
    width = got_ref.shape[2]
    for source in range(sources):
        out_ref[source * img_half : (source + 1) * img_half] = got_ref[
            source, deep : deep + img_half
        ]
        prev_ref[source * img_half : (source + 1) * img_half] = got_ref[
            source, deep + img_half : deep + 2 * img_half
        ]
    at = deep + 2 * img_half
    texts = [got_ref[source, at : at + 8].astype(F32)[:txt_half] for source in range(sources)]
    vectors = []
    for which in range(2):
        chosen = mod_ref[which, 0:1].astype(F32)
        for b in range(1, mod_ref.shape[1]):
            chosen = jnp.where(far == b, mod_ref[which, b : b + 1].astype(F32), chosen)
        vectors.append(chosen)
    tail = jnp.concatenate(texts + vectors + [jnp.zeros((6, width), F32)], axis=0)
    out_ref[sources * img_half :] = tail.astype(BF16)


def norm_body(x_ref, prev_ref, mod_ref):
    groups, rows, width = x_ref.shape
    vectors = rows - 8
    features = groups * width
    sums = x_ref[0].astype(F32)
    for g in range(1, groups):
        sums = sums + x_ref[g].astype(F32)
    center = jnp.sum(sums, axis=1, keepdims=True) / features
    squares = jnp.square(x_ref[0].astype(F32) - center)
    for g in range(1, groups):
        squares = squares + jnp.square(x_ref[g].astype(F32) - center)
    squares = jnp.sum(squares, axis=1, keepdims=True)
    inv = lax.rsqrt(squares / features + EPS)
    for g in range(groups):
        values = x_ref[g].astype(F32)
        shift = values[vectors : vectors + 1]
        scale = values[vectors + 1 : vectors + 2]
        mod_ref[g] = ((values - center) * inv * (1.0 + scale) + shift).astype(BF16)
    far = lax.axis_index(FAR)
    own = mod_ref.at[lax.axis_index(TP)]
    previous = prev_ref[...].astype(F32)
    numer = jnp.abs(own[: prev_ref.shape[0]].astype(F32) - previous)
    denom = jnp.abs(previous)
    lane = lax.broadcasted_iota(jnp.int32, (1, width), 1)
    line = jnp.where(lane == far, jnp.sum(numer), 0.0)
    line = jnp.where(lane == 4 + far, jnp.sum(denom), line)
    mod_ref[0, vectors:] = stacked_parts(line, 8).astype(BF16)


def project_body(own_ref, other_ref, w_ref, gain_ref, query_ref, pair_ref):
    groups, rows, width = own_ref.shape
    _, sources, deep, columns = w_ref.shape
    near = cores = 2
    xs = w_ref.shape[0] // near
    ys = near * sources // cores
    per_group = width // deep
    total = jnp.zeros((2 * rows, columns), F32)
    for g in range(groups):
        pieces = []
        for step in range(per_group):
            flat = g * per_group + step
            core = flat % cores
            y = flat // cores % ys
            x = flat // cores // ys
            pieces.append(w_ref[y % near * xs + x, y // near * cores + core])
        left = jnp.concatenate([own_ref[g], other_ref[g]], axis=0)
        total = total + jnp.dot(
            left, jnp.concatenate(pieces, axis=0), preferred_element_type=F32
        )
    parts = []
    for kind in range(2):
        part = total[:, kind * HD : (kind + 1) * HD]
        gain = jnp.where(
            lax.axis_index(CORE) == 0, gain_ref[kind : kind + 1, :HD], gain_ref[kind : kind + 1, HD:]
        )
        mean = jnp.mean(jnp.square(part), axis=1, keepdims=True)
        parts.append(part * lax.rsqrt(mean + EPS) * gain)
    query, keyed = parts
    valued = total[:, 2 * HD :].astype(BF16)
    img = query_ref.shape[1]
    for half, ref in enumerate((own_ref, other_ref)):
        at = half * rows
        query_ref[half] = query[at : at + img].astype(BF16)
        carried = ref[0, rows - 8 :, :HD]
        keys = keyed[at : at + rows - 8].astype(BF16)
        for copy in range(pair_ref.shape[0]):
            pair_ref[copy, half, : rows - 8, :HD] = keys
            pair_ref[copy, half, rows - 8 :, :HD] = carried
            pair_ref[copy, half, :, HD:] = valued[at : at + rows]


def attend_body(img_half, txt_half, limit_ref, query_ref, pair_ref, out_ref):
    blocks, halves, rows, _ = pair_ref.shape
    sources = out_ref.shape[0]
    img = sources * img_half
    txt = sources * txt_half
    count = blocks * rows
    far, core = lax.axis_index(FAR), lax.axis_index(CORE)
    query = query_ref[...].reshape(2 * img, HD)
    index = lax.broadcasted_iota(jnp.int32, (1, count), 1)
    slot = index % rows
    block = index // rows
    source = (slot - img) // txt_half
    y = source // 2 * 2 + block // 4
    device = (block % 4 * 8 + y) * 2 + source % 2
    raw_of = []
    rel = jnp.zeros((1, HD), F32)
    for half in range(halves):
        actual = jnp.where(half == 0, core, 1 - core)
        keys = pair_ref[:, half, :, :HD].reshape(count, HD)
        raw = lax.dot_general(
            query, keys, (((1,), (1,)), ((), ())), preferred_element_type=F32
        )
        text = device * 4 + actual * txt_half + (slot - img) % txt_half
        valid = (slot < img) | ((slot < img + txt) & (text < limit_ref[far]))
        raw_of.append(raw + jnp.where(valid, 0.0, NEG))
        for b in range(blocks):
            carried = pair_ref[b, half, rows - 8 :, :HD].astype(F32)
            rel = rel + jnp.sum(carried, axis=0, keepdims=True)
    factor = math.log2(math.e) / HD**0.5
    top = functools.reduce(jnp.maximum, [jnp.max(r, axis=1, keepdims=True) for r in raw_of])
    total = jnp.zeros((2 * img, 1), F32)
    summed = jnp.zeros((2 * img, HD), F32)
    for half in range(halves):
        weights = jnp.exp2((raw_of[half] - top) * factor)
        total = total + jnp.sum(weights, axis=1, keepdims=True)
        values = pair_ref[:, half, :, HD:].reshape(count, HD)
        summed = summed + jnp.dot(weights.astype(BF16), values, preferred_element_type=F32)
    attended = (summed / total).astype(BF16)
    tail = stacked_parts(rel, 8).astype(BF16)
    for half in range(halves):
        actual = jnp.where(half == 0, core, 1 - core)
        at = pl.multiple_of(actual * img_half, img_half)
        for source in range(sources):
            start = half * img + source * img_half
            out_ref[source, pl.ds(at, img_half)] = attended[start : start + img_half]
    for source in range(sources):
        out_ref[source, 2 * img_half :] = tail


def slots_of(flag_ref, batch, count):
    order = [jnp.int32(0)] * count
    seen = jnp.int32(0)
    slot = []
    for b in range(batch):
        on = flag_ref[b] == 1
        slot.append(seen)
        for i in range(count):
            order[i] = jnp.where(on & (seen == i), jnp.int32(b), order[i])
        seen = seen + jnp.where(on, 1, 0)
    return order, slot


def mix_body(img_rows, flag_ref, att_ref, w_ref, out_ref):
    groups, rows, width = out_ref.shape
    heads = w_ref.shape[0] // HD
    batch = att_ref.shape[0] // heads
    slots = (rows - 8) // img_rows
    order, _ = slots_of(flag_ref, batch, slots)
    lefts = []
    for h in range(heads):
        lefts.append(
            jnp.concatenate([att_ref[order[i] * heads + h, :img_rows] for i in range(slots)], axis=0)
        )
    left = jnp.concatenate(lefts, axis=1)
    rel = jnp.zeros((8, HD), F32)
    for b in range(batch):
        rel = rel + att_ref[b * heads, img_rows:].astype(F32)
    tail = stacked_parts(jnp.sum(rel, axis=0, keepdims=True), 8)
    tail = jnp.concatenate([tail, jnp.zeros((8, width - HD), F32)], axis=1).astype(BF16)
    for g in range(groups):
        mixed = jnp.dot(left, w_ref[:, g * width : (g + 1) * width], preferred_element_type=F32)
        out_ref[g, : rows - 8] = mixed.astype(BF16)
        out_ref[g, rows - 8 :] = tail


def final_body(flag_ref, part_ref, cache_ref, img_ref, mod_ref, out_ref, new_ref, rel_ref, sum_ref):
    groups, rows, _ = part_ref.shape
    batch, img_rows, _ = img_ref.shape
    slots = (rows - 8) // img_rows
    mixed = part_ref[0].astype(F32)
    for g in range(1, groups):
        mixed = mixed + part_ref[g].astype(F32)
    sum_ref[...] = mixed
    _, slot = slots_of(flag_ref, batch, slots)
    for b in range(batch):
        gate = mod_ref[2, b : b + 1].astype(F32)
        at = pl.multiple_of(jnp.minimum(slot[b], slots - 1) * img_rows, img_rows)
        resid = gate * sum_ref[pl.ds(at, img_rows)]
        fresh = jnp.where(flag_ref[b] == 1, resid, cache_ref[b])
        new_ref[b] = fresh
        out_ref[b] = img_ref[b].astype(F32) + fresh
    sums = jnp.sum(mixed[rows - 8 :, :HD], axis=0, keepdims=True)
    lane = lax.broadcasted_iota(jnp.int32, (1, HD), 1)
    for b in range(batch):
        numer = jnp.sum(jnp.where(lane == b, sums, 0.0))
        denom = jnp.sum(jnp.where(lane == 4 + b, sums, 0.0))
        rel_ref[b] = numer / jnp.maximum(denom, 1.0)


def local(img, txt, prev_mod, cache, modulation, w_qkv, qk_gain, output_weight, text_len, refresh):
    batch, img_rows, width = img.shape
    xs, fars, nears, cores = (lax.axis_size(a) for a in SEQ)
    tps = lax.axis_size(TP)
    deep, kinds, _ = w_qkv.shape
    sources = fars * cores
    around = xs * nears
    img_half, txt_half = img_rows // cores, txt.shape[1] // cores
    rows = sources * (img_half + txt_half) + 8
    arrays = (w_qkv.transpose(1, 0, 2), img, prev_mod, txt)
    smem = lambda *shape: pltpu.SMEM(shape, jnp.int32)
    got, tail_no = call(
        pack_body,
        (
            shaped(sources, deep + 2 * img_half + 8, width),
            pltpu.HBM((1,), jnp.int32),
        ),
        [HBM] * 5,
        8,
        outs=(VMEM, HBM),
        scratch=[pltpu.VMEM(a.shape, a.dtype) for a in arrays]
        + [smem(batch), smem(1), pltpu.SemaphoreType.DMA((len(arrays) + 2,))],
    )(*(pltpu.with_memory_space_constraint(a, pltpu.HBM) for a in arrays + (refresh,)))
    got = swap(got, (FAR, CORE))
    weight = call(
        spread_body,
        pltpu.HBM((around, sources * deep, kinds * HD), BF16),
        [VMEM],
        8,
        outs=HBM,
        scratch=[
            pltpu.VMEM((sources * deep, kinds * HD), BF16),
            pltpu.SemaphoreType.DMA((around,)),
        ],
    )(got)
    weight = swap(weight, (NEAR, X)).reshape(around, sources, deep, kinds * HD)

    joined, previous = call(
        functools.partial(join_body, deep, img_half, txt_half),
        (shaped(rows, width), shaped(sources * img_half, width)),
        [VMEM] * 2,
        8,
    )(got, modulation)
    wide = lax.all_gather(joined, TP, axis=0, tiled=False)
    own = call(norm_body, shaped(tps, rows, width), [VMEM] * 2, 12)(wide, previous)
    other = lax.ppermute(own, CORE, [(0, 1), (1, 0)])

    query, pairs = call(
        project_body,
        (shaped(2, sources * img_half, HD), shaped(around, 2, rows, 2 * HD)),
        [VMEM] * 4,
        16,
    )(own, other, weight, qk_gain)
    pairs = swap(pairs, (NEAR, X))
    attended = call(
        functools.partial(attend_body, img_half, txt_half),
        shaped(sources, img_rows + 8, HD),
        [SMEM, VMEM, VMEM],
        24,
    )(text_len, query, pairs)
    attended = swap(attended, (FAR, CORE))

    tails = [functools.partial(finish, slots) for slots in range(1, batch)]
    return lax.switch(tail_no[0], tails, refresh, attended, output_weight, cache, img, modulation)


def finish(slots, refresh, attended, output_weight, cache, img, modulation):
    batch, img_rows, width = img.shape
    rows = slots * img_rows + 8
    parts = call(
        functools.partial(mix_body, img_rows),
        shaped(lax.axis_size(TP), rows, width),
        [SMEM, VMEM, VMEM],
        12,
    )(refresh, attended, output_weight)
    parts = swap(parts, TP)
    whole = shaped(batch, img_rows, width, dtype=F32)
    return call(
        final_body,
        (whole, whole, shaped(batch, dtype=F32)),
        [SMEM] + [VMEM] * 4,
        8,
        outs=(VMEM, VMEM, SMEM),
        scratch=[pltpu.VMEM((rows, width), F32)],
    )(refresh, parts, cache, img, modulation)


def solution(mesh):
    finer = Mesh(mesh.devices.reshape(4, 4, 2, 2, mesh.shape["tp"]), SEQ + (TP,))
    in_specs = (
        P(None, SEQ, TP),
        P(None, SEQ, TP),
        P(None, SEQ, TP),
        P(None, SEQ, TP),
        P(None, None, TP),
        P(SEQ, None, TP),
        P(None, TP),
        P(TP, None),
        P(),
        P(),
    )
    out_specs = (P(None, SEQ, TP), P(None, SEQ, TP), P())

    return jax.shard_map(local, mesh=finer, in_specs=in_specs, out_specs=out_specs, check_vma=False)
```

```python
import functools
import math

import jax
import jax.numpy as jnp
from jax import lax
from jax.experimental import pallas as pl
from jax.experimental.pallas import tpu as pltpu
from jax.sharding import Mesh
from jax.sharding import PartitionSpec as P


X, FAR, NEAR, CORE, TP = "seq_0", "seq_1a", "seq_1b", "seq_2", "tp"
SEQ = (X, FAR, NEAR, CORE)
HD = 128
EPS = 0.1
NEG = -1e30
F32 = jnp.float32
BF16 = jnp.bfloat16

VMEM = pl.BlockSpec(memory_space=pltpu.VMEM)
SMEM = pl.BlockSpec(memory_space=pltpu.SMEM)
HBM = pl.BlockSpec(memory_space=pltpu.HBM)


def call(body, out_shape, in_specs, mebibytes, outs=None, scratch=()):
    outs = outs or jax.tree.map(lambda _: VMEM, out_shape)
    return pl.pallas_call(
        body,
        out_shape=out_shape,
        in_specs=in_specs,
        out_specs=outs,
        scratch_shapes=scratch,
        compiler_params=pltpu.CompilerParams(vmem_limit_bytes=mebibytes << 20),
    )


def shaped(*shape, dtype=BF16):
    return jax.ShapeDtypeStruct(shape, dtype)


def swap(value, axis):
    return lax.all_to_all(value, axis, 0, 0, tiled=True)


def split_three(value):
    high = value.astype(BF16).astype(F32)
    rest = value - high
    middle = rest.astype(BF16).astype(F32)
    return high, middle, rest - middle


def stacked_parts(value, rows):
    row = lax.broadcasted_iota(jnp.int32, (rows, value.shape[1]), 0)
    high, middle, low = split_three(value)
    return jnp.where(row == 0, high, jnp.where(row == 1, middle, jnp.where(row == 2, low, 0.0)))


def pack_body(
    w_hbm, img_hbm, prev_hbm, txt_hbm, flag_hbm, out_ref, tail_hbm,
    w_ref, img_ref, prev_ref, txt_ref, flag_ref, tail_ref, sems,
):
    copies = [
        pltpu.make_async_copy(source, target, sems.at[i])
        for i, (source, target) in enumerate(
            (
                (flag_hbm, flag_ref),
                (w_hbm, w_ref),
                (img_hbm, img_ref),
                (prev_hbm, prev_ref),
                (txt_hbm, txt_ref),
            )
        )
    ]
    for copy in copies:
        copy.start()
    copies[0].wait()
    tail_no = jnp.int32(-1)
    for b in range(img_ref.shape[0]):
        tail_no = tail_no + jnp.where(flag_ref[b] == 1, 1, 0)
    tail_ref[0] = tail_no
    tell = pltpu.make_async_copy(tail_ref, tail_hbm, sems.at[len(copies)])
    tell.start()
    for copy in copies[1:]:
        copy.wait()
    kinds, deep, columns = w_ref.shape
    batch, img_rows, width = img_ref.shape
    cores = columns // HD
    img_half = img_rows // cores
    txt_half = txt_ref.shape[1] // cores
    for b in range(batch):
        for c in range(cores):
            to = b * cores + c
            for kind in range(kinds):
                out_ref[to, :deep, kind * HD : (kind + 1) * HD] = w_ref[
                    kind, :, c * HD : (c + 1) * HD
                ]
            at = deep
            for ref in (img_ref, prev_ref):
                out_ref[to, at : at + img_half] = ref[b, c * img_half : (c + 1) * img_half]
                at += img_half
            text = txt_ref[b].astype(F32)[c * txt_half : (c + 1) * txt_half]
            text = jnp.concatenate([text, jnp.zeros((8 - txt_half, width), F32)], axis=0)
            out_ref[to, at : at + 8] = text.astype(BF16)
    tell.wait()


def spread_body(got_ref, out_hbm, block_ref, sems):
    sources = got_ref.shape[0]
    deep = block_ref.shape[0] // sources
    for source in range(sources):
        block_ref[source * deep : (source + 1) * deep] = got_ref[source, :deep]
    copies = [
        pltpu.make_async_copy(block_ref, out_hbm.at[copy], sems.at[copy])
        for copy in range(out_hbm.shape[0])
    ]
    for copy in copies:
        copy.start()
    for copy in copies:
        copy.wait()


def join_body(deep, img_half, txt_half, got_ref, mod_ref, out_ref, prev_ref):
    far = lax.axis_index(FAR)
    sources = got_ref.shape[0]
    width = got_ref.shape[2]
    for source in range(sources):
        out_ref[source * img_half : (source + 1) * img_half] = got_ref[
            source, deep : deep + img_half
        ]
        prev_ref[source * img_half : (source + 1) * img_half] = got_ref[
            source, deep + img_half : deep + 2 * img_half
        ]
    at = deep + 2 * img_half
    texts = [got_ref[source, at : at + 8].astype(F32)[:txt_half] for source in range(sources)]
    vectors = []
    for which in range(2):
        chosen = mod_ref[which, 0:1].astype(F32)
        for b in range(1, mod_ref.shape[1]):
            chosen = jnp.where(far == b, mod_ref[which, b : b + 1].astype(F32), chosen)
        vectors.append(chosen)
    tail = jnp.concatenate(texts + vectors + [jnp.zeros((6, width), F32)], axis=0)
    out_ref[sources * img_half :] = tail.astype(BF16)


def norm_body(x_ref, prev_ref, mod_ref):
    groups, rows, width = x_ref.shape
    vectors = rows - 8
    features = groups * width
    sums = x_ref[0].astype(F32)
    for g in range(1, groups):
        sums = sums + x_ref[g].astype(F32)
    center = jnp.sum(sums, axis=1, keepdims=True) / features
    squares = jnp.square(x_ref[0].astype(F32) - center)
    for g in range(1, groups):
        squares = squares + jnp.square(x_ref[g].astype(F32) - center)
    squares = jnp.sum(squares, axis=1, keepdims=True)
    inv = lax.rsqrt(squares / features + EPS)
    for g in range(groups):
        values = x_ref[g].astype(F32)
        shift = values[vectors : vectors + 1]
        scale = values[vectors + 1 : vectors + 2]
        mod_ref[g] = ((values - center) * inv * (1.0 + scale) + shift).astype(BF16)
    far = lax.axis_index(FAR)
    own = mod_ref.at[lax.axis_index(TP)]
    previous = prev_ref[...].astype(F32)
    numer = jnp.abs(own[: prev_ref.shape[0]].astype(F32) - previous)
    denom = jnp.abs(previous)
    lane = lax.broadcasted_iota(jnp.int32, (1, width), 1)
    line = jnp.where(lane == far, jnp.sum(numer), 0.0)
    line = jnp.where(lane == 4 + far, jnp.sum(denom), line)
    mod_ref[0, vectors:] = stacked_parts(line, 8).astype(BF16)


def project_body(own_ref, other_ref, w_ref, gain_ref, query_ref, pair_ref):
    groups, rows, width = own_ref.shape
    _, sources, deep, columns = w_ref.shape
    near = cores = 2
    xs = w_ref.shape[0] // near
    ys = near * sources // cores
    per_group = width // deep
    total = jnp.zeros((2 * rows, columns), F32)
    for g in range(groups):
        pieces = []
        for step in range(per_group):
            flat = g * per_group + step
            core = flat % cores
            y = flat // cores % ys
            x = flat // cores // ys
            pieces.append(w_ref[y % near * xs + x, y // near * cores + core])
        left = jnp.concatenate([own_ref[g], other_ref[g]], axis=0)
        total = total + jnp.dot(
            left, jnp.concatenate(pieces, axis=0), preferred_element_type=F32
        )
    parts = []
    for kind in range(2):
        part = total[:, kind * HD : (kind + 1) * HD]
        gain = jnp.where(
            lax.axis_index(CORE) == 0, gain_ref[kind : kind + 1, :HD], gain_ref[kind : kind + 1, HD:]
        )
        mean = jnp.mean(jnp.square(part), axis=1, keepdims=True)
        parts.append(part * lax.rsqrt(mean + EPS) * gain)
    query, keyed = parts
    valued = total[:, 2 * HD :].astype(BF16)
    img = query_ref.shape[1]
    carried = jnp.zeros((8, HD), F32)
    for half, ref in enumerate((own_ref, other_ref)):
        at = half * rows
        query_ref[half] = query[at : at + img].astype(BF16)
        keys = keyed[at : at + rows - 8].astype(BF16)
        to = slice(half * (rows - 8), (half + 1) * (rows - 8))
        for copy in range(pair_ref.shape[0]):
            pair_ref[copy, to, :HD] = keys
            pair_ref[copy, to, HD:] = valued[at : at + rows - 8]
        carried = carried + ref[0, rows - 8 :, :HD].astype(F32)
    tail = stacked_parts(jnp.sum(carried, axis=0, keepdims=True), 8).astype(BF16)
    for copy in range(pair_ref.shape[0]):
        pair_ref[copy, 2 * (rows - 8) :, :HD] = tail
        pair_ref[copy, 2 * (rows - 8) :, HD:] = jnp.zeros((8, HD), BF16)


def attend_body(img_half, txt_half, limit_ref, query_ref, pair_ref, out_ref):
    blocks, rows, _ = pair_ref.shape
    halves = 2
    sources = out_ref.shape[0]
    img = sources * img_half
    txt = sources * txt_half
    count = blocks * rows
    far, core = lax.axis_index(FAR), lax.axis_index(CORE)
    query = query_ref[...].reshape(halves * img, HD)
    index = lax.broadcasted_iota(jnp.int32, (1, count), 1)
    spot = index % rows
    block = index // rows
    half = jnp.where(spot >= img + txt, 1, 0)
    slot = spot - half * (img + txt)
    source = (slot - img) // txt_half
    y = source // 2 * 2 + block // 4
    device = (block % 4 * 8 + y) * 2 + source % 2
    actual = jnp.where(half == 0, core, 1 - core)
    text = device * 4 + actual * txt_half + (slot - img) % txt_half
    valid = (slot < img) | ((slot < img + txt) & (text < limit_ref[far]))
    bias = jnp.where(valid & (spot < halves * (img + txt)), 0.0, NEG)
    keys = pair_ref[:, :, :HD].reshape(count, HD)
    raw = lax.dot_general(
        query, keys, (((1,), (1,)), ((), ())), preferred_element_type=F32
    ) + bias
    rel = jnp.zeros((1, HD), F32)
    for b in range(blocks):
        carried = pair_ref[b, rows - 8 :, :HD].astype(F32)
        rel = rel + jnp.sum(carried, axis=0, keepdims=True)
    factor = math.log2(math.e) / HD**0.5
    top = jnp.max(raw, axis=1, keepdims=True)
    weights = jnp.exp2((raw - top) * factor)
    total = jnp.sum(weights, axis=1, keepdims=True)
    values = pair_ref[:, :, HD:].reshape(count, HD)
    summed = jnp.dot(weights.astype(BF16), values, preferred_element_type=F32)
    attended = (summed / total).astype(BF16)
    tail = stacked_parts(rel, 8).astype(BF16)
    for half in range(halves):
        actual = jnp.where(half == 0, core, 1 - core)
        at = pl.multiple_of(actual * img_half, img_half)
        for source in range(sources):
            start = half * img + source * img_half
            out_ref[source, pl.ds(at, img_half)] = attended[start : start + img_half]
    for source in range(sources):
        out_ref[source, 2 * img_half :] = tail


def slots_of(flag_ref, batch, count):
    order = [jnp.int32(0)] * count
    seen = jnp.int32(0)
    slot = []
    for b in range(batch):
        on = flag_ref[b] == 1
        slot.append(seen)
        for i in range(count):
            order[i] = jnp.where(on & (seen == i), jnp.int32(b), order[i])
        seen = seen + jnp.where(on, 1, 0)
    return order, slot


def mix_body(img_rows, flag_ref, att_ref, w_ref, out_ref):
    groups, rows, width = out_ref.shape
    heads = w_ref.shape[0] // HD
    batch = att_ref.shape[0] // heads
    slots = (rows - 8) // img_rows
    order, _ = slots_of(flag_ref, batch, slots)
    lefts = []
    for h in range(heads):
        lefts.append(
            jnp.concatenate([att_ref[order[i] * heads + h, :img_rows] for i in range(slots)], axis=0)
        )
    left = jnp.concatenate(lefts, axis=1)
    rel = jnp.zeros((8, HD), F32)
    for b in range(batch):
        rel = rel + att_ref[b * heads, img_rows:].astype(F32)
    tail = stacked_parts(jnp.sum(rel, axis=0, keepdims=True), 8)
    tail = jnp.concatenate([tail, jnp.zeros((8, width - HD), F32)], axis=1).astype(BF16)
    for g in range(groups):
        mixed = jnp.dot(left, w_ref[:, g * width : (g + 1) * width], preferred_element_type=F32)
        out_ref[g, : rows - 8] = mixed.astype(BF16)
        out_ref[g, rows - 8 :] = tail


def final_body(flag_ref, part_ref, cache_ref, img_ref, mod_ref, out_ref, new_ref, rel_ref, sum_ref):
    groups, rows, _ = part_ref.shape
    batch, img_rows, _ = img_ref.shape
    slots = (rows - 8) // img_rows
    mixed = part_ref[0].astype(F32)
    for g in range(1, groups):
        mixed = mixed + part_ref[g].astype(F32)
    sum_ref[...] = mixed
    _, slot = slots_of(flag_ref, batch, slots)
    for b in range(batch):
        gate = mod_ref[2, b : b + 1].astype(F32)
        at = pl.multiple_of(jnp.minimum(slot[b], slots - 1) * img_rows, img_rows)
        resid = gate * sum_ref[pl.ds(at, img_rows)]
        fresh = jnp.where(flag_ref[b] == 1, resid, cache_ref[b])
        new_ref[b] = fresh
        out_ref[b] = img_ref[b].astype(F32) + fresh
    sums = jnp.sum(mixed[rows - 8 :, :HD], axis=0, keepdims=True)
    lane = lax.broadcasted_iota(jnp.int32, (1, HD), 1)
    for b in range(batch):
        numer = jnp.sum(jnp.where(lane == b, sums, 0.0))
        denom = jnp.sum(jnp.where(lane == 4 + b, sums, 0.0))
        rel_ref[b] = numer / jnp.maximum(denom, 1.0)


def local(img, txt, prev_mod, cache, modulation, w_qkv, qk_gain, output_weight, text_len, refresh):
    batch, img_rows, width = img.shape
    xs, fars, nears, cores = (lax.axis_size(a) for a in SEQ)
    tps = lax.axis_size(TP)
    deep, kinds, _ = w_qkv.shape
    sources = fars * cores
    around = xs * nears
    img_half, txt_half = img_rows // cores, txt.shape[1] // cores
    rows = sources * (img_half + txt_half) + 8
    arrays = (w_qkv.transpose(1, 0, 2), img, prev_mod, txt)
    smem = lambda *shape: pltpu.SMEM(shape, jnp.int32)
    got, tail_no = call(
        pack_body,
        (
            shaped(sources, deep + 2 * img_half + 8, width),
            pltpu.HBM((1,), jnp.int32),
        ),
        [HBM] * 5,
        8,
        outs=(VMEM, HBM),
        scratch=[pltpu.VMEM(a.shape, a.dtype) for a in arrays]
        + [smem(batch), smem(1), pltpu.SemaphoreType.DMA((len(arrays) + 2,))],
    )(*(pltpu.with_memory_space_constraint(a, pltpu.HBM) for a in arrays + (refresh,)))
    got = swap(got, (FAR, CORE))
    weight = call(
        spread_body,
        pltpu.HBM((around, sources * deep, kinds * HD), BF16),
        [VMEM],
        8,
        outs=HBM,
        scratch=[
            pltpu.VMEM((sources * deep, kinds * HD), BF16),
            pltpu.SemaphoreType.DMA((around,)),
        ],
    )(got)
    weight = swap(weight, (NEAR, X)).reshape(around, sources, deep, kinds * HD)

    joined, previous = call(
        functools.partial(join_body, deep, img_half, txt_half),
        (shaped(rows, width), shaped(sources * img_half, width)),
        [VMEM] * 2,
        8,
    )(got, modulation)
    wide = lax.all_gather(joined, TP, axis=0, tiled=False)
    own = call(norm_body, shaped(tps, rows, width), [VMEM] * 2, 12)(wide, previous)
    other = lax.ppermute(own, CORE, [(0, 1), (1, 0)])

    query, pairs = call(
        project_body,
        (shaped(2, sources * img_half, HD), shaped(around, 2 * rows - 8, 2 * HD)),
        [VMEM] * 4,
        16,
    )(own, other, weight, qk_gain)
    pairs = swap(pairs, (NEAR, X))
    attended = call(
        functools.partial(attend_body, img_half, txt_half),
        shaped(sources, img_rows + 8, HD),
        [SMEM, VMEM, VMEM],
        24,
    )(text_len, query, pairs)
    attended = swap(attended, (FAR, CORE))

    tails = [functools.partial(finish, slots) for slots in range(1, batch)]
    return lax.switch(tail_no[0], tails, refresh, attended, output_weight, cache, img, modulation)


def finish(slots, refresh, attended, output_weight, cache, img, modulation):
    batch, img_rows, width = img.shape
    rows = slots * img_rows + 8
    parts = call(
        functools.partial(mix_body, img_rows),
        shaped(lax.axis_size(TP), rows, width),
        [SMEM, VMEM, VMEM],
        12,
    )(refresh, attended, output_weight)
    parts = swap(parts, TP)
    whole = shaped(batch, img_rows, width, dtype=F32)
    return call(
        final_body,
        (whole, whole, shaped(batch, dtype=F32)),
        [SMEM] + [VMEM] * 4,
        8,
        outs=(VMEM, VMEM, SMEM),
        scratch=[pltpu.VMEM((rows, width), F32)],
    )(refresh, parts, cache, img, modulation)


def solution(mesh):
    finer = Mesh(mesh.devices.reshape(4, 4, 2, 2, mesh.shape["tp"]), SEQ + (TP,))
    in_specs = (
        P(None, SEQ, TP),
        P(None, SEQ, TP),
        P(None, SEQ, TP),
        P(None, SEQ, TP),
        P(None, None, TP),
        P(SEQ, None, TP),
        P(None, TP),
        P(TP, None),
        P(),
        P(),
    )
    out_specs = (P(None, SEQ, TP), P(None, SEQ, TP), P())

    return jax.shard_map(local, mesh=finer, in_specs=in_specs, out_specs=out_specs, check_vma=False)
```
